32 devices in a mesh: slab: 2 (over x), row: 8 (over z, y), col: 2 (over core).
Axes of the slice: x: 2, y: 2, z: 4, core: 2. Of those that a mesh axis runs over, the one named last changes fastest.
Arguments:
- image: float32 [1024, 4096], P(('slab', 'row'), 'col'), parts along dimension 0, may hold values from -6 to 6
Outputs:
- dog_fine: bfloat16 [4, 1024, 4096], P(None, ('slab', 'row'), 'col'), parts along dimension 1
- hessian_fine: bfloat16 [2, 1024, 4096], P(None, ('slab', 'row'), 'col'), parts along dimension 1
- dog_coarse: bfloat16 [4, 512, 2048], P(None, ('slab', 'row', 'col')), parts along dimension 1
- hessian_coarse: bfloat16 [2, 512, 2048], P(None, ('slab', 'row', 'col')), parts along dimension 1
The draws below stay inside these ranges and needn't reach their ends.
There are 2 independent parts, one for each index of `slab`. The reference program is written for one: setup_inputs(seed, part) draws one part's arguments, and reference() takes and returns one part's arrays. A program takes and returns all parts, laid end to end along the dimension named above; each array names one. Nothing has to cross between parts.
All inputs are finite; a program needn't handle non-finite values.
Results may differ from the reference program's by a relative error of at most 0.0013.
Values may be sent and summed in bfloat16 or wider, within the bound.
No kernel may reach another device: no remote copies, remote signals or barrier semaphores. Data moves between devices by JAX's collectives and lax.ppermute only.
A program may use at most 64 MiB of HBM per device.

```python
import jax
import jax.numpy as jnp
from jax import lax

H = 512
W = 4096


def block_scale(rng, extent, split, low, largest):
    def one(dim, blocks):
        heights = jax.random.uniform(jax.random.fold_in(jax.random.fold_in(rng, 6), dim), (blocks,), jnp.float32, low / len(split), largest / len(split))
        return jnp.repeat(jnp.exp(heights), extent[dim] // blocks).reshape((-1,) + (1,) * (len(extent) - dim - 1))

    loudness = one(*split[0])
    for cut in split[1:]:
        loudness = loudness * one(*cut)
    return loudness


def normal_values(own_key, extent, scale, limit, cuts=(), kind=jnp.bfloat16):
    entries = jax.random.normal(own_key, extent, jnp.float32) * scale
    if len(cuts) > 0:
        entries = block_scale(own_key, extent, cuts, -0.22, 0.18) * entries
    return jnp.clip(entries, min=-limit, max=limit).astype(kind)


def setup_inputs(seed: int = 0, part: int = 0) -> dict:
    streams_of = jax.random.split(jax.random.key(seed), 2)
    part_splits = jax.random.split(jax.random.fold_in(streams_of[1], part), 2)
    return {
        "image": normal_values(part_splits[0], (H, W), 1.0, 6.0, ((0, 8), (1, 2)), jnp.float32),
    }


SIGMAS = [1.6 * 2.0 ** (k / 4.0) for k in range(5)]


def taps(sigma):
    offset = jnp.arange(25).astype(jnp.float32) - 12.0
    weights = jnp.exp(-offset * offset / (2.0 * sigma * sigma))
    return weights / jnp.sum(weights)


def blur(field, sigma):
    kernel = taps(sigma)
    data = field[None, None]
    vertical = lax.conv_general_dilated(data, kernel[None, None, :, None], (1, 1), ((12, 12), (0, 0)), precision=lax.Precision.HIGHEST)
    both = lax.conv_general_dilated(vertical, kernel[None, None, None, :], (1, 1), ((0, 0), (12, 12)), precision=lax.Precision.HIGHEST)
    return both[0, 0]


def hessian(diff):
    padded = jnp.pad(diff, 1)
    dxx = padded[1:-1, 2:] + padded[1:-1, :-2] - 2.0 * diff
    dyy = padded[2:, 1:-1] + padded[:-2, 1:-1] - 2.0 * diff
    dxy = (padded[2:, 2:] - padded[2:, :-2] - padded[:-2, 2:] + padded[:-2, :-2]) / 4.0
    return dxx * dyy - dxy * dxy


def octave(base, dog_gain, hess_gain):
    levels = [blur(base, s) for s in SIGMAS]
    diffs = [levels[k + 1] - levels[k] for k in range(4)]
    dogs = jnp.stack([(dog_gain * d).astype(jnp.bfloat16) for d in diffs])
    hess = jnp.stack([(hess_gain * hessian(diffs[m + 1])).astype(jnp.bfloat16) for m in range(2)])
    return dogs, hess, levels[4]


def reference(image):
    dog_fine, hessian_fine, top_level = octave(image, 20.0, 5000.0)
    coarse_base = top_level[0::2, 0::2]
    dog_coarse, hessian_coarse, unused = octave(coarse_base, 80.0, 200000.0)
    return dog_fine, hessian_fine, dog_coarse, hessian_coarse
```

```python
import jax
import jax.numpy as jnp
import numpy as np
from jax import lax
from jax.experimental import pallas as pl
from jax.experimental.pallas import tpu as pltpu
from jax.sharding import PartitionSpec as P

SIGMAS = [1.6 * 2.0 ** (k / 4.0) for k in range(5)]
LEVELS = len(SIGMAS)
REACH = 12
LANES = 128
BLOCK = 256
PAD = 8
FAR = 40
NEAR = 8
BF16 = jnp.bfloat16
F32 = jnp.float32


def taps(sigma):
    offset = np.arange(2 * REACH + 1, dtype=np.float64) - REACH
    weights = np.exp(-offset * offset / (2.0 * sigma * sigma))
    return (weights / weights.sum()).astype(np.float32)


def two_parts(matrix):
    high = np.asarray(matrix, np.float32).astype(BF16)
    low = (np.asarray(matrix, np.float32) - high.astype(np.float32)).astype(BF16)
    return high, low


def tap_at(sigma, index):
    weights = taps(sigma)
    inside = (index >= 0) & (index <= 2 * REACH)
    return np.where(inside, weights[np.clip(index, 0, 2 * REACH)], np.float32(0.0))


def row_matrix(sigma, centres, inputs):
    return tap_at(sigma, inputs[None, :] - centres[:, None] + REACH)


def column_weights(sigma, step):
    width = BLOCK * step
    out = np.arange(BLOCK)[None, :] * step
    high, low = two_parts(tap_at(sigma, np.arange(width)[:, None] - out + REACH))
    lane = np.arange(LANES)[:, None]
    right = np.where(lane < REACH, tap_at(sigma, width + lane - out + REACH), 0.0)
    left = np.where(lane >= LANES - REACH, tap_at(sigma, lane - LANES - out + REACH), 0.0)
    edge_high, edge_low = two_parts(right + left)
    edge = np.concatenate([edge_high.astype(np.float32), edge_high.astype(np.float32)])
    edge[:LANES] += np.roll(edge_low.astype(np.float32), 32, axis=0)
    return high, low, edge.astype(BF16)


def split(value):
    high = value.astype(BF16)
    low = (value - high.astype(F32)).astype(BF16)
    return high, low


def mm(a, b):
    return jnp.dot(a, b, preferred_element_type=F32)


def edge_columns(high, low, at, width):
    def both(ref):
        left = ref[:, at - LANES : at].astype(F32)
        right = ref[:, at + width : at + width + LANES].astype(F32)
        lane = lax.broadcasted_iota(jnp.int32, left.shape, 1)
        return jnp.where(lane < LANES // 2, right, left), lane

    eh, lane = both(high)
    el, _ = both(low)
    again = pltpu.roll(eh, 32, 1)
    eh = jnp.where((lane >= 16) & (lane < 64), again, eh)
    return jnp.concatenate([eh.astype(BF16), el.astype(BF16)], axis=1)


def hess_rows(d, first, count, at, width):
    up = d[first - 1 : first - 1 + count, at : at + width]
    mid = d[first : first + count, at : at + width]
    down = d[first + 1 : first + 1 + count, at : at + width]
    whole = slice(first - 1, first + count + 1)
    after = d[whole, at + 1 : at + width + 1]
    before = d[whole, at - 1 : at + width - 1]
    across = after - before
    twice = 2.0 * mid
    dxx = after[1:-1] + before[1:-1] - twice
    dyy = up + down - twice
    dxy = (across[2:] - across[:-2]) * 0.25
    return dxx * dyy - dxy * dxy


def pack_kernel(x_ref, side_ref, own_ref, up_ref, down_ref):
    rows, cols = x_ref.shape

    def put(value, lo, hi):
        high, low = split(value)
        own_ref[:rows, lo:hi] = high
        own_ref[rows:, lo:hi] = low
        up_ref[:FAR, lo:hi] = high[:FAR]
        up_ref[FAR:, lo:hi] = low[:NEAR]
        down_ref[:FAR, lo:hi] = high[rows - FAR :]
        down_ref[FAR:, lo:hi] = low[rows - NEAR :]

    for at in range(0, cols, BLOCK):
        put(x_ref[:, at : at + BLOCK], at, at + BLOCK)
    put(side_ref[...], cols, cols + LANES)


def fine_kernel(place_ref, own_ref, top_ref, bot_ref, lh_ref, ll_ref, bh_ref, bl_ref,
                wc_ref, wl_ref, we_ref, dc_ref, dl_ref, de_ref,
                dog_ref, hess_ref, keep_ref, send_ref,
                vh, vl, bvh, bvl, lev, d1, d2):
    _, out_rows, cols = dog_ref.shape
    row, col, last_row, coarse_height = place_ref[0], place_ref[1], place_ref[2], place_ref[3]
    tall = out_rows + 2 * PAD
    base_rows = bh_ref.shape[1]
    diffs = {1: d1, 2: d2}
    is_left = col == 0

    def rows_of(at, width):
        stack = jnp.concatenate(
            [own_ref[:, at : at + width], top_ref[:, at : at + width], bot_ref[:, at : at + width]], axis=0
        )
        base = mm(bh_ref[col], stack) + mm(bl_ref[col], stack)
        yield None, base
        for s in range(LEVELS):
            part = slice(s * tall, (s + 1) * tall)
            yield s, mm(lh_ref[part], stack) + mm(ll_ref[part], stack)

    for at in range(0, cols, BLOCK):
        for s, value in rows_of(at, BLOCK):
            high, low = split(value)
            to = slice(LANES + at, LANES + at + BLOCK)
            if s is None:
                bvh[:, to], bvl[:, to] = high, low
            else:
                vh[s, :, to], vl[s, :, to] = high, low
    for s, value in rows_of(cols, LANES):
        left = jnp.where(is_left, 0.0, value)
        right = jnp.where(is_left, value, 0.0)
        for part, to in ((left, slice(0, LANES)), (right, slice(LANES + cols, 2 * LANES + cols))):
            high, low = split(part)
            if s is None:
                bvh[:, to], bvl[:, to] = high, low
            else:
                vh[s, :, to], vl[s, :, to] = high, low

    first_keep = row * (out_rows // 2) - REACH - 1 + col * (out_rows // 4)
    first_send = row * (out_rows // 2) - REACH - 1 + (1 - col) * (out_rows // 4)
    half = base_rows // 2
    index = lax.broadcasted_iota(jnp.int32, (base_rows, BLOCK), 0)
    place = jnp.where(index < half, first_keep + index, first_send + index - half)
    inside = (place >= 0) & (place < coarse_height)
    for j in range(cols // (2 * BLOCK)):
        at = LANES + 2 * BLOCK * j
        high = bvh[:, at : at + 2 * BLOCK]
        low = bvl[:, at : at + 2 * BLOCK]
        edge = edge_columns(bvh, bvl, at, 2 * BLOCK)
        value = mm(high, dc_ref[...]) + mm(low, dc_ref[...]) + mm(high, dl_ref[...]) + mm(edge, de_ref[...])
        value = jnp.where(inside, value, 0.0)
        keep_ref[:, j * BLOCK : (j + 1) * BLOCK] = value[:half]
        send_ref[:, j * BLOCK : (j + 1) * BLOCK] = value[half:]

    group = 4
    seam = pl.multiple_of(jnp.where(is_left, cols, 0), LANES)
    for s in range(LEVELS):
        k = s - 1
        for g in range(0, cols // BLOCK, group):
            ats = [LANES + BLOCK * (g + i) for i in range(group)]
            high = jnp.concatenate([vh[s, :, at : at + BLOCK] for at in ats], axis=0)
            low = jnp.concatenate([vl[s, :, at : at + BLOCK] for at in ats], axis=0)
            edge = jnp.concatenate([edge_columns(vh.at[s], vl.at[s], at, BLOCK) for at in ats], axis=0)
            value = mm(high, wc_ref[s]) + mm(low, wc_ref[s]) + mm(high, wl_ref[s]) + mm(edge, we_ref[s])
            for i, at in enumerate(ats):
                new = value[i * tall : (i + 1) * tall]
                if s > 0:
                    d = new - lev[:, at : at + BLOCK]
                    dog_ref[k, :, at - LANES : at - LANES + BLOCK] = (20.0 * d[PAD : PAD + out_rows]).astype(BF16)
                    if k in diffs:
                        diffs[k][:, at : at + BLOCK] = d
                lev[:, at : at + BLOCK] = new
        if s in (1, 2, 3):
            high = vh[s, :, pl.ds(seam, BLOCK)]
            low = vl[s, :, pl.ds(seam, BLOCK)]
            new = mm(high, wc_ref[s]) + mm(low, wc_ref[s]) + mm(high, wl_ref[s])
            if s > 1:
                d = new - lev[:, cols + 2 * LANES :]
                diffs[k][:, :LANES] = jnp.where(is_left, 0.0, d[:, :LANES])
                diffs[k][:, cols + LANES :] = jnp.where(is_left, d[:, LANES:], 0.0)
            lev[:, cols + 2 * LANES :] = new

    for m, k in enumerate((1, 2)):
        d = diffs[k]

        @pl.when(row == 0)
        def _():
            d[PAD - 1 : PAD, :] = jnp.zeros((1, d.shape[1]), F32)

        @pl.when(row == last_row)
        def _():
            d[PAD + out_rows : PAD + out_rows + 1, :] = jnp.zeros((1, d.shape[1]), F32)

        for at in range(0, cols, BLOCK):
            h = hess_rows(d, PAD, out_rows, LANES + at, BLOCK)
            hess_ref[m, :, at : at + BLOCK] = (5000.0 * h).astype(BF16)


def coarse_kernel(place_ref, keep_ref, other_ref, lh_ref, wc_ref, wl_ref, we_ref,
                  dog_ref, hess_ref, vh, vl, lev, d1, d2):
    _, out_rows, cols = dog_ref.shape
    row, col, last_row = place_ref[0], place_ref[1], place_ref[2]
    tall = out_rows + 2 * PAD
    diffs = {1: d1, 2: d2}
    is_left = col == 0
    half = cols // 2
    zero = jnp.zeros((tall, LANES), BF16)
    for s in range(LEVELS):
        for ref in (vh, vl):
            ref[s, :, :LANES] = zero
            ref[s, :, LANES + cols :] = zero
    zero = jnp.zeros((tall, LANES), F32)
    for d in (d1, d2):
        d[:, :LANES] = zero
        d[:, LANES + cols :] = zero

    for at in range(0, cols, BLOCK):
        source = slice(at % half, at % half + BLOCK)
        first = is_left if at < half else jnp.logical_not(is_left)
        high, low = split(jnp.where(first, keep_ref[:, source], other_ref[:, source]))
        stack = jnp.concatenate([high, low, high], axis=0)
        value = mm(lh_ref[...], stack)
        to = slice(LANES + at, LANES + at + BLOCK)
        for s in range(LEVELS):
            vh[s, :, to], vl[s, :, to] = split(value[s * tall : (s + 1) * tall])

    group = 8
    for s in range(LEVELS):
        k = s - 1
        for g in range(0, cols // BLOCK, group):
            ats = [LANES + BLOCK * (g + i) for i in range(group)]
            high = jnp.concatenate([vh[s, :, at : at + BLOCK] for at in ats], axis=0)
            low = jnp.concatenate([vl[s, :, at : at + BLOCK] for at in ats], axis=0)
            edge = jnp.concatenate([edge_columns(vh.at[s], vl.at[s], at, BLOCK) for at in ats], axis=0)
            value = mm(high, wc_ref[s]) + mm(low, wc_ref[s]) + mm(high, wl_ref[s]) + mm(edge, we_ref[s])
            for i, at in enumerate(ats):
                new = value[i * tall : (i + 1) * tall]
                if s > 0:
                    d = new - lev[:, at : at + BLOCK]
                    dog_ref[k, :, at - LANES : at - LANES + BLOCK] = (80.0 * d[PAD : PAD + out_rows]).astype(BF16)
                    if k in diffs:
                        diffs[k][:, at : at + BLOCK] = d
                lev[:, at : at + BLOCK] = new

    for m, k in enumerate((1, 2)):
        d = diffs[k]

        @pl.when((row == 0) & (col == 0))
        def _():
            d[PAD - 1 : PAD, :] = jnp.zeros((1, d.shape[1]), F32)

        @pl.when((row == last_row) & (col == 1))
        def _():
            d[PAD + out_rows : PAD + out_rows + 1, :] = jnp.zeros((1, d.shape[1]), F32)

        for at in range(0, cols, BLOCK):
            h = hess_rows(d, PAD, out_rows, LANES + at, BLOCK)
            hess_ref[m, :, at : at + BLOCK] = (200000.0 * h).astype(BF16)


def fine_constants(rows):
    own = np.arange(rows)
    top = np.arange(-FAR, 0)
    bot = np.arange(rows, rows + FAR)
    inputs = np.concatenate([own, own, top, top[FAR - NEAR :], bot, bot[:NEAR]])
    is_high = np.concatenate(
        [np.ones(rows), np.zeros(rows), np.ones(FAR), np.zeros(NEAR), np.ones(FAR), np.zeros(NEAR)]
    )

    def matrices(sigma, centres, valid):
        high, low = two_parts(row_matrix(sigma, centres, inputs) * valid[:, None])
        return high, (low.astype(np.float32) * is_high[None, :]).astype(BF16)

    centres = np.arange(-PAD, rows + PAD)
    valid = ((centres >= -1) & (centres <= rows)).astype(np.float32)
    level = [matrices(s, centres, valid) for s in SIGMAS]
    strip = rows // 4
    count = strip + 2 * (REACH + 1)
    padded = -(-count // 16) * 16
    ok = (np.arange(padded) < count).astype(np.float32)
    base = []
    for core in range(2):
        both = [2 * (c * strip - REACH - 1 + np.arange(padded)) for c in (core, 1 - core)]
        base.append(matrices(SIGMAS[-1], np.concatenate(both), np.concatenate([ok, ok])))
    return (
        np.concatenate([a for a, _ in level]),
        np.concatenate([b for _, b in level]),
        np.stack([a for a, _ in base]),
        np.stack([b for _, b in base]),
        padded,
    )


def coarse_constants(strip, padded):
    inputs = np.arange(padded) - REACH - 1
    centres = np.arange(-PAD, strip + PAD)
    valid = ((centres >= -1) & (centres <= strip)).astype(np.float32)
    parts = []
    for s in SIGMAS:
        high, low = two_parts(row_matrix(s, centres, inputs) * valid[:, None])
        parts.append(np.concatenate([high, high, low], axis=1))
    return np.concatenate(parts)


def vmem_specs(count):
    return [pl.BlockSpec(memory_space=pltpu.VMEM) for _ in range(count)]


def local(image):
    rows, cols = image.shape
    row_count = lax.axis_size("row")
    row = lax.axis_index("row")
    col = lax.axis_index("col")
    strip = rows // 4
    lh, ll, bh, bl, padded = fine_constants(rows)
    cw = coarse_constants(strip, padded)
    bands = [column_weights(s, 1) for s in SIGMAS]
    wc, wl, we = (np.stack([b[i] for b in bands]) for i in range(3))
    dc, dl, de = column_weights(SIGMAS[-1], 2)
    place = jnp.stack([row, col, jnp.int32(row_count - 1), jnp.int32(row_count * rows // 2)]).astype(jnp.int32)

    side = jnp.where(col == 0, image[:, cols - LANES :], image[:, :LANES])
    side = lax.ppermute(side, "col", [(0, 1), (1, 0)])
    wide = cols + LANES
    own, up, down = pl.pallas_call(
        pack_kernel,
        out_shape=(
            jax.ShapeDtypeStruct((2 * rows, wide), BF16),
            jax.ShapeDtypeStruct((FAR + NEAR, wide), BF16),
            jax.ShapeDtypeStruct((FAR + NEAR, wide), BF16),
        ),
        in_specs=vmem_specs(2),
        out_specs=tuple(vmem_specs(3)),
        name="pack",
    )(image, side)
    bot = lax.ppermute(up, "row", [(i + 1, i) for i in range(row_count - 1)])
    top = lax.ppermute(down, "row", [(i, i + 1) for i in range(row_count - 1)])

    tall = rows + 2 * PAD
    smem = pl.BlockSpec(memory_space=pltpu.SMEM)
    dog_fine, hess_fine, keep, send = pl.pallas_call(
        fine_kernel,
        out_shape=(
            jax.ShapeDtypeStruct((4, rows, cols), BF16),
            jax.ShapeDtypeStruct((2, rows, cols), BF16),
            jax.ShapeDtypeStruct((padded, cols // 2), F32),
            jax.ShapeDtypeStruct((padded, cols // 2), F32),
        ),
        in_specs=[smem] + vmem_specs(13),
        out_specs=tuple(vmem_specs(4)),
        scratch_shapes=[
            pltpu.VMEM((LEVELS, tall, cols + 2 * LANES), BF16),
            pltpu.VMEM((LEVELS, tall, cols + 2 * LANES), BF16),
            pltpu.VMEM((2 * padded, cols + 2 * LANES), BF16),
            pltpu.VMEM((2 * padded, cols + 2 * LANES), BF16),
            pltpu.VMEM((tall, cols + 2 * LANES + BLOCK), F32),
            pltpu.VMEM((tall, cols + 2 * LANES), F32),
            pltpu.VMEM((tall, cols + 2 * LANES), F32),
        ],
        name="fine",
    )(place, own, top, bot, lh, ll, bh, bl, wc, wl, we, dc, dl, de)

    other = lax.ppermute(send, "col", [(0, 1), (1, 0)])
    small = strip + 2 * PAD
    dog_coarse, hess_coarse = pl.pallas_call(
        coarse_kernel,
        out_shape=(
            jax.ShapeDtypeStruct((4, strip, cols), BF16),
            jax.ShapeDtypeStruct((2, strip, cols), BF16),
        ),
        in_specs=[smem] + vmem_specs(6),
        out_specs=tuple(vmem_specs(2)),
        scratch_shapes=[
            pltpu.VMEM((LEVELS, small, cols + 2 * LANES), BF16),
            pltpu.VMEM((LEVELS, small, cols + 2 * LANES), BF16),
            pltpu.VMEM((small, cols + 2 * LANES), F32),
            pltpu.VMEM((small, cols + 2 * LANES), F32),
            pltpu.VMEM((small, cols + 2 * LANES), F32),
        ],
        name="coarse",
    )(place, keep, other, cw, wc, wl, we)
    return dog_fine, hess_fine, dog_coarse, hess_coarse


def solution(mesh):
    return jax.shard_map(
        local,
        mesh=mesh,
        in_specs=(P(("slab", "row"), "col"),),
        out_specs=(
            P(None, ("slab", "row"), "col"),
            P(None, ("slab", "row"), "col"),
            P(None, ("slab", "row", "col"), None),
            P(None, ("slab", "row", "col"), None),
        ),
        check_vma=False,
    )
```

```python
import jax
import jax.numpy as jnp
import numpy as np
from jax import lax
from jax.experimental import pallas as pl
from jax.experimental.pallas import tpu as pltpu
from jax.sharding import PartitionSpec as P

SIGMAS = [1.6 * 2.0 ** (k / 4.0) for k in range(5)]
LEVELS = len(SIGMAS)
REACH = 12
LANES = 128
BLOCK = 256
PAD = 8
FAR = 40
NEAR = 8
BF16 = jnp.bfloat16
F32 = jnp.float32


def taps(sigma):
    offset = np.arange(2 * REACH + 1, dtype=np.float64) - REACH
    weights = np.exp(-offset * offset / (2.0 * sigma * sigma))
    return (weights / weights.sum()).astype(np.float32)


def two_parts(matrix):
    high = np.asarray(matrix, np.float32).astype(BF16)
    low = (np.asarray(matrix, np.float32) - high.astype(np.float32)).astype(BF16)
    return high, low


def tap_at(sigma, index):
    weights = taps(sigma)
    inside = (index >= 0) & (index <= 2 * REACH)
    return np.where(inside, weights[np.clip(index, 0, 2 * REACH)], np.float32(0.0))


def row_matrix(sigma, centres, inputs):
    return tap_at(sigma, inputs[None, :] - centres[:, None] + REACH)


def column_weights(sigma, step):
    width = BLOCK * step
    out = np.arange(BLOCK)[None, :] * step
    high, low = two_parts(tap_at(sigma, np.arange(width)[:, None] - out + REACH))
    lane = np.arange(LANES)[:, None]
    right = np.where(lane < REACH, tap_at(sigma, width + lane - out + REACH), 0.0)
    left = np.where(lane >= LANES - REACH, tap_at(sigma, lane - LANES - out + REACH), 0.0)
    edge_high, edge_low = two_parts(right + left)
    edge = np.concatenate([edge_high.astype(np.float32), edge_high.astype(np.float32)])
    edge[:LANES] += np.roll(edge_low.astype(np.float32), 32, axis=0)
    return high, low, edge.astype(BF16)


def split(value):
    high = value.astype(BF16)
    low = (value - high.astype(F32)).astype(BF16)
    return high, low


def mm(a, b):
    return jnp.dot(a, b, preferred_element_type=F32)


def edge_columns(high, low, at, width):
    def both(ref):
        left = ref[:, at - LANES : at].astype(F32)
        right = ref[:, at + width : at + width + LANES].astype(F32)
        lane = lax.broadcasted_iota(jnp.int32, left.shape, 1)
        return jnp.where(lane < LANES // 2, right, left), lane

    eh, lane = both(high)
    el, _ = both(low)
    again = pltpu.roll(eh, 32, 1)
    eh = jnp.where((lane >= 16) & (lane < 64), again, eh)
    return jnp.concatenate([eh.astype(BF16), el.astype(BF16)], axis=1)


def hess_tiles(d, rows, first_tile, count, gain, put):
    tall = rows + 2 * PAD
    lane = lax.broadcasted_iota(jnp.int32, (tall, LANES), 1)
    tile = lambda t: d[:, (first_tile + t + 1) * LANES : (first_tile + t + 2) * LANES]
    tiles = {-1: tile(-1), 0: tile(0)}
    back = {t: pltpu.roll(tiles[t], 1, 1) for t in (-1, 0)}
    ahead = {0: pltpu.roll(tiles[0], LANES - 1, 1)}
    for t in range(count):
        tiles[t + 1] = tile(t + 1)
        back[t + 1] = pltpu.roll(tiles[t + 1], 1, 1)
        ahead[t + 1] = pltpu.roll(tiles[t + 1], LANES - 1, 1)
        before = jnp.where(lane == 0, back[t - 1], back[t])
        after = jnp.where(lane == LANES - 1, ahead[t + 1], ahead[t])
        across = after - before
        mid = slice(PAD, PAD + rows)
        up, down = pltpu.roll(tiles[t], 1, 0)[mid], pltpu.roll(tiles[t], tall - 1, 0)[mid]
        twice = 2.0 * tiles[t][mid]
        dxx = after[mid] + before[mid] - twice
        dyy = up + down - twice
        dxy = (pltpu.roll(across, tall - 1, 0)[mid] - pltpu.roll(across, 1, 0)[mid]) * 0.25
        put(first_tile + t, (gain * (dxx * dyy - dxy * dxy)).astype(BF16))


def pack_kernel(x_hbm, own_ref, up_ref, down_ref, x_ref, sem):
    copy = pltpu.make_async_copy(x_hbm, x_ref, sem)
    copy.start()
    copy.wait()
    rows, cols = x_ref.shape
    for at in range(0, cols, BLOCK):
        to = slice(at, at + BLOCK)
        pack(x_ref[:, to], to, own_ref, up_ref, down_ref)


def pack(value, to, own_ref, up_ref, down_ref):
    rows = value.shape[0]
    high, low = split(value)
    own_ref[:rows, to] = high
    own_ref[rows:, to] = low
    near = 2 * NEAR
    up_ref[: 2 * near, to] = high[: 2 * near]
    up_ref[2 * near :, to] = jnp.concatenate([low[:NEAR], high[2 * near : FAR]], axis=0)
    down_ref[:near, to] = high[rows - near :]
    down_ref[near:FAR, to] = high[rows - FAR : rows - near]
    down_ref[FAR:, to] = low[rows - NEAR :]


def side_kernel(side_ref, own_in, up_in, down_in, own_ref, up_ref, down_ref):
    cols = own_ref.shape[1] - LANES
    pack(side_ref[...], slice(cols, cols + LANES), own_ref, up_ref, down_ref)


def stage_kernel(*refs):
    count = (len(refs) - 1) // 2
    sems = refs[-1]
    copies = [pltpu.make_async_copy(refs[i], refs[count + i], sems.at[i]) for i in range(count)]
    for copy in copies:
        copy.start()
    for copy in copies:
        copy.wait()


def base_kernel(place_ref, own_ref, top_ref, bot_ref, bh_ref, bl_ref, dc_ref, dl_ref, de_ref,
                keep_ref, send_ref, bvh, bvl):
    row, col, coarse_height = place_ref[0], place_ref[1], place_ref[3]
    tile_rows = own_ref.shape[0] // 2
    cols = own_ref.shape[1] - LANES
    base_rows = bh_ref.shape[1]
    is_left = col == 0
    bh, bl = bh_ref[col], bl_ref[col]

    def rows_of(at, width):
        part = slice(at, at + width)
        stack = jnp.concatenate([own_ref[:, part], top_ref[:, part], bot_ref[:, part]], axis=0)
        return mm(bh, stack) + mm(bl, stack)

    for at in range(0, cols, BLOCK):
        to = slice(LANES + at, LANES + at + BLOCK)
        bvh[:, to], bvl[:, to] = split(rows_of(at, BLOCK))
    value = rows_of(cols, LANES)
    bvh[:, :LANES], bvl[:, :LANES] = split(jnp.where(is_left, 0.0, value))
    bvh[:, LANES + cols :], bvl[:, LANES + cols :] = split(jnp.where(is_left, value, 0.0))

    first_keep = row * (tile_rows // 2) - REACH - 1 + col * (tile_rows // 4)
    first_send = row * (tile_rows // 2) - REACH - 1 + (1 - col) * (tile_rows // 4)
    half = base_rows // 2
    index = lax.broadcasted_iota(jnp.int32, (base_rows, BLOCK), 0)
    place = jnp.where(index < half, first_keep + index, first_send + index - half)
    inside = (place >= 0) & (place < coarse_height)
    for j in range(cols // (2 * BLOCK)):
        at = LANES + 2 * BLOCK * j
        high = bvh[:, at : at + 2 * BLOCK]
        low = bvl[:, at : at + 2 * BLOCK]
        edge = edge_columns(bvh, bvl, at, 2 * BLOCK)
        value = mm(high, dc_ref[...]) + mm(low, dc_ref[...]) + mm(high, dl_ref[...]) + mm(edge, de_ref[...])
        value = jnp.where(inside, value, 0.0)
        keep_ref[:, j * BLOCK : (j + 1) * BLOCK] = value[:half]
        send_ref[:, j * BLOCK : (j + 1) * BLOCK] = value[half:]


def filter_columns(vh, vl, w_refs, group, rows, cols, lev, diffs, gains, dog_ref, hess_ref, seam, border):
    wc_ref, wl_ref, we_ref = w_refs
    tall = rows + 2 * PAD
    tiles = group * BLOCK // LANES
    for s in range(LEVELS):
        k = s - 1
        for g in range(0, cols // BLOCK, group):
            ats = [LANES + BLOCK * (g + i) for i in range(group)]
            high = jnp.concatenate([vh[s, :, at : at + BLOCK] for at in ats], axis=0)
            low = jnp.concatenate([vl[s, :, at : at + BLOCK] for at in ats], axis=0)
            edge = jnp.concatenate([edge_columns(vh.at[s], vl.at[s], at, BLOCK) for at in ats], axis=0)
            value = mm(high, wc_ref[s]) + mm(low, wc_ref[s]) + mm(high, wl_ref[s]) + mm(edge, we_ref[s])
            for i, at in enumerate(ats):
                new = value[i * tall : (i + 1) * tall]
                if s > 0:
                    d = new - lev[:, at : at + BLOCK]
                    dog_ref[k, :, at - LANES : at - LANES + BLOCK] = (gains[0] * d[PAD : PAD + rows]).astype(BF16)
                    if k in diffs:
                        diffs[k][:, at : at + BLOCK] = d
                if s + 1 < LEVELS:
                    lev[:, at : at + BLOCK] = new
            m = s - 3
            if m >= 0:

                def put(t, value):
                    hess_ref[m, :, t * LANES : (t + 1) * LANES] = value

                hess_tiles(diffs[m + 1], rows, g * BLOCK // LANES, tiles, gains[1], put)
        if s in (1, 2, 3):
            seam(s)
        if k in diffs:
            d = diffs[k]
            d[:PAD, :] = jnp.where(border[0], 0.0, d[:PAD, :])
            d[PAD + rows :, :] = jnp.where(border[1], 0.0, d[PAD + rows :, :])


def fine_kernel(place_ref, own_ref, top_ref, bot_ref, lh_ref, wc_ref, wl_ref, we_ref,
                dog_ref, hess_ref, vh, vl, lev, d1, d2):
    _, rows, cols = dog_ref.shape
    row, col, last_row = place_ref[0], place_ref[1], place_ref[2]
    tall = rows + 2 * PAD
    diffs = {1: d1, 2: d2}
    is_left = col == 0
    near = 2 * NEAR

    def rows_of(at, width):
        part = slice(at, at + width)
        own = own_ref[:, part]
        top_near, bot_near = top_ref[:near, part], bot_ref[:near, part]
        lows = jnp.concatenate([bot_ref[2 * near : FAR, part], top_ref[FAR:, part]], axis=0)
        again = jnp.concatenate([bot_near[:NEAR], top_near[NEAR:]], axis=0)
        stack = jnp.concatenate([own, own[:rows], top_near, bot_near, lows, again], axis=0)
        return mm(lh_ref[...], stack)

    for at in range(0, cols, BLOCK):
        value = rows_of(at, BLOCK)
        to = slice(LANES + at, LANES + at + BLOCK)
        for s in range(LEVELS):
            vh[s, :, to], vl[s, :, to] = split(value[s * tall : (s + 1) * tall])
    value = rows_of(cols, LANES)
    for s in range(LEVELS):
        part = value[s * tall : (s + 1) * tall]
        left = slice(0, LANES)
        right = slice(LANES + cols, 2 * LANES + cols)
        vh[s, :, left], vl[s, :, left] = split(jnp.where(is_left, 0.0, part))
        vh[s, :, right], vl[s, :, right] = split(jnp.where(is_left, part, 0.0))

    start = pl.multiple_of(jnp.where(is_left, cols, 0), LANES)

    def seam(s):
        high = vh[s, :, pl.ds(start, BLOCK)]
        low = vl[s, :, pl.ds(start, BLOCK)]
        new = mm(high, wc_ref[s]) + mm(low, wc_ref[s]) + mm(high, wl_ref[s])
        if s > 1:
            d = new - lev[:, cols + 2 * LANES :]
            diffs[s - 1][:, :LANES] = jnp.where(is_left, 0.0, d[:, :LANES])
            diffs[s - 1][:, cols + LANES :] = jnp.where(is_left, d[:, LANES:], 0.0)
        lev[:, cols + 2 * LANES :] = new

    filter_columns(vh, vl, (wc_ref, wl_ref, we_ref), 4, rows, cols, lev, diffs, (20.0, 5000.0),
                   dog_ref, hess_ref, seam, (row == 0, row == last_row))


def coarse_kernel(place_ref, keep_ref, other_ref, fine_dog_ref, fine_hess_ref, lh_ref, wc_ref, wl_ref, we_ref,
                  fine_dog_hbm, fine_hess_hbm, dog_hbm, hess_hbm,
                  dog_ref, hess_ref, vh, vl, lev, d1, d2, sems):
    fine_copies = [
        pltpu.make_async_copy(fine_dog_ref, fine_dog_hbm, sems.at[0]),
        pltpu.make_async_copy(fine_hess_ref, fine_hess_hbm, sems.at[1]),
    ]
    for copy in fine_copies:
        copy.start()
    _, rows, cols = dog_ref.shape
    row, col, last_row = place_ref[0], place_ref[1], place_ref[2]
    tall = rows + 2 * PAD
    diffs = {1: d1, 2: d2}
    is_left = col == 0
    half = cols // 2
    zero = jnp.zeros((tall, LANES), BF16)
    for s in range(LEVELS):
        for ref in (vh, vl):
            ref[s, :, :LANES] = zero
            ref[s, :, LANES + cols :] = zero
    zero = jnp.zeros((tall, LANES), F32)
    for d in (d1, d2):
        d[:, :LANES] = zero
        d[:, LANES + cols :] = zero

    for at in range(0, cols, BLOCK):
        source = slice(at % half, at % half + BLOCK)
        first = is_left if at < half else jnp.logical_not(is_left)
        high, low = split(jnp.where(first, keep_ref[:, source], other_ref[:, source]))
        stack = jnp.concatenate([high, low, high], axis=0)
        value = mm(lh_ref[...], stack)
        to = slice(LANES + at, LANES + at + BLOCK)
        for s in range(LEVELS):
            vh[s, :, to], vl[s, :, to] = split(value[s * tall : (s + 1) * tall])

    filter_columns(vh, vl, (wc_ref, wl_ref, we_ref), 8, rows, cols, lev, diffs, (80.0, 200000.0),
                   dog_ref, hess_ref, lambda s: None,
                   ((row == 0) & (col == 0), (row == last_row) & (col == 1)))
    copies = [
        pltpu.make_async_copy(dog_ref, dog_hbm, sems.at[2]),
        pltpu.make_async_copy(hess_ref, hess_hbm, sems.at[3]),
    ]
    for copy in copies:
        copy.start()
    for copy in fine_copies + copies:
        copy.wait()


def fine_constants(rows):
    near = 2 * NEAR
    own = np.arange(rows)
    top = np.concatenate([np.arange(-near, 0), np.arange(-FAR, -near)])
    bot = rows + np.arange(FAR)
    inputs = np.concatenate([own, own, top, np.arange(-NEAR, 0), bot[: 2 * near], bot[:NEAR], bot[2 * near :]])
    is_high = np.ones(inputs.shape)
    is_high[rows : 2 * rows] = 0
    is_high[2 * rows + FAR : 2 * rows + FAR + NEAR] = 0
    is_high[2 * rows + FAR + NEAR + 2 * near : 2 * rows + FAR + NEAR + FAR] = 0
    low_part = np.zeros(rows * 3 + 2 * near + 2 * near, bool)
    low_part[2 * rows : 3 * rows] = True
    low_part[3 * rows + 3 * near :] = True
    near_inputs = np.concatenate(
        [own, own, own, top[:near], bot[:near], bot[:NEAR], top[NEAR:near], bot[:NEAR], top[NEAR:near]]
    )

    def level_matrix(sigma, centres, valid):
        high, low = two_parts(row_matrix(sigma, centres, near_inputs) * valid[:, None])
        return np.where(low_part[None, :], low.astype(np.float32), high.astype(np.float32)).astype(BF16)

    def matrices(sigma, centres, valid):
        high, low = two_parts(row_matrix(sigma, centres, inputs) * valid[:, None])
        return high, (low.astype(np.float32) * is_high[None, :]).astype(BF16)

    centres = np.arange(-PAD, rows + PAD)
    valid = ((centres >= -1) & (centres <= rows)).astype(np.float32)
    level = [level_matrix(s, centres, valid) for s in SIGMAS]
    strip = rows // 4
    count = strip + 2 * (REACH + 1)
    padded = -(-count // 16) * 16
    ok = (np.arange(padded) < count).astype(np.float32)
    base = []
    for core in range(2):
        both = [2 * (c * strip - REACH - 1 + np.arange(padded)) for c in (core, 1 - core)]
        base.append(matrices(SIGMAS[-1], np.concatenate(both), np.concatenate([ok, ok])))
    return (
        np.concatenate(level),
        np.stack([a for a, _ in base]),
        np.stack([b for _, b in base]),
        padded,
    )


def coarse_constants(strip, padded):
    inputs = np.arange(padded) - REACH - 1
    centres = np.arange(-PAD, strip + PAD)
    valid = ((centres >= -1) & (centres <= strip)).astype(np.float32)
    parts = []
    for s in SIGMAS:
        high, low = two_parts(row_matrix(s, centres, inputs) * valid[:, None])
        parts.append(np.concatenate([high, high, low], axis=1))
    return np.concatenate(parts)


def vmem_specs(count):
    return [pl.BlockSpec(memory_space=pltpu.VMEM) for _ in range(count)]


def far_specs(count):
    return [pl.BlockSpec(memory_space=pltpu.HBM) for _ in range(count)]


def limit(mib):
    return pltpu.CompilerParams(vmem_limit_bytes=mib * 2**20)


def like(value):
    return jax.ShapeDtypeStruct(value.shape, value.dtype)


def local(image):
    rows, cols = image.shape
    row_count = lax.axis_size("row")
    row = lax.axis_index("row")
    col = lax.axis_index("col")
    strip = rows // 4
    wide = cols + LANES
    tall = rows + 2 * PAD
    small = strip + 2 * PAD
    lh, bh, bl, padded = fine_constants(rows)
    cw = coarse_constants(strip, padded)
    bands = [column_weights(s, 1) for s in SIGMAS]
    wc, wl, we = (np.stack([b[i] for b in bands]) for i in range(3))
    dc, dl, de = column_weights(SIGMAS[-1], 2)
    place = jnp.stack([row, col, jnp.int32(row_count - 1), jnp.int32(row_count * rows // 2)]).astype(jnp.int32)
    smem = pl.BlockSpec(memory_space=pltpu.SMEM)

    side = jnp.where(col == 0, image[:, cols - LANES :], image[:, :LANES])
    side = lax.ppermute(side, "col", [(0, 1), (1, 0)])
    packed = (
        jax.ShapeDtypeStruct((2 * rows, wide), BF16),
        jax.ShapeDtypeStruct((FAR + NEAR, wide), BF16),
        jax.ShapeDtypeStruct((FAR + NEAR, wide), BF16),
    )
    own, up, down = pl.pallas_call(
        pack_kernel,
        out_shape=packed,
        in_specs=far_specs(1),
        out_specs=tuple(vmem_specs(3)),
        scratch_shapes=[pltpu.VMEM((rows, cols), F32), pltpu.SemaphoreType.DMA],
        compiler_params=limit(4),
        name="pack",
    )(pltpu.with_memory_space_constraint(image, pltpu.HBM))
    own, up, down = pl.pallas_call(
        side_kernel,
        out_shape=packed,
        in_specs=vmem_specs(4),
        out_specs=tuple(vmem_specs(3)),
        input_output_aliases={1: 0, 2: 1, 3: 2},
        compiler_params=limit(4),
        name="side",
    )(side, own, up, down)
    bot = lax.ppermute(up, "row", [(i + 1, i) for i in range(row_count - 1)])
    top = lax.ppermute(down, "row", [(i, i + 1) for i in range(row_count - 1)])

    constants = [pltpu.with_memory_space_constraint(jnp.asarray(c), pltpu.HBM) for c in (lh, bh, bl, wc, wl, we, dc, dl, de, cw)]
    lh, bh, bl, wc, wl, we, dc, dl, de, cw = pl.pallas_call(
        stage_kernel,
        out_shape=tuple(like(c) for c in constants),
        in_specs=far_specs(len(constants)),
        out_specs=tuple(vmem_specs(len(constants))),
        scratch_shapes=[pltpu.SemaphoreType.DMA((len(constants),))],
        compiler_params=limit(8),
        name="stage",
    )(*constants)

    keep, send = pl.pallas_call(
        base_kernel,
        out_shape=(
            jax.ShapeDtypeStruct((padded, cols // 2), F32),
            jax.ShapeDtypeStruct((padded, cols // 2), F32),
        ),
        in_specs=[smem] + vmem_specs(8),
        out_specs=tuple(vmem_specs(2)),
        scratch_shapes=[
            pltpu.VMEM((2 * padded, cols + 2 * LANES), BF16),
            pltpu.VMEM((2 * padded, cols + 2 * LANES), BF16),
        ],
        compiler_params=limit(8),
        name="base",
    )(place, own, top, bot, bh, bl, dc, dl, de)
    other = lax.ppermute(send, "col", [(0, 1), (1, 0)])
    fine_shapes = (
        jax.ShapeDtypeStruct((4, rows, cols), BF16),
        jax.ShapeDtypeStruct((2, rows, cols), BF16),
    )
    coarse_shapes = (
        jax.ShapeDtypeStruct((4, strip, cols), BF16),
        jax.ShapeDtypeStruct((2, strip, cols), BF16),
    )
    dog_fine, hess_fine = pl.pallas_call(
        fine_kernel,
        out_shape=fine_shapes,
        in_specs=[smem] + vmem_specs(7),
        out_specs=tuple(vmem_specs(2)),
        scratch_shapes=[
            pltpu.VMEM((LEVELS, tall, cols + 2 * LANES), BF16),
            pltpu.VMEM((LEVELS, tall, cols + 2 * LANES), BF16),
            pltpu.VMEM((tall, cols + 2 * LANES + BLOCK), F32),
            pltpu.VMEM((tall, cols + 2 * LANES), F32),
            pltpu.VMEM((tall, cols + 2 * LANES), F32),
        ],
        compiler_params=limit(16),
        name="fine",
    )(place, own, top, bot, lh, wc, wl, we)

    return pl.pallas_call(
        coarse_kernel,
        out_shape=fine_shapes + coarse_shapes,
        in_specs=[smem] + vmem_specs(8),
        out_specs=tuple(far_specs(4)),
        scratch_shapes=[
            pltpu.VMEM((4, strip, cols), BF16),
            pltpu.VMEM((2, strip, cols), BF16),
            pltpu.VMEM((LEVELS, small, cols + 2 * LANES), BF16),
            pltpu.VMEM((LEVELS, small, cols + 2 * LANES), BF16),
            pltpu.VMEM((small, cols + 2 * LANES), F32),
            pltpu.VMEM((small, cols + 2 * LANES), F32),
            pltpu.VMEM((small, cols + 2 * LANES), F32),
            pltpu.SemaphoreType.DMA((4,)),
        ],
        compiler_params=limit(12),
        name="coarse",
    )(place, keep, other, dog_fine, hess_fine, cw, wc, wl, we)


def solution(mesh):
    return jax.shard_map(
        local,
        mesh=mesh,
        in_specs=(P(("slab", "row"), "col"),),
        out_specs=(
            P(None, ("slab", "row"), "col"),
            P(None, ("slab", "row"), "col"),
            P(None, ("slab", "row", "col"), None),
            P(None, ("slab", "row", "col"), None),
        ),
        check_vma=False,
    )
```

```python
import functools

import jax
import jax.numpy as jnp
import numpy as np
from jax import lax
from jax.experimental import pallas as pl
from jax.experimental.pallas import tpu as pltpu
from jax.sharding import PartitionSpec as P

SIGMAS = [1.6 * 2.0 ** (k / 4.0) for k in range(5)]
LEVELS = len(SIGMAS)
REACH = 12
LANES = 128
BLOCK = 256
PAD = 8
NEAR = 16
LOW = 4
SPAN = 19
PART = 10
FINE = 4
BF16 = jnp.bfloat16
F32 = jnp.float32


def taps(sigma):
    offset = np.arange(2 * REACH + 1, dtype=np.float64) - REACH
    weights = np.exp(-offset * offset / (2.0 * sigma * sigma))
    return (weights / weights.sum()).astype(np.float32)


def two_parts(matrix):
    high = np.asarray(matrix, np.float32).astype(BF16)
    low = (np.asarray(matrix, np.float32) - high.astype(np.float32)).astype(BF16)
    return high, low


def tap_at(sigma, index):
    weights = taps(sigma)
    inside = (index >= 0) & (index <= 2 * REACH)
    return np.where(inside, weights[np.clip(index, 0, 2 * REACH)], np.float32(0.0))


def row_matrix(sigma, centres, inputs):
    return tap_at(sigma, inputs[None, :] - centres[:, None] + REACH)


def column_weights(sigma, step):
    width = BLOCK * step
    out = np.arange(BLOCK)[None, :] * step
    high, low = two_parts(tap_at(sigma, np.arange(width)[:, None] - out + REACH))
    lane = np.arange(LANES)[:, None]
    right = np.where(lane < REACH, tap_at(sigma, width + lane - out + REACH), 0.0)
    left = np.where(lane >= LANES - REACH, tap_at(sigma, lane - LANES - out + REACH), 0.0)
    edge_high, edge_low = two_parts(right + left)
    edge = np.concatenate([edge_high.astype(np.float32), edge_high.astype(np.float32)])
    edge[:LANES] += np.roll(edge_low.astype(np.float32), 32, axis=0)
    return high, low, edge.astype(BF16)


def split(value):
    high = value.astype(BF16)
    low = (value - high.astype(F32)).astype(BF16)
    return high, low


def mm(a, b):
    return jnp.dot(a, b, preferred_element_type=F32)


def edge_columns(high, low, at, width):
    def both(ref):
        left = ref[:, at - LANES : at].astype(F32)
        right = ref[:, at + width : at + width + LANES].astype(F32)
        lane = lax.broadcasted_iota(jnp.int32, left.shape, 1)
        return jnp.where(lane < LANES // 2, right, left), lane

    eh, lane = both(high)
    el, _ = both(low)
    again = pltpu.roll(eh, 32, 1)
    eh = jnp.where((lane >= 16) & (lane < 64), again, eh)
    return jnp.concatenate([eh.astype(BF16), el.astype(BF16)], axis=1)


def hess_tiles(d, rows, first_tile, count, gain, put):
    tall = rows + 2 * PAD
    lane = lax.broadcasted_iota(jnp.int32, (tall, LANES), 1)
    tile = lambda t: d[:, (first_tile + t + 1) * LANES : (first_tile + t + 2) * LANES]
    tiles = {-1: tile(-1), 0: tile(0)}
    back = {t: pltpu.roll(tiles[t], 1, 1) for t in (-1, 0)}
    ahead = {0: pltpu.roll(tiles[0], LANES - 1, 1)}
    for t in range(count):
        tiles[t + 1] = tile(t + 1)
        back[t + 1] = pltpu.roll(tiles[t + 1], 1, 1)
        ahead[t + 1] = pltpu.roll(tiles[t + 1], LANES - 1, 1)
        before = jnp.where(lane == 0, back[t - 1], back[t])
        after = jnp.where(lane == LANES - 1, ahead[t + 1], ahead[t])
        across = after - before
        mid = slice(PAD, PAD + rows)
        up, down = pltpu.roll(tiles[t], 1, 0)[mid], pltpu.roll(tiles[t], tall - 1, 0)[mid]
        twice = 2.0 * tiles[t][mid]
        dxx = after[mid] + before[mid] - twice
        dyy = up + down - twice
        dxy = (pltpu.roll(across, tall - 1, 0)[mid] - pltpu.roll(across, 1, 0)[mid]) * 0.25
        put(first_tile + t, (gain * (dxx * dyy - dxy * dxy)).astype(BF16))


def mesh_place():
    return lax.axis_index("row"), lax.axis_index("col")


def pack_kernel(x_hbm, *refs):
    count = (len(refs) - 3) // 2
    far, own_ref, near, x_ref, sems = refs[:count], refs[count], refs[count + 1 : -2], refs[-2], refs[-1]
    copies = [pltpu.make_async_copy(x_hbm, x_ref, sems.at[0])]
    copies += [pltpu.make_async_copy(f, n, sems.at[i + 1]) for i, (f, n) in enumerate(zip(far, near))]
    for copy in copies:
        copy.start()
    copies[0].wait()
    rows, cols = x_ref.shape
    for at in range(0, cols, BLOCK):
        to = slice(at, at + BLOCK)
        own_ref[:rows, to], own_ref[rows:, to] = split(x_ref[:, to])
    for copy in copies[1:]:
        copy.wait()


def send_kernel(side_ref, own_in, bm_ref, dc_ref, dl_ref, de_ref,
                own_ref, even_ref, odd_ref, base_ref, bvh, bvl):
    row, col = mesh_place()
    rows = own_ref.shape[0] // 2
    cols = own_ref.shape[1] - LANES
    is_left = col == 0
    even = row % 2 == 0
    own_ref[:rows, cols:], own_ref[rows:, cols:] = split(side_ref[...])

    def rows_of(part):
        own = own_ref[:, part]
        return mm(bm_ref[...], jnp.concatenate([own, own[:rows]], axis=0))

    for at in range(0, cols, BLOCK):
        to = slice(LANES + at, LANES + at + BLOCK)
        bvh[:, to], bvl[:, to] = split(rows_of(slice(at, at + BLOCK)))
    value = rows_of(slice(cols, cols + LANES))
    bvh[:, :LANES], bvl[:, :LANES] = split(jnp.where(is_left, 0.0, value))
    bvh[:, LANES + cols :], bvl[:, LANES + cols :] = split(jnp.where(is_left, value, 0.0))
    for j in range(cols // (2 * BLOCK)):
        at = LANES + 2 * BLOCK * j
        high = bvh[:, at : at + 2 * BLOCK]
        low = bvl[:, at : at + 2 * BLOCK]
        edge = edge_columns(bvh, bvl, at, 2 * BLOCK)
        base_ref[:, j * BLOCK : (j + 1) * BLOCK] = (
            mm(high, dc_ref[...]) + mm(low, dc_ref[...]) + mm(high, dl_ref[...]) + mm(edge, de_ref[...])
        )

    half = cols // 2
    first_up = REACH + 1 - 6
    first_down = REACH + 1 + SPAN
    for at in range(0, cols + LANES, LANES):
        to = slice(at, at + LANES)
        up_near, down_near = own_ref[:NEAR, to].astype(F32), own_ref[rows - NEAR : rows, to].astype(F32)
        up_low = own_ref[rows : rows + NEAR, to].astype(F32)[:LOW]
        down_low = own_ref[2 * rows - NEAR :, to].astype(F32)[NEAR - LOW :]
        if at < cols:
            lanes = slice(at % half, at % half + LANES)
            skip = PART * (at // half)
            up_part = base_ref[first_up + skip : first_up + skip + PART, lanes]
            down_part = base_ref[first_down + skip : first_down + skip + PART, lanes]
            skip = FINE // 2 * (at // half)

            def low_of(start):
                value = base_ref[start + skip : start + skip + FINE // 2, lanes]
                return value - value.astype(BF16).astype(F32)

            up_fine = low_of(first_up + SPAN - 13)
            down_fine = low_of(first_down + 13 - FINE)
        else:
            up_part = down_part = jnp.zeros((PART, LANES), F32)
            up_fine = down_fine = jnp.zeros((FINE // 2, LANES), F32)
        up = jnp.concatenate([up_near, up_low, up_fine, up_part], axis=0)
        down = jnp.concatenate([down_near, down_part, down_fine, down_low], axis=0)
        even_ref[:, to] = jnp.where(even, down, up).astype(BF16)
        odd_ref[:, to] = jnp.where(even, up, down).astype(BF16)


def stage_kernel(*refs):
    count = (len(refs) - 1) // 2
    sems = refs[-1]
    copies = [pltpu.make_async_copy(refs[i], refs[count + i], sems.at[i]) for i in range(count)]
    for copy in copies:
        copy.start()
    for copy in copies:
        copy.wait()


def base_kernel(row_count, tile_base, base_ref, even_ref, odd_ref, _, keep_ref, send_ref, sum_ref):
    row, col = mesh_place()
    base_rows, half = base_ref.shape
    count = keep_ref.shape[0]
    shift = tile_base // 2
    even = row % 2 == 0
    is_left = col == 0
    index = lax.broadcasted_iota(jnp.int32, (base_rows, LANES), 0)
    place = row * tile_base - REACH - 1 + index
    inside = (place >= 0) & (place < row_count * tile_base)
    first_bot = tile_base + REACH + 1 - 6
    for at in range(0, half, LANES):
        def message(ref_a, ref_b):
            both = []
            for lanes in (slice(at, at + LANES), slice(half + at, half + at + LANES)):
                a, b = ref_a[NEAR:, lanes].astype(F32), ref_b[NEAR:, lanes].astype(F32)
                both.append(jnp.where(even, a, b))
            return both

        to = slice(at, at + LANES)
        left, right = message(odd_ref, even_ref)
        top = jnp.concatenate([left[:PART], right[: SPAN - PART]], axis=0)
        top_fine = jnp.concatenate([left[PART : PART + FINE // 2], right[PART : PART + FINE // 2]], axis=0)
        left, right = message(even_ref, odd_ref)
        skip = LOW + FINE // 2
        bot = jnp.concatenate([left[skip:], right[skip : skip + SPAN - PART]], axis=0)
        bot_fine = jnp.concatenate([left[LOW:skip], right[LOW:skip]], axis=0)
        sum_ref[...] = base_ref[:, to]
        sum_ref[:SPAN, :] += top
        sum_ref[13 - FINE : 13, :] += top_fine
        sum_ref[first_bot : first_bot + SPAN, :] += bot
        first_fine = first_bot + SPAN - 13
        sum_ref[first_fine : first_fine + FINE, :] += bot_fine
        total = jnp.where(inside, sum_ref[...], 0.0)
        keep_ref[:, to] = jnp.where(is_left, total[:count], total[shift : shift + count])
        send_ref[:, to] = jnp.where(is_left, total[shift : shift + count], total[:count])


def filter_columns(vh, vl, w_refs, group, rows, cols, lev, diffs, gains, dog_ref, hess_ref, seam, border):
    wc_ref, wl_ref, we_ref = w_refs
    tall = rows + 2 * PAD
    tiles = group * BLOCK // LANES
    for s in range(LEVELS):
        k = s - 1
        for g in range(0, cols // BLOCK, group):
            ats = [LANES + BLOCK * (g + i) for i in range(group)]
            high = jnp.concatenate([vh[s, :, at : at + BLOCK] for at in ats], axis=0)
            low = jnp.concatenate([vl[s, :, at : at + BLOCK] for at in ats], axis=0)
            edge = jnp.concatenate([edge_columns(vh.at[s], vl.at[s], at, BLOCK) for at in ats], axis=0)
            value = mm(high, wc_ref[s]) + mm(low, wc_ref[s]) + mm(high, wl_ref[s]) + mm(edge, we_ref[s])
            for i, at in enumerate(ats):
                new = value[i * tall : (i + 1) * tall]
                if s > 0:
                    d = new - lev[:, at : at + BLOCK]
                    dog_ref[k, :, at - LANES : at - LANES + BLOCK] = (gains[0] * d[PAD : PAD + rows]).astype(BF16)
                    if k in diffs:
                        diffs[k][:, at : at + BLOCK] = d
                if s + 1 < LEVELS:
                    lev[:, at : at + BLOCK] = new
            m = s - 3
            if m >= 0:

                def put(t, value):
                    hess_ref[m, :, t * LANES : (t + 1) * LANES] = value

                hess_tiles(diffs[m + 1], rows, g * BLOCK // LANES, tiles, gains[1], put)
        if s in (1, 2, 3):
            seam(s)
        if k in diffs:
            d = diffs[k]
            d[:PAD, :] = jnp.where(border[0], 0.0, d[:PAD, :])
            d[PAD + rows :, :] = jnp.where(border[1], 0.0, d[PAD + rows :, :])


def fine_kernel(last_row, own_ref, even_ref, odd_ref, lh_ref, wc_ref, wl_ref, we_ref,
                dog_ref, hess_ref, vh, vl, lev, d1, d2):
    _, rows, cols = dog_ref.shape
    row, col = mesh_place()
    tall = rows + 2 * PAD
    diffs = {1: d1, 2: d2}
    is_left = col == 0
    even = row % 2 == 0

    def rows_of(at, width):
        part = slice(at, at + width)
        own = own_ref[:, part]
        a, b = even_ref[:, part], odd_ref[:, part]
        bot, top = jnp.where(even, a, b), jnp.where(even, b, a)
        lows = jnp.concatenate([bot[NEAR : NEAR + 8], top[NEAR + 8 :]], axis=0)
        again = jnp.concatenate([bot[:8], top[8:NEAR]], axis=0)
        stack = jnp.concatenate([own, own[:rows], top[:NEAR], bot[:NEAR], lows, again], axis=0)
        return mm(lh_ref[...], stack)

    for at in range(0, cols, BLOCK):
        value = rows_of(at, BLOCK)
        to = slice(LANES + at, LANES + at + BLOCK)
        for s in range(LEVELS):
            vh[s, :, to], vl[s, :, to] = split(value[s * tall : (s + 1) * tall])
    value = rows_of(cols, LANES)
    for s in range(LEVELS):
        part = value[s * tall : (s + 1) * tall]
        left = slice(0, LANES)
        right = slice(LANES + cols, 2 * LANES + cols)
        vh[s, :, left], vl[s, :, left] = split(jnp.where(is_left, 0.0, part))
        vh[s, :, right], vl[s, :, right] = split(jnp.where(is_left, part, 0.0))

    start = pl.multiple_of(jnp.where(is_left, cols, 0), LANES)

    def seam(s):
        high = vh[s, :, pl.ds(start, BLOCK)]
        low = vl[s, :, pl.ds(start, BLOCK)]
        new = mm(high, wc_ref[s]) + mm(low, wc_ref[s]) + mm(high, wl_ref[s])
        if s > 1:
            d = new - lev[:, cols + 2 * LANES :]
            diffs[s - 1][:, :LANES] = jnp.where(is_left, 0.0, d[:, :LANES])
            diffs[s - 1][:, cols + LANES :] = jnp.where(is_left, d[:, LANES:], 0.0)
        lev[:, cols + 2 * LANES :] = new

    filter_columns(vh, vl, (wc_ref, wl_ref, we_ref), 4, rows, cols, lev, diffs, (20.0, 5000.0),
                   dog_ref, hess_ref, seam, (row == 0, row == last_row))


def coarse_kernel(last_row, keep_ref, other_ref, fine_dog_ref, fine_hess_ref, lh_ref, wc_ref, wl_ref, we_ref,
                  fine_dog_hbm, fine_hess_hbm, dog_hbm, hess_hbm,
                  dog_ref, hess_ref, vh, vl, lev, d1, d2, sems):
    fine_copies = [
        pltpu.make_async_copy(fine_dog_ref, fine_dog_hbm, sems.at[0]),
        pltpu.make_async_copy(fine_hess_ref, fine_hess_hbm, sems.at[1]),
    ]
    for copy in fine_copies:
        copy.start()
    _, rows, cols = dog_ref.shape
    row, col = mesh_place()
    tall = rows + 2 * PAD
    diffs = {1: d1, 2: d2}
    is_left = col == 0
    half = cols // 2
    zero = jnp.zeros((tall, LANES), BF16)
    for s in range(LEVELS):
        for ref in (vh, vl):
            ref[s, :, :LANES] = zero
            ref[s, :, LANES + cols :] = zero
    zero = jnp.zeros((tall, LANES), F32)
    for d in (d1, d2):
        d[:, :LANES] = zero
        d[:, LANES + cols :] = zero

    for at in range(0, cols, BLOCK):
        source = slice(at % half, at % half + BLOCK)
        first = is_left if at < half else jnp.logical_not(is_left)
        high, low = split(jnp.where(first, keep_ref[:, source], other_ref[:, source]))
        stack = jnp.concatenate([high, low, high], axis=0)
        value = mm(lh_ref[...], stack)
        to = slice(LANES + at, LANES + at + BLOCK)
        for s in range(LEVELS):
            vh[s, :, to], vl[s, :, to] = split(value[s * tall : (s + 1) * tall])

    filter_columns(vh, vl, (wc_ref, wl_ref, we_ref), 8, rows, cols, lev, diffs, (80.0, 200000.0),
                   dog_ref, hess_ref, lambda s: None,
                   ((row == 0) & (col == 0), (row == last_row) & (col == 1)))
    copies = [
        pltpu.make_async_copy(dog_ref, dog_hbm, sems.at[2]),
        pltpu.make_async_copy(hess_ref, hess_hbm, sems.at[3]),
    ]
    for copy in copies:
        copy.start()
    for copy in fine_copies + copies:
        copy.wait()


def fine_constants(rows):
    own = np.arange(rows)
    top, bot = np.arange(-NEAR, 0), rows + np.arange(NEAR)
    nowhere = -1000
    lows = np.full(NEAR, nowhere)
    lows[:LOW] = bot[:LOW]
    lows[NEAR - LOW :] = top[NEAR - LOW :]
    again = np.concatenate([bot[:8], top[8:]])
    inputs = np.concatenate([own, own, own, top, bot, lows, again])
    use_low = np.zeros(inputs.shape, bool)
    use_low[2 * rows : 3 * rows] = True
    use_low[-NEAR:] = True

    def matrix(sigma, centres, valid, inputs, use_low):
        high, low = two_parts(row_matrix(sigma, centres, inputs) * valid[:, None])
        return np.where(use_low[None, :], low.astype(np.float32), high.astype(np.float32)).astype(BF16)

    centres = np.arange(-PAD, rows + PAD)
    valid = ((centres >= -1) & (centres <= rows)).astype(np.float32)
    level = [matrix(s, centres, valid, inputs, use_low) for s in SIGMAS]
    count = rows // 2 + 2 * (REACH + 1)
    index = np.arange(-(-count // 8) * 8)
    base = matrix(
        SIGMAS[-1], 2 * (index - REACH - 1), (index < count).astype(np.float32), inputs[: 3 * rows], use_low[: 3 * rows]
    )
    strip_rows = -(-(rows // 4 + 2 * (REACH + 1)) // 16) * 16
    return np.concatenate(level), base, strip_rows


def coarse_constants(strip, padded):
    inputs = np.arange(padded) - REACH - 1
    centres = np.arange(-PAD, strip + PAD)
    valid = ((centres >= -1) & (centres <= strip)).astype(np.float32)
    parts = []
    for s in SIGMAS:
        high, low = two_parts(row_matrix(s, centres, inputs) * valid[:, None])
        parts.append(np.concatenate([high, high, low], axis=1))
    return np.concatenate(parts)


def vmem_specs(count):
    return [pl.BlockSpec(memory_space=pltpu.VMEM) for _ in range(count)]


def far_specs(count):
    return [pl.BlockSpec(memory_space=pltpu.HBM) for _ in range(count)]


def limit(mib):
    return pltpu.CompilerParams(vmem_limit_bytes=mib * 2**20)


def like(value):
    return jax.ShapeDtypeStruct(value.shape, value.dtype)


def far(value):
    return pltpu.with_memory_space_constraint(jnp.asarray(value), pltpu.HBM)


def local(image):
    rows, cols = image.shape
    row_count = lax.axis_size("row")
    col = lax.axis_index("col")
    strip = rows // 4
    wide = cols + LANES
    tall = rows + 2 * PAD
    small = strip + 2 * PAD
    lh, bm, strip_rows = fine_constants(rows)
    cw = coarse_constants(strip, strip_rows)
    bands = [column_weights(s, 1) for s in SIGMAS]
    wc, wl, we = (np.stack([b[i] for b in bands]) for i in range(3))
    early = [far(c) for c in (bm, *column_weights(SIGMAS[-1], 2))]
    late = [far(c) for c in (lh, wc, wl, we, cw)]

    side = jnp.where(col == 0, image[:, cols - LANES :], image[:, :LANES])
    side = lax.ppermute(side, "col", [(0, 1), (1, 0)])
    own, bm, dc, dl, de = pl.pallas_call(
        pack_kernel,
        out_shape=(jax.ShapeDtypeStruct((2 * rows, wide), BF16), *(like(c) for c in early)),
        in_specs=far_specs(1 + len(early)),
        out_specs=tuple(vmem_specs(1 + len(early))),
        scratch_shapes=[pltpu.VMEM((rows, cols), F32), pltpu.SemaphoreType.DMA((1 + len(early),))],
        compiler_params=limit(4),
        name="pack",
    )(far(image), *early)
    message = jax.ShapeDtypeStruct((2 * NEAR, wide), BF16)
    base_rows = bm.shape[0]
    own, to_even, to_odd, base = pl.pallas_call(
        send_kernel,
        out_shape=(
            jax.ShapeDtypeStruct((2 * rows, wide), BF16),
            message,
            message,
            jax.ShapeDtypeStruct((base_rows, cols // 2), F32),
        ),
        in_specs=vmem_specs(6),
        out_specs=tuple(vmem_specs(4)),
        scratch_shapes=[
            pltpu.VMEM((base_rows, cols + 2 * LANES), BF16),
            pltpu.VMEM((base_rows, cols + 2 * LANES), BF16),
        ],
        input_output_aliases={1: 0},
        compiler_params=limit(6),
        name="send",
    )(side, own, bm, dc, dl, de)

    def swap(value, first):
        pairs = [(i, i + 1) for i in range(first, row_count - 1, 2)]
        return lax.ppermute(value, "row", pairs + [(j, i) for i, j in pairs])

    even, odd = swap(to_even, 0), swap(to_odd, 1)

    lh, wc, wl, we, cw = pl.pallas_call(
        stage_kernel,
        out_shape=tuple(like(c) for c in late),
        in_specs=far_specs(len(late)),
        out_specs=tuple(vmem_specs(len(late))),
        scratch_shapes=[pltpu.SemaphoreType.DMA((len(late),))],
        compiler_params=limit(6),
        cost_estimate=pl.CostEstimate(flops=10**8, bytes_accessed=10**7, transcendentals=0),
        name="stage",
    )(*late)

    keep, send = pl.pallas_call(
        functools.partial(base_kernel, row_count, rows // 2),
        out_shape=(
            jax.ShapeDtypeStruct((strip_rows, cols // 2), F32),
            jax.ShapeDtypeStruct((strip_rows, cols // 2), F32),
        ),
        in_specs=vmem_specs(3) + [pl.BlockSpec(memory_space=pl.ANY)],
        out_specs=tuple(vmem_specs(2)),
        scratch_shapes=[pltpu.VMEM((base_rows, LANES), F32)],
        compiler_params=limit(4),
        name="base",
    )(base, even, odd, cw)
    other = lax.ppermute(send, "col", [(0, 1), (1, 0)])
    fine_shapes = (
        jax.ShapeDtypeStruct((4, rows, cols), BF16),
        jax.ShapeDtypeStruct((2, rows, cols), BF16),
    )
    coarse_shapes = (
        jax.ShapeDtypeStruct((4, strip, cols), BF16),
        jax.ShapeDtypeStruct((2, strip, cols), BF16),
    )
    dog_fine, hess_fine = pl.pallas_call(
        functools.partial(fine_kernel, row_count - 1),
        out_shape=fine_shapes,
        in_specs=vmem_specs(7),
        out_specs=tuple(vmem_specs(2)),
        scratch_shapes=[
            pltpu.VMEM((LEVELS, tall, cols + 2 * LANES), BF16),
            pltpu.VMEM((LEVELS, tall, cols + 2 * LANES), BF16),
            pltpu.VMEM((tall, cols + 2 * LANES + BLOCK), F32),
            pltpu.VMEM((tall, cols + 2 * LANES), F32),
            pltpu.VMEM((tall, cols + 2 * LANES), F32),
        ],
        compiler_params=limit(16),
        name="fine",
    )(own, even, odd, lh, wc, wl, we)

    return pl.pallas_call(
        functools.partial(coarse_kernel, row_count - 1),
        out_shape=fine_shapes + coarse_shapes,
        in_specs=vmem_specs(8),
        out_specs=tuple(far_specs(4)),
        scratch_shapes=[
            pltpu.VMEM((4, strip, cols), BF16),
            pltpu.VMEM((2, strip, cols), BF16),
            pltpu.VMEM((LEVELS, small, cols + 2 * LANES), BF16),
            pltpu.VMEM((LEVELS, small, cols + 2 * LANES), BF16),
            pltpu.VMEM((small, cols + 2 * LANES), F32),
            pltpu.VMEM((small, cols + 2 * LANES), F32),
            pltpu.VMEM((small, cols + 2 * LANES), F32),
            pltpu.SemaphoreType.DMA((4,)),
        ],
        compiler_params=limit(12),
        name="coarse",
    )(keep, other, dog_fine, hess_fine, cw, wc, wl, we)


def solution(mesh):
    return jax.shard_map(
        local,
        mesh=mesh,
        in_specs=(P(("slab", "row"), "col"),),
        out_specs=(
            P(None, ("slab", "row"), "col"),
            P(None, ("slab", "row"), "col"),
            P(None, ("slab", "row", "col"), None),
            P(None, ("slab", "row", "col"), None),
        ),
        check_vma=False,
    )
```

```python
import functools

import jax
import jax.numpy as jnp
import numpy as np
from jax import lax
from jax.experimental import pallas as pl
from jax.experimental.pallas import tpu as pltpu
from jax.sharding import PartitionSpec as P

SIGMAS = [1.6 * 2.0 ** (k / 4.0) for k in range(5)]
LEVELS = len(SIGMAS)
REACH = 12
LANES = 128
BLOCK = 256
PAD = 8
RIM = 16
NEAR = 16
LOW = 4
SPAN = 19
PART = 10
FINE = 4
BF16 = jnp.bfloat16
F32 = jnp.float32


def taps(sigma):
    offset = np.arange(2 * REACH + 1, dtype=np.float64) - REACH
    weights = np.exp(-offset * offset / (2.0 * sigma * sigma))
    return (weights / weights.sum()).astype(np.float32)


def two_parts(matrix):
    high = np.asarray(matrix, np.float32).astype(BF16)
    low = (np.asarray(matrix, np.float32) - high.astype(np.float32)).astype(BF16)
    return high, low


def tap_at(sigma, index):
    weights = taps(sigma)
    inside = (index >= 0) & (index <= 2 * REACH)
    return np.where(inside, weights[np.clip(index, 0, 2 * REACH)], np.float32(0.0))


def row_matrix(sigma, centres, inputs):
    return tap_at(sigma, inputs[None, :] - centres[:, None] + REACH)


def column_weights(sigma, step):
    width = BLOCK * step
    out = np.arange(BLOCK)[None, :] * step
    high, low = two_parts(tap_at(sigma, np.arange(width)[:, None] - out + REACH))
    lane = np.arange(LANES)[:, None]
    right = np.where(lane < REACH, tap_at(sigma, width + lane - out + REACH), 0.0)
    left = np.where(lane >= LANES - REACH, tap_at(sigma, lane - LANES - out + REACH), 0.0)
    edge_high, edge_low = two_parts(right + left)
    edge = np.concatenate([edge_high.astype(np.float32), edge_high.astype(np.float32)])
    edge[:LANES] += np.roll(edge_low.astype(np.float32), 32, axis=0)
    return high, low, edge.astype(BF16)


def split(value):
    high = value.astype(BF16)
    low = (value - high.astype(F32)).astype(BF16)
    return high, low


def mm(a, b):
    return jnp.dot(a, b, preferred_element_type=F32)


def edge_columns(high, low, at, width):
    def both(ref):
        left = ref[:, at - LANES : at].astype(F32)
        right = ref[:, at + width : at + width + LANES].astype(F32)
        lane = lax.broadcasted_iota(jnp.int32, left.shape, 1)
        return jnp.where(lane < LANES // 2, right, left), lane

    eh, lane = both(high)
    el, _ = both(low)
    again = pltpu.roll(eh, 32, 1)
    eh = jnp.where((lane >= 16) & (lane < 64), again, eh)
    return jnp.concatenate([eh.astype(BF16), el.astype(BF16)], axis=1)


def hess_tiles(d, top, rows, first_tile, count, gain, put):
    tall = rows + 2 * PAD
    lane = lax.broadcasted_iota(jnp.int32, (tall, LANES), 1)
    tile = lambda t: d[top : top + tall, (first_tile + t + 1) * LANES : (first_tile + t + 2) * LANES]
    tiles = {-1: tile(-1), 0: tile(0)}
    back = {t: pltpu.roll(tiles[t], 1, 1) for t in (-1, 0)}
    ahead = {0: pltpu.roll(tiles[0], LANES - 1, 1)}
    for t in range(count):
        tiles[t + 1] = tile(t + 1)
        back[t + 1] = pltpu.roll(tiles[t + 1], 1, 1)
        ahead[t + 1] = pltpu.roll(tiles[t + 1], LANES - 1, 1)
        before = jnp.where(lane == 0, back[t - 1], back[t])
        after = jnp.where(lane == LANES - 1, ahead[t + 1], ahead[t])
        across = after - before
        mid = slice(PAD, PAD + rows)
        up, down = pltpu.roll(tiles[t], 1, 0)[mid], pltpu.roll(tiles[t], tall - 1, 0)[mid]
        twice = 2.0 * tiles[t][mid]
        dxx = after[mid] + before[mid] - twice
        dyy = up + down - twice
        dxy = (pltpu.roll(across, tall - 1, 0)[mid] - pltpu.roll(across, 1, 0)[mid]) * 0.25
        put(first_tile + t, (gain * (dxx * dyy - dxy * dxy)).astype(BF16))


def mesh_place():
    return lax.axis_index("row"), lax.axis_index("col")


def pack_kernel(x_hbm, *refs):
    count = (len(refs) - 3) // 2
    far, own_ref, near, x_ref, sems = refs[:count], refs[count], refs[count + 1 : -2], refs[-2], refs[-1]
    copies = [pltpu.make_async_copy(x_hbm, x_ref, sems.at[0])]
    copies += [pltpu.make_async_copy(f, n, sems.at[i + 1]) for i, (f, n) in enumerate(zip(far, near))]
    for copy in copies:
        copy.start()
    copies[0].wait()
    rows, cols = x_ref.shape
    for at in range(0, cols, BLOCK):
        to = slice(at, at + BLOCK)
        own_ref[:rows, to], own_ref[rows:, to] = split(x_ref[:, to])
    for copy in copies[1:]:
        copy.wait()


def send_kernel(side_ref, own_in, bm_ref, dc_ref, dl_ref, de_ref,
                own_ref, even_ref, odd_ref, base_ref, bvh, bvl):
    row, col = mesh_place()
    rows = own_ref.shape[0] // 2
    cols = own_ref.shape[1] - LANES
    is_left = col == 0
    even = row % 2 == 0
    own_ref[:rows, cols:], own_ref[rows:, cols:] = split(side_ref[...])

    def rows_of(part):
        own = own_ref[:, part]
        return mm(bm_ref[...], jnp.concatenate([own, own[:rows]], axis=0))

    for at in range(0, cols, BLOCK):
        to = slice(LANES + at, LANES + at + BLOCK)
        bvh[:, to], bvl[:, to] = split(rows_of(slice(at, at + BLOCK)))
    value = rows_of(slice(cols, cols + LANES))
    bvh[:, :LANES], bvl[:, :LANES] = split(jnp.where(is_left, 0.0, value))
    bvh[:, LANES + cols :], bvl[:, LANES + cols :] = split(jnp.where(is_left, value, 0.0))
    for j in range(cols // (2 * BLOCK)):
        at = LANES + 2 * BLOCK * j
        high = bvh[:, at : at + 2 * BLOCK]
        low = bvl[:, at : at + 2 * BLOCK]
        edge = edge_columns(bvh, bvl, at, 2 * BLOCK)
        base_ref[:, j * BLOCK : (j + 1) * BLOCK] = (
            mm(high, dc_ref[...]) + mm(low, dc_ref[...]) + mm(high, dl_ref[...]) + mm(edge, de_ref[...])
        )

    half = cols // 2
    first_up = REACH + 1 - 6
    first_down = REACH + 1 + SPAN
    for at in range(0, cols + LANES, LANES):
        to = slice(at, at + LANES)
        up_near, down_near = own_ref[:NEAR, to].astype(F32), own_ref[rows - NEAR : rows, to].astype(F32)
        up_low = own_ref[rows : rows + NEAR, to].astype(F32)[:LOW]
        down_low = own_ref[2 * rows - NEAR :, to].astype(F32)[NEAR - LOW :]
        if at < cols:
            lanes = slice(at % half, at % half + LANES)
            skip = PART * (at // half)
            up_part = base_ref[first_up + skip : first_up + skip + PART, lanes]
            down_part = base_ref[first_down + skip : first_down + skip + PART, lanes]
            skip = FINE // 2 * (at // half)

            def low_of(start):
                value = base_ref[start + skip : start + skip + FINE // 2, lanes]
                return value - value.astype(BF16).astype(F32)

            up_fine = low_of(first_up + SPAN - 13)
            down_fine = low_of(first_down + 13 - FINE)
        else:
            up_part = down_part = jnp.zeros((PART, LANES), F32)
            up_fine = down_fine = jnp.zeros((FINE // 2, LANES), F32)
        up = jnp.concatenate([up_near, up_low, up_fine, up_part], axis=0)
        down = jnp.concatenate([down_near, down_part, down_fine, down_low], axis=0)
        even_ref[:, to] = jnp.where(even, down, up).astype(BF16)
        odd_ref[:, to] = jnp.where(even, up, down).astype(BF16)


def base_kernel(row_count, tile_base, base_ref, even_ref, odd_ref, _, keep_ref, send_ref, sum_ref):
    row, col = mesh_place()
    base_rows, half = base_ref.shape
    count = keep_ref.shape[0]
    shift = tile_base // 2
    even = row % 2 == 0
    is_left = col == 0
    index = lax.broadcasted_iota(jnp.int32, (base_rows, LANES), 0)
    place = row * tile_base - REACH - 1 + index
    inside = (place >= 0) & (place < row_count * tile_base)
    first_bot = tile_base + REACH + 1 - 6
    for at in range(0, half, LANES):
        def message(ref_a, ref_b):
            both = []
            for lanes in (slice(at, at + LANES), slice(half + at, half + at + LANES)):
                a, b = ref_a[NEAR:, lanes].astype(F32), ref_b[NEAR:, lanes].astype(F32)
                both.append(jnp.where(even, a, b))
            return both

        to = slice(at, at + LANES)
        left, right = message(odd_ref, even_ref)
        top = jnp.concatenate([left[:PART], right[: SPAN - PART]], axis=0)
        top_fine = jnp.concatenate([left[PART : PART + FINE // 2], right[PART : PART + FINE // 2]], axis=0)
        left, right = message(even_ref, odd_ref)
        skip = LOW + FINE // 2
        bot = jnp.concatenate([left[skip:], right[skip : skip + SPAN - PART]], axis=0)
        bot_fine = jnp.concatenate([left[LOW:skip], right[LOW:skip]], axis=0)
        sum_ref[...] = base_ref[:, to]
        sum_ref[:SPAN, :] += top
        sum_ref[13 - FINE : 13, :] += top_fine
        sum_ref[first_bot : first_bot + SPAN, :] += bot
        first_fine = first_bot + SPAN - 13
        sum_ref[first_fine : first_fine + FINE, :] += bot_fine
        total = jnp.where(inside, sum_ref[...], 0.0)
        keep_ref[:, to] = jnp.where(is_left, total[:count], total[shift : shift + count])
        send_ref[:, to] = jnp.where(is_left, total[shift : shift + count], total[:count])


def filter_columns(vh, vl, w_refs, group, cols, lev, emit, after_group, after_level):
    wc_ref, wl_ref, we_ref = w_refs
    tall = vh.shape[1]
    for s in range(LEVELS):
        for g in range(0, cols // BLOCK, group):
            ats = [LANES + BLOCK * (g + i) for i in range(group)]
            high = jnp.concatenate([vh[s, :, at : at + BLOCK] for at in ats], axis=0)
            low = jnp.concatenate([vl[s, :, at : at + BLOCK] for at in ats], axis=0)
            edge = jnp.concatenate([edge_columns(vh.at[s], vl.at[s], at, BLOCK) for at in ats], axis=0)
            value = mm(high, wc_ref[s]) + mm(low, wc_ref[s]) + mm(high, wl_ref[s]) + mm(edge, we_ref[s])
            for i, at in enumerate(ats):
                new = value[i * tall : (i + 1) * tall]
                if s > 0:
                    emit(s - 1, at, new - lev[:, at : at + BLOCK])
                if s + 1 < LEVELS:
                    lev[:, at : at + BLOCK] = new
            if s >= 3:
                after_group(s - 3, g * BLOCK // LANES, group * BLOCK // LANES)
        after_level(s)


def place_rows(vh, vl, rows_of, cols, is_left):
    tall = vh.shape[1]
    for at in range(0, cols, BLOCK):
        value = rows_of(slice(at, at + BLOCK))
        to = slice(LANES + at, LANES + at + BLOCK)
        for s in range(LEVELS):
            vh[s, :, to], vl[s, :, to] = split(value[s * tall : (s + 1) * tall])
    value = rows_of(slice(cols, cols + LANES))
    left, right = slice(0, LANES), slice(LANES + cols, 2 * LANES + cols)
    for s in range(LEVELS):
        part = value[s * tall : (s + 1) * tall]
        vh[s, :, left], vl[s, :, left] = split(jnp.where(is_left, 0.0, part))
        vh[s, :, right], vl[s, :, right] = split(jnp.where(is_left, part, 0.0))


def seam_filter(vh, vl, w_refs, cols, lev, is_left, emit):
    wc_ref, wl_ref, _ = w_refs
    start = pl.multiple_of(jnp.where(is_left, cols, 0), LANES)

    def seam(s):
        if s not in (1, 2, 3):
            return
        high = vh[s, :, pl.ds(start, BLOCK)]
        low = vl[s, :, pl.ds(start, BLOCK)]
        new = mm(high, wc_ref[s]) + mm(low, wc_ref[s]) + mm(high, wl_ref[s])
        if s > 1:
            d = new - lev[:, cols + 2 * LANES :]
            emit(s - 1, 0, jnp.where(is_left, 0.0, d[:, :LANES]))
            emit(s - 1, cols + LANES, jnp.where(is_left, d[:, LANES:], 0.0))
        if s < 3:
            lev[:, cols + 2 * LANES :] = new

    return seam


def inner_kernel(own_ref, lh_hbm, wc_hbm, wl_hbm, we_hbm, cw_hbm, lt_hbm,
                 dog_ref, hess_ref, rim_ref, wc_ref, wl_ref, we_ref, cw_ref, lt_ref,
                 lh_ref, vh, vl, lev, d1, d2, sems):
    far = (lh_hbm, wc_hbm, wl_hbm, we_hbm, cw_hbm, lt_hbm)
    near = (lh_ref, wc_ref, wl_ref, we_ref, cw_ref, lt_ref)
    copies = [pltpu.make_async_copy(f, n, sems.at[i]) for i, (f, n) in enumerate(zip(far, near))]
    for copy in copies:
        copy.start()
    _, rows, cols = dog_ref.shape
    _, col = mesh_place()
    is_left = col == 0
    diffs = {1: d1, 2: d2}
    tall = rows + 2 * PAD
    mid_rows = rows - 2 * RIM
    rim_tall = RIM + 2 * PAD

    def rows_of(part):
        own = own_ref[:, part]
        return mm(lh_ref[...], jnp.concatenate([own, own[:rows]], axis=0))

    def emit(k, at, d):
        to = slice(at, at + d.shape[1])
        rim_ref[k, :rim_tall, to] = d[:rim_tall]
        rim_ref[k, rim_tall:, to] = d[tall - rim_tall :]
        if 0 < at <= cols:
            mid = d[PAD + RIM : PAD + RIM + mid_rows]
            dog_ref[k, RIM : RIM + mid_rows, at - LANES : at - LANES + BLOCK] = (20.0 * mid).astype(BF16)
        if k in diffs:
            diffs[k][:, to] = d

    def after_group(m, first, count):
        def put(t, value):
            hess_ref[m, RIM : RIM + mid_rows, t * LANES : (t + 1) * LANES] = value

        hess_tiles(diffs[m + 1], RIM, mid_rows, first, count, 5000.0, put)

    copies[0].wait()
    place_rows(vh, vl, rows_of, cols, is_left)
    for copy in copies[1:]:
        copy.wait()
    w_refs = (wc_ref, wl_ref, we_ref)
    seam = seam_filter(vh, vl, w_refs, cols, lev, is_left, emit)
    filter_columns(vh, vl, w_refs, 4, cols, lev, emit, after_group, seam)


def outer_kernel(last_row, even_ref, odd_ref, lt_ref, wc_ref, wl_ref, we_ref, rim_ref, dog_in, hess_in,
                 dog_ref, hess_ref, vh, vl, lev, d1, d2):
    _, rows, cols = dog_ref.shape
    row, col = mesh_place()
    is_left = col == 0
    even = row % 2 == 0
    diffs = {1: d1, 2: d2}
    rim_tall = RIM + 2 * PAD

    def rows_of(part):
        a, b = even_ref[:, part], odd_ref[:, part]
        bot, top = jnp.where(even, a, b), jnp.where(even, b, a)
        lows = jnp.concatenate([bot[NEAR : NEAR + 8], top[NEAR + 8 :]], axis=0)
        again = jnp.concatenate([bot[:8], top[8:NEAR]], axis=0)
        return mm(lt_ref[...], jnp.concatenate([top[:NEAR], bot[:NEAR], lows, again], axis=0))

    def emit(k, at, d):
        to = slice(at, at + d.shape[1])
        zero = lambda count: jnp.zeros((count, d.shape[1]), F32)
        top = rim_ref[k, :rim_tall, to] + jnp.concatenate(
            [zero(PAD - 1), d[:RIM], zero(rim_tall - RIM - PAD + 1)], axis=0
        )
        bot = rim_ref[k, rim_tall:, to] + jnp.concatenate(
            [zero(rim_tall - RIM - PAD + 1), d[RIM:], zero(PAD - 1)], axis=0
        )
        if 0 < at <= cols:
            out = slice(at - LANES, at - LANES + BLOCK)
            dog_ref[k, :RIM, out] = (20.0 * top[PAD : PAD + RIM]).astype(BF16)
            dog_ref[k, rows - RIM :, out] = (20.0 * bot[PAD : PAD + RIM]).astype(BF16)
        if k in diffs:
            d = diffs[k]
            d[:PAD, to] = jnp.where(row == 0, 0.0, top[:PAD])
            d[PAD:rim_tall, to] = top[PAD:]
            d[rim_tall : 2 * rim_tall - PAD, to] = bot[: rim_tall - PAD]
            d[2 * rim_tall - PAD :, to] = jnp.where(row == last_row, 0.0, bot[rim_tall - PAD :])

    def after_group(m, first, count):
        for top, to in ((0, slice(0, RIM)), (rim_tall, slice(rows - RIM, rows))):

            def put(t, value):
                hess_ref[m, to, t * LANES : (t + 1) * LANES] = value

            hess_tiles(diffs[m + 1], top, RIM, first, count, 5000.0, put)

    place_rows(vh, vl, rows_of, cols, is_left)
    w_refs = (wc_ref, wl_ref, we_ref)
    seam = seam_filter(vh, vl, w_refs, cols, lev, is_left, emit)
    filter_columns(vh, vl, w_refs, 8, cols, lev, emit, after_group, seam)


def coarse_kernel(last_row, keep_ref, other_ref, fine_dog_ref, fine_hess_ref, lh_ref, wc_ref, wl_ref, we_ref,
                  fine_dog_hbm, fine_hess_hbm, dog_hbm, hess_hbm,
                  dog_ref, hess_ref, vh, vl, lev, d1, d2, sems):
    fine_copies = [
        pltpu.make_async_copy(fine_dog_ref, fine_dog_hbm, sems.at[0]),
        pltpu.make_async_copy(fine_hess_ref, fine_hess_hbm, sems.at[1]),
    ]
    for copy in fine_copies:
        copy.start()
    _, rows, cols = dog_ref.shape
    row, col = mesh_place()
    tall = rows + 2 * PAD
    diffs = {1: d1, 2: d2}
    is_left = col == 0
    half = cols // 2
    zero = jnp.zeros((tall, LANES), BF16)
    for s in range(LEVELS):
        for ref in (vh, vl):
            ref[s, :, :LANES] = zero
            ref[s, :, LANES + cols :] = zero
    zero = jnp.zeros((tall, LANES), F32)
    for d in (d1, d2):
        d[:, :LANES] = zero
        d[:, LANES + cols :] = zero

    for at in range(0, cols, BLOCK):
        source = slice(at % half, at % half + BLOCK)
        first = is_left if at < half else jnp.logical_not(is_left)
        high, low = split(jnp.where(first, keep_ref[:, source], other_ref[:, source]))
        stack = jnp.concatenate([high, low, high], axis=0)
        value = mm(lh_ref[...], stack)
        to = slice(LANES + at, LANES + at + BLOCK)
        for s in range(LEVELS):
            vh[s, :, to], vl[s, :, to] = split(value[s * tall : (s + 1) * tall])

    def emit(k, at, d):
        dog_ref[k, :, at - LANES : at - LANES + BLOCK] = (80.0 * d[PAD : PAD + rows]).astype(BF16)
        if k in diffs:
            to = slice(at, at + BLOCK)
            diffs[k][:PAD, to] = jnp.where((row == 0) & (col == 0), 0.0, d[:PAD])
            diffs[k][PAD : PAD + rows, to] = d[PAD : PAD + rows]
            diffs[k][PAD + rows :, to] = jnp.where((row == last_row) & (col == 1), 0.0, d[PAD + rows :])

    def after_group(m, first, count):
        def put(t, value):
            hess_ref[m, :, t * LANES : (t + 1) * LANES] = value

        hess_tiles(diffs[m + 1], 0, rows, first, count, 200000.0, put)

    filter_columns(vh, vl, (wc_ref, wl_ref, we_ref), 8, cols, lev, emit, after_group, lambda s: None)
    copies = [
        pltpu.make_async_copy(dog_ref, dog_hbm, sems.at[2]),
        pltpu.make_async_copy(hess_ref, hess_hbm, sems.at[3]),
    ]
    for copy in copies:
        copy.start()
    for copy in fine_copies + copies:
        copy.wait()


def fine_constants(rows):
    own = np.arange(rows)
    top, bot = np.arange(-NEAR, 0), rows + np.arange(NEAR)
    nowhere = -1000
    lows = np.full(NEAR, nowhere)
    lows[:LOW] = bot[:LOW]
    lows[NEAR - LOW :] = top[NEAR - LOW :]
    again = np.concatenate([bot[:8], top[8:]])
    own_inputs = np.concatenate([own, own, own])
    own_low = np.arange(3 * rows) >= 2 * rows
    far_inputs = np.concatenate([top, bot, lows, again])
    far_low = np.arange(4 * NEAR) >= 3 * NEAR

    def matrix(sigma, centres, valid, inputs, use_low):
        high, low = two_parts(row_matrix(sigma, centres, inputs) * valid[:, None])
        return np.where(use_low[None, :], low.astype(np.float32), high.astype(np.float32)).astype(BF16)

    centres = np.arange(-PAD, rows + PAD)
    valid = ((centres >= -1) & (centres <= rows)).astype(np.float32)
    level = [matrix(s, centres, valid, own_inputs, own_low) for s in SIGMAS]
    rim = np.concatenate([np.arange(-1, RIM - 1), np.arange(rows + 1 - RIM, rows + 1)])
    halo = [matrix(s, rim, np.ones(rim.shape, np.float32), far_inputs, far_low) for s in SIGMAS]
    count = rows // 2 + 2 * (REACH + 1)
    index = np.arange(-(-count // 8) * 8)
    base = matrix(SIGMAS[-1], 2 * (index - REACH - 1), (index < count).astype(np.float32), own_inputs, own_low)
    strip_rows = -(-(rows // 4 + 2 * (REACH + 1)) // 16) * 16
    return np.concatenate(level), np.concatenate(halo), base, strip_rows


def coarse_constants(strip, padded):
    inputs = np.arange(padded) - REACH - 1
    centres = np.arange(-PAD, strip + PAD)
    valid = ((centres >= -1) & (centres <= strip)).astype(np.float32)
    parts = []
    for s in SIGMAS:
        high, low = two_parts(row_matrix(s, centres, inputs) * valid[:, None])
        parts.append(np.concatenate([high, high, low], axis=1))
    return np.concatenate(parts)


def vmem_specs(count):
    return [pl.BlockSpec(memory_space=pltpu.VMEM) for _ in range(count)]


def far_specs(count):
    return [pl.BlockSpec(memory_space=pltpu.HBM) for _ in range(count)]


def limit(mib):
    return pltpu.CompilerParams(vmem_limit_bytes=mib * 2**20)


def like(value):
    return jax.ShapeDtypeStruct(value.shape, value.dtype)


def far(value):
    return pltpu.with_memory_space_constraint(jnp.asarray(value), pltpu.HBM)


def local(image):
    rows, cols = image.shape
    row_count = lax.axis_size("row")
    col = lax.axis_index("col")
    strip = rows // 4
    wide = cols + LANES
    tall = rows + 2 * PAD
    small = strip + 2 * PAD
    lh, lt, bm, strip_rows = fine_constants(rows)
    cw = coarse_constants(strip, strip_rows)
    bands = [column_weights(s, 1) for s in SIGMAS]
    wc, wl, we = (np.stack([b[i] for b in bands]) for i in range(3))
    early = [far(c) for c in (bm, *column_weights(SIGMAS[-1], 2))]
    late = [far(c) for c in (lh, wc, wl, we, cw, lt)]

    side = jnp.where(col == 0, image[:, cols - LANES :], image[:, :LANES])
    side = lax.ppermute(side, "col", [(0, 1), (1, 0)])
    own, bm, dc, dl, de = pl.pallas_call(
        pack_kernel,
        out_shape=(jax.ShapeDtypeStruct((2 * rows, wide), BF16), *(like(c) for c in early)),
        in_specs=far_specs(1 + len(early)),
        out_specs=tuple(vmem_specs(1 + len(early))),
        scratch_shapes=[pltpu.VMEM((rows, cols), F32), pltpu.SemaphoreType.DMA((1 + len(early),))],
        compiler_params=limit(4),
        name="pack",
    )(far(image), *early)
    message = jax.ShapeDtypeStruct((2 * NEAR, wide), BF16)
    base_rows = bm.shape[0]
    own, to_even, to_odd, base = pl.pallas_call(
        send_kernel,
        out_shape=(
            jax.ShapeDtypeStruct((2 * rows, wide), BF16),
            message,
            message,
            jax.ShapeDtypeStruct((base_rows, cols // 2), F32),
        ),
        in_specs=vmem_specs(6),
        out_specs=tuple(vmem_specs(4)),
        scratch_shapes=[
            pltpu.VMEM((base_rows, cols + 2 * LANES), BF16),
            pltpu.VMEM((base_rows, cols + 2 * LANES), BF16),
        ],
        input_output_aliases={1: 0},
        compiler_params=limit(6),
        name="send",
    )(side, own, bm, dc, dl, de)

    def swap(value, first):
        pairs = [(i, i + 1) for i in range(first, row_count - 1, 2)]
        return lax.ppermute(value, "row", pairs + [(j, i) for i, j in pairs])

    even, odd = swap(to_even, 0), swap(to_odd, 1)

    fine_shapes = (
        jax.ShapeDtypeStruct((4, rows, cols), BF16),
        jax.ShapeDtypeStruct((2, rows, cols), BF16),
    )
    coarse_shapes = (
        jax.ShapeDtypeStruct((4, strip, cols), BF16),
        jax.ShapeDtypeStruct((2, strip, cols), BF16),
    )

    def scratch(count, height, seam):
        padded_cols = cols + 2 * LANES
        return [
            pltpu.VMEM((LEVELS, height, padded_cols), BF16),
            pltpu.VMEM((LEVELS, height, padded_cols), BF16),
            pltpu.VMEM((height, padded_cols + seam), F32),
            pltpu.VMEM((count, padded_cols), F32),
            pltpu.VMEM((count, padded_cols), F32),
        ]

    rim_tall = RIM + 2 * PAD
    dog_fine, hess_fine, rim, wc, wl, we, cw, lt = pl.pallas_call(
        inner_kernel,
        out_shape=(
            *fine_shapes,
            jax.ShapeDtypeStruct((4, 2 * rim_tall, cols + 2 * LANES), F32),
            *(like(c) for c in late[1:]),
        ),
        in_specs=vmem_specs(1) + far_specs(len(late)),
        out_specs=tuple(vmem_specs(3 + len(late) - 1)),
        scratch_shapes=[
            pltpu.VMEM(late[0].shape, late[0].dtype),
            *scratch(tall, tall, BLOCK),
            pltpu.SemaphoreType.DMA((len(late),)),
        ],
        compiler_params=limit(18),
        cost_estimate=pl.CostEstimate(flops=2 * 10**9, bytes_accessed=10**7, transcendentals=0),
        name="inner",
    )(own, *late)

    keep, send = pl.pallas_call(
        functools.partial(base_kernel, row_count, rows // 2),
        out_shape=(
            jax.ShapeDtypeStruct((strip_rows, cols // 2), F32),
            jax.ShapeDtypeStruct((strip_rows, cols // 2), F32),
        ),
        in_specs=vmem_specs(3) + [pl.BlockSpec(memory_space=pl.ANY)],
        out_specs=tuple(vmem_specs(2)),
        scratch_shapes=[pltpu.VMEM((base_rows, LANES), F32)],
        compiler_params=limit(4),
        name="base",
    )(base, even, odd, cw)
    other = lax.ppermute(send, "col", [(0, 1), (1, 0)])
    dog_fine, hess_fine = pl.pallas_call(
        functools.partial(outer_kernel, row_count - 1),
        out_shape=fine_shapes,
        in_specs=vmem_specs(9),
        out_specs=tuple(vmem_specs(2)),
        scratch_shapes=scratch(2 * rim_tall, 2 * RIM, BLOCK),
        input_output_aliases={7: 0, 8: 1},
        compiler_params=limit(14),
        cost_estimate=pl.CostEstimate(flops=10**9, bytes_accessed=10**6, transcendentals=0),
        name="outer",
    )(even, odd, lt, wc, wl, we, rim, dog_fine, hess_fine)

    return pl.pallas_call(
        functools.partial(coarse_kernel, row_count - 1),
        out_shape=fine_shapes + coarse_shapes,
        in_specs=vmem_specs(8),
        out_specs=tuple(far_specs(4)),
        scratch_shapes=[
            pltpu.VMEM((4, strip, cols), BF16),
            pltpu.VMEM((2, strip, cols), BF16),
            *scratch(small, small, 0),
            pltpu.SemaphoreType.DMA((4,)),
        ],
        compiler_params=limit(12),
        name="coarse",
    )(keep, other, dog_fine, hess_fine, cw, wc, wl, we)


def solution(mesh):
    return jax.shard_map(
        local,
        mesh=mesh,
        in_specs=(P(("slab", "row"), "col"),),
        out_specs=(
            P(None, ("slab", "row"), "col"),
            P(None, ("slab", "row"), "col"),
            P(None, ("slab", "row", "col"), None),
            P(None, ("slab", "row", "col"), None),
        ),
        check_vma=False,
    )
```

```python
import functools

import jax
import jax.numpy as jnp
import numpy as np
from jax import lax
from jax.experimental import pallas as pl
from jax.experimental.pallas import tpu as pltpu
from jax.sharding import PartitionSpec as P

SIGMAS = [1.6 * 2.0 ** (k / 4.0) for k in range(5)]
LEVELS = len(SIGMAS)
REACH = 12
LANES = 128
BLOCK = 256
PAD = 8
RIM = 16
NEAR = REACH + 1
SPAN = 19
PART = 10
MESSAGE = NEAR + 1 + PART
BF16 = jnp.bfloat16
F32 = jnp.float32


def taps(sigma):
    offset = np.arange(2 * REACH + 1, dtype=np.float64) - REACH
    weights = np.exp(-offset * offset / (2.0 * sigma * sigma))
    return (weights / weights.sum()).astype(np.float32)


def two_parts(matrix):
    high = np.asarray(matrix, np.float32).astype(BF16)
    low = (np.asarray(matrix, np.float32) - high.astype(np.float32)).astype(BF16)
    return high, low


def tap_at(sigma, index):
    weights = taps(sigma)
    inside = (index >= 0) & (index <= 2 * REACH)
    return np.where(inside, weights[np.clip(index, 0, 2 * REACH)], np.float32(0.0))


def row_matrix(sigma, centres, inputs):
    return tap_at(sigma, inputs[None, :] - centres[:, None] + REACH)


def column_weights(sigma, step):
    width = BLOCK * step
    out = np.arange(BLOCK)[None, :] * step
    high, low = two_parts(tap_at(sigma, np.arange(width)[:, None] - out + REACH))
    lane = np.arange(LANES)[:, None]
    right = np.where(lane < REACH, tap_at(sigma, width + lane - out + REACH), 0.0)
    left = np.where(lane >= LANES - REACH, tap_at(sigma, lane - LANES - out + REACH), 0.0)
    edge_high, edge_low = two_parts(right + left)
    edge = np.concatenate([edge_high.astype(np.float32), edge_high.astype(np.float32)])
    edge[:LANES] += np.roll(edge_low.astype(np.float32), 32, axis=0)
    return high, low, edge.astype(BF16)


def split(value):
    high = value.astype(BF16)
    low = (value - high.astype(F32)).astype(BF16)
    return high, low


def mm(a, b):
    return jnp.dot(a, b, preferred_element_type=F32)


def edge_pair(high_left, high_right, low_left, low_right):
    lane = lax.broadcasted_iota(jnp.int32, high_left.shape, 1)
    eh = jnp.where(lane < LANES // 2, high_right.astype(F32), high_left.astype(F32))
    el = jnp.where(lane < LANES // 2, low_right.astype(F32), low_left.astype(F32))
    again = pltpu.roll(eh, 32, 1)
    eh = jnp.where((lane >= 16) & (lane < 64), again, eh)
    return jnp.concatenate([eh.astype(BF16), el.astype(BF16)], axis=1)


def edge_columns(high, low, at, width):
    left, right = slice(at - LANES, at), slice(at + width, at + width + LANES)
    return edge_pair(high[:, left], high[:, right], low[:, left], low[:, right])


def hess_tiles(d, top, rows, first_tile, count, gain, put):
    tall = rows + 2 * PAD
    lane = lax.broadcasted_iota(jnp.int32, (tall, LANES), 1)
    tile = lambda t: d[top : top + tall, (first_tile + t + 1) * LANES : (first_tile + t + 2) * LANES]
    tiles = {-1: tile(-1), 0: tile(0)}
    back = {t: pltpu.roll(tiles[t], 1, 1) for t in (-1, 0)}
    ahead = {0: pltpu.roll(tiles[0], LANES - 1, 1)}
    for t in range(count):
        tiles[t + 1] = tile(t + 1)
        back[t + 1] = pltpu.roll(tiles[t + 1], 1, 1)
        ahead[t + 1] = pltpu.roll(tiles[t + 1], LANES - 1, 1)
        before = jnp.where(lane == 0, back[t - 1], back[t])
        after = jnp.where(lane == LANES - 1, ahead[t + 1], ahead[t])
        across = after - before
        mid = slice(PAD, PAD + rows)
        up, down = pltpu.roll(tiles[t], 1, 0)[mid], pltpu.roll(tiles[t], tall - 1, 0)[mid]
        twice = 2.0 * tiles[t][mid]
        dxx = after[mid] + before[mid] - twice
        dyy = up + down - twice
        dxy = (pltpu.roll(across, tall - 1, 0)[mid] - pltpu.roll(across, 1, 0)[mid]) * 0.25
        put(first_tile + t, (gain * (dxx * dyy - dxy * dxy)).astype(BF16))


def mesh_place():
    return lax.axis_index("row"), lax.axis_index("col")


def pack_kernel(x_hbm, early_hbm, own_ref, side_ref, early_ref, x_ref, sems):
    copy = pltpu.make_async_copy(x_hbm, x_ref, sems.at[0])
    constants = pltpu.make_async_copy(early_hbm, early_ref, sems.at[1])
    copy.start()
    constants.start()
    _, col = mesh_place()
    rows, cols = x_ref.shape
    copy.wait()
    side_ref[...] = jnp.where(col == 0, x_ref[:, cols - LANES :], x_ref[:, :LANES])
    for at in range(0, cols, BLOCK):
        to = slice(at, at + BLOCK)
        own_ref[:rows, to], own_ref[rows:, to] = split(x_ref[:, to])
    constants.wait()


def build_message(own_ref, part, rows, to):
    up_near = own_ref[:rows, to].astype(F32)[:NEAR]
    down_near = own_ref[:rows, to].astype(F32)[rows - NEAR :]
    up_low = own_ref[rows:, to].astype(F32)[:1]
    down_low = own_ref[rows:, to].astype(F32)[rows - 1 :]
    up = jnp.concatenate([up_near, up_low, part[0]], axis=0)
    down = jnp.concatenate([down_near, down_low, part[1]], axis=0)
    return up, down


def send_kernel(own_ref, early_ref, even_ref, odd_ref, base_ref, bvh, bvl):
    row, col = mesh_place()
    rows = own_ref.shape[0] // 2
    cols = own_ref.shape[1] - LANES
    half = cols // 2
    base_rows = base_ref.shape[0]
    is_left = col == 0
    even = row % 2 == 0
    bm = early_ref[:base_rows, : 3 * rows]
    dc = early_ref[base_rows : base_rows + 2 * BLOCK]
    dl = early_ref[base_rows + 2 * BLOCK : base_rows + 4 * BLOCK]
    de = early_ref[base_rows + 4 * BLOCK :]

    zero = jnp.zeros((base_rows, LANES), BF16)
    for ref in (bvh, bvl):
        ref[:, :LANES] = zero
        ref[:, LANES + cols :] = zero
    for at in range(0, cols, BLOCK):
        own = own_ref[:, at : at + BLOCK]
        value = mm(bm, jnp.concatenate([own, own[:rows]], axis=0))
        to = slice(LANES + at, LANES + at + BLOCK)
        bvh[:, to], bvl[:, to] = split(value)
    for j in range(cols // (2 * BLOCK)):
        at = LANES + 2 * BLOCK * j
        high = bvh[:, at : at + 2 * BLOCK]
        low = bvl[:, at : at + 2 * BLOCK]
        edge = edge_columns(bvh, bvl, at, 2 * BLOCK)
        base_ref[:, j * BLOCK : (j + 1) * BLOCK] = mm(high, dc) + mm(low, dc) + mm(high, dl) + mm(edge, de)
    first, last = slice(LANES, 2 * LANES), slice(cols, cols + LANES)
    none = jnp.zeros((base_rows, LANES), BF16)
    pick = lambda ref: (
        jnp.where(is_left, ref[:, last].astype(F32), 0.0),
        jnp.where(is_left, 0.0, ref[:, first].astype(F32)),
    )
    value = mm(edge_pair(*pick(bvh), *pick(bvl)), de)
    base_ref[:, half:] = jnp.where(is_left, value[:, :LANES], value[:, LANES:])

    first_up = REACH + 1 - 6
    first_down = REACH + 1 + SPAN
    for at in range(0, cols + LANES, LANES):
        to = slice(at, at + LANES)
        if at < cols:
            lanes = slice(at % half, at % half + LANES)
            skip = PART * (at // half)
            part = [base_ref[f + skip : f + skip + PART, lanes] for f in (first_up, first_down)]
        else:
            part = [
                base_ref[f : f + PART, half:] + pltpu.roll(base_ref[f + PART : f + 2 * PART, half:], LANES // 2, 1)
                for f in (first_up, first_down)
            ]
        up, down = build_message(own_ref, part, rows, to)
        if at == cols:
            index = lax.broadcasted_iota(jnp.int32, up.shape, 0)
            up = jnp.where(index > NEAR, up, 0.0)
            down = jnp.where(index > NEAR, down, 0.0)
        even_ref[:, to] = jnp.where(even, down, up).astype(BF16)
        odd_ref[:, to] = jnp.where(even, up, down).astype(BF16)


def side_kernel(side_ref, own_in, even_in, odd_in, own_ref, even_ref, odd_ref):
    row, _ = mesh_place()
    rows = own_ref.shape[0] // 2
    cols = own_ref.shape[1] - LANES
    even = row % 2 == 0
    high, low = split(side_ref[...])
    own_ref[:rows, cols:] = high
    own_ref[rows:, cols:] = low
    high, low = high.astype(F32), low.astype(F32)
    none = jnp.zeros((PART, LANES), F32)
    up = jnp.concatenate([high[:NEAR], low[:1], none], axis=0)
    down = jnp.concatenate([high[rows - NEAR :], low[rows - 1 :], none], axis=0)
    index = lax.broadcasted_iota(jnp.int32, up.shape, 0)
    for old, ref, a, b in ((even_in, even_ref, down, up), (odd_in, odd_ref, up, down)):
        kept = old[:, cols:].astype(F32)
        ref[:, cols:] = jnp.where(index > NEAR, kept, jnp.where(even, a, b)).astype(BF16)


def base_kernel(row_count, tile_base, base_ref, even_ref, odd_ref, _, keep_ref, send_ref, sum_ref):
    row, col = mesh_place()
    base_rows, wide = base_ref.shape
    half = wide - LANES
    count = keep_ref.shape[0]
    shift = tile_base // 2
    even = row % 2 == 0
    is_left = col == 0
    index = lax.broadcasted_iota(jnp.int32, (base_rows, LANES), 0)
    lane = lax.broadcasted_iota(jnp.int32, (PART, LANES), 1)
    outside = (lane >= LANES // 4) & (lane < 3 * LANES // 4)
    place = row * tile_base - REACH - 1 + index
    inside = (place >= 0) & (place < row_count * tile_base)
    first_bot = tile_base + REACH + 1 - 6

    def parts(ref_a, ref_b, at):
        def rows_of(lanes):
            a, b = ref_a[:, lanes].astype(F32), ref_b[:, lanes].astype(F32)
            return jnp.where(even, a, b)[NEAR + 1 :]

        if at < half:
            both = [rows_of(slice(at, at + LANES)), rows_of(slice(half + at, half + at + LANES))]
        else:
            value = rows_of(slice(2 * half, 2 * half + LANES))
            both = [jnp.where(outside, 0.0, v) for v in (value, pltpu.roll(value, LANES // 2, 1))]
        return jnp.concatenate([both[0], both[1][: SPAN - PART]], axis=0)

    for at in range(0, wide, LANES):
        to = slice(at, at + LANES)
        sum_ref[...] = base_ref[:, to]
        sum_ref[:SPAN, :] += parts(odd_ref, even_ref, at)
        sum_ref[first_bot : first_bot + SPAN, :] += parts(even_ref, odd_ref, at)
        total = jnp.where(inside, sum_ref[...], 0.0)
        keep_ref[:, to] = jnp.where(is_left, total[:count], total[shift : shift + count])
        send_ref[:, to] = jnp.where(is_left, total[shift : shift + count], total[:count])


def filter_columns(vh, vl, w_refs, group, cols, lev, emit, after_group, after_level):
    wc_ref, wl_ref, we_ref = w_refs
    tall = vh.shape[1]
    for s in range(LEVELS):
        band = slice(s * BLOCK, (s + 1) * BLOCK)
        for g in range(0, cols // BLOCK, group):
            ats = [LANES + BLOCK * (g + i) for i in range(group)]
            high = jnp.concatenate([vh[s, :, at : at + BLOCK] for at in ats], axis=0)
            low = jnp.concatenate([vl[s, :, at : at + BLOCK] for at in ats], axis=0)
            edge = jnp.concatenate([edge_columns(vh.at[s], vl.at[s], at, BLOCK) for at in ats], axis=0)
            value = (
                mm(high, wc_ref[band]) + mm(low, wc_ref[band]) + mm(high, wl_ref[band]) + mm(edge, we_ref[band])
            )
            for i, at in enumerate(ats):
                new = value[i * tall : (i + 1) * tall]
                if s > 0:
                    emit(s - 1, at, new - lev[:, at : at + BLOCK])
                if s + 1 < LEVELS:
                    lev[:, at : at + BLOCK] = new
            if s >= 3:
                after_group(s - 3, g * BLOCK // LANES, group * BLOCK // LANES)
        after_level(s)


def place_rows(vh, vl, rows_of, cols, is_left):
    tall = vh.shape[1]
    for at in range(0, cols, BLOCK):
        value = rows_of(slice(at, at + BLOCK))
        to = slice(LANES + at, LANES + at + BLOCK)
        for s in range(LEVELS):
            vh[s, :, to], vl[s, :, to] = split(value[s * tall : (s + 1) * tall])
    value = rows_of(slice(cols, cols + LANES))
    left, right = slice(0, LANES), slice(LANES + cols, 2 * LANES + cols)
    for s in range(LEVELS):
        part = value[s * tall : (s + 1) * tall]
        vh[s, :, left], vl[s, :, left] = split(jnp.where(is_left, 0.0, part))
        vh[s, :, right], vl[s, :, right] = split(jnp.where(is_left, part, 0.0))


def seam_filter(vh, vl, w_refs, cols, lev, is_left, emit):
    wc_ref, wl_ref, _ = w_refs
    start = pl.multiple_of(jnp.where(is_left, cols, 0), LANES)

    def seam(s):
        if s not in (1, 2, 3):
            return
        high = vh[s, :, pl.ds(start, BLOCK)]
        low = vl[s, :, pl.ds(start, BLOCK)]
        band = slice(s * BLOCK, (s + 1) * BLOCK)
        new = mm(high, wc_ref[band]) + mm(low, wc_ref[band]) + mm(high, wl_ref[band])
        if s > 1:
            d = new - lev[:, cols + 2 * LANES :]
            emit(s - 1, 0, jnp.where(is_left, 0.0, d[:, :LANES]))
            emit(s - 1, cols + LANES, jnp.where(is_left, d[:, LANES:], 0.0))
        if s < 3:
            lev[:, cols + 2 * LANES :] = new

    return seam


def band_refs(late_ref):
    size = LEVELS * BLOCK
    return [late_ref.at[i * size : (i + 1) * size] for i in range(3)]


def inner_kernel(own_ref, late_ref, dog_ref, hess_ref, rim_ref, vh, vl, lev, d1, d2):
    _, rows, cols = dog_ref.shape
    _, col = mesh_place()
    is_left = col == 0
    diffs = {1: d1, 2: d2}
    tall = rows + 2 * PAD
    mid_rows = rows - 2 * RIM
    rim_tall = RIM + 2 * PAD

    def rows_of(part):
        own = own_ref[:, part]
        return mm(lh, jnp.concatenate([own, own[:rows]], axis=0))

    def emit(k, at, d):
        to = slice(at, at + d.shape[1])
        rim_ref[k, :rim_tall, to] = d[:rim_tall]
        rim_ref[k, rim_tall:, to] = d[tall - rim_tall :]
        if 0 < at <= cols:
            mid = d[PAD + RIM : PAD + RIM + mid_rows]
            dog_ref[k, RIM : RIM + mid_rows, at - LANES : at - LANES + BLOCK] = (20.0 * mid).astype(BF16)
        if k in diffs:
            diffs[k][:, to] = d

    def after_group(m, first, count):
        def put(t, value):
            hess_ref[m, RIM : RIM + mid_rows, t * LANES : (t + 1) * LANES] = value

        hess_tiles(diffs[m + 1], RIM, mid_rows, first, count, 5000.0, put)

    first = 3 * LEVELS * BLOCK
    lh = late_ref[first : first + LEVELS * tall, : 3 * rows]
    place_rows(vh, vl, rows_of, cols, is_left)
    w_refs = band_refs(late_ref)
    seam = seam_filter(vh, vl, w_refs, cols, lev, is_left, emit)
    filter_columns(vh, vl, w_refs, 4, cols, lev, emit, after_group, seam)


def outer_kernel(last_row, even_ref, odd_ref, late_ref, rim_ref, dog_in, hess_in,
                 dog_ref, hess_ref, vh, vl, lev, d1, d2):
    _, rows, cols = dog_ref.shape
    row, col = mesh_place()
    is_left = col == 0
    even = row % 2 == 0
    diffs = {1: d1, 2: d2}
    rim_tall = RIM + 2 * PAD

    def rows_of(part):
        a, b = even_ref[:, part], odd_ref[:, part]
        bot, top = jnp.where(even, a, b), jnp.where(even, b, a)
        ends = jnp.concatenate([top[16:], bot[16:]], axis=0)
        stack = jnp.concatenate([top[:16], bot[:16], ends], axis=0)
        return mm(lt, jnp.concatenate([stack, stack], axis=0))

    def emit(k, at, d):
        to = slice(at, at + d.shape[1])
        zero = lambda count: jnp.zeros((count, d.shape[1]), F32)
        top = rim_ref[k, :rim_tall, to] + jnp.concatenate(
            [zero(PAD - 1), d[:RIM], zero(rim_tall - RIM - PAD + 1)], axis=0
        )
        bot = rim_ref[k, rim_tall:, to] + jnp.concatenate(
            [zero(rim_tall - RIM - PAD + 1), d[RIM:], zero(PAD - 1)], axis=0
        )
        if 0 < at <= cols:
            out = slice(at - LANES, at - LANES + BLOCK)
            dog_ref[k, :RIM, out] = (20.0 * top[PAD : PAD + RIM]).astype(BF16)
            dog_ref[k, rows - RIM :, out] = (20.0 * bot[PAD : PAD + RIM]).astype(BF16)
        if k in diffs:
            d = diffs[k]
            d[:PAD, to] = jnp.where(row == 0, 0.0, top[:PAD])
            d[PAD:rim_tall, to] = top[PAD:]
            d[rim_tall : 2 * rim_tall - PAD, to] = bot[: rim_tall - PAD]
            d[2 * rim_tall - PAD :, to] = jnp.where(row == last_row, 0.0, bot[rim_tall - PAD :])

    def after_group(m, first, count):
        for top, to in ((0, slice(0, RIM)), (rim_tall, slice(rows - RIM, rows))):

            def put(t, value):
                hess_ref[m, to, t * LANES : (t + 1) * LANES] = value

            hess_tiles(diffs[m + 1], top, RIM, first, count, 5000.0, put)

    first = 3 * LEVELS * BLOCK + LEVELS * (rows + 2 * PAD)
    lt = late_ref[first : first + LEVELS * 2 * RIM, : 4 * MESSAGE]
    place_rows(vh, vl, rows_of, cols, is_left)
    w_refs = band_refs(late_ref)
    seam = seam_filter(vh, vl, w_refs, cols, lev, is_left, emit)
    filter_columns(vh, vl, w_refs, 8, cols, lev, emit, after_group, seam)


def coarse_kernel(last_row, keep_ref, other_ref, fine_dog_ref, fine_hess_ref, late_ref,
                  fine_dog_hbm, fine_hess_hbm, dog_hbm, hess_hbm,
                  dog_ref, hess_ref, vh, vl, lev, d1, d2, sems):
    fine_copies = [
        pltpu.make_async_copy(fine_dog_ref, fine_dog_hbm, sems.at[0]),
        pltpu.make_async_copy(fine_hess_ref, fine_hess_hbm, sems.at[1]),
    ]
    for copy in fine_copies:
        copy.start()
    _, rows, cols = dog_ref.shape
    row, col = mesh_place()
    tall = rows + 2 * PAD
    diffs = {1: d1, 2: d2}
    is_left = col == 0
    half = cols // 2
    zero = jnp.zeros((tall, LANES), BF16)
    for s in range(LEVELS):
        for ref in (vh, vl):
            ref[s, :, :LANES] = zero
            ref[s, :, LANES + cols :] = zero
    zero = jnp.zeros((tall, LANES), F32)
    for d in (d1, d2):
        d[:, :LANES] = zero
        d[:, LANES + cols :] = zero

    strip_rows = keep_ref.shape[0]
    lh = late_ref[late_ref.shape[0] - LEVELS * tall :, : 3 * strip_rows]
    for at in range(0, cols, BLOCK):
        source = slice(at % half, at % half + BLOCK)
        first = is_left if at < half else jnp.logical_not(is_left)
        value = jnp.where(first, keep_ref[:, source], other_ref[:, source])
        if at in (half - BLOCK, half):
            extra = jnp.where(first, other_ref[:, half:], keep_ref[:, half:])
            none = jnp.zeros(extra.shape, F32)
            value = value + jnp.concatenate([none, extra] if at < half else [extra, none], axis=1)
        high, low = split(value)
        stack = jnp.concatenate([high, low, high], axis=0)
        value = mm(lh, stack)
        to = slice(LANES + at, LANES + at + BLOCK)
        for s in range(LEVELS):
            vh[s, :, to], vl[s, :, to] = split(value[s * tall : (s + 1) * tall])

    def emit(k, at, d):
        dog_ref[k, :, at - LANES : at - LANES + BLOCK] = (80.0 * d[PAD : PAD + rows]).astype(BF16)
        if k in diffs:
            to = slice(at, at + BLOCK)
            diffs[k][:PAD, to] = jnp.where((row == 0) & (col == 0), 0.0, d[:PAD])
            diffs[k][PAD : PAD + rows, to] = d[PAD : PAD + rows]
            diffs[k][PAD + rows :, to] = jnp.where((row == last_row) & (col == 1), 0.0, d[PAD + rows :])

    def after_group(m, first, count):
        def put(t, value):
            hess_ref[m, :, t * LANES : (t + 1) * LANES] = value

        hess_tiles(diffs[m + 1], 0, rows, first, count, 200000.0, put)

    filter_columns(vh, vl, band_refs(late_ref), 8, cols, lev, emit, after_group, lambda s: None)
    copies = [
        pltpu.make_async_copy(dog_ref, dog_hbm, sems.at[2]),
        pltpu.make_async_copy(hess_ref, hess_hbm, sems.at[3]),
    ]
    for copy in copies:
        copy.start()
    for copy in fine_copies + copies:
        copy.wait()


def fine_constants(rows):
    own = np.arange(rows)
    own_inputs = np.concatenate([own, own, own])
    own_low = np.arange(3 * rows) >= 2 * rows
    nowhere = -1000
    top = np.full(MESSAGE, nowhere)
    top[: NEAR + 1] = np.append(np.arange(-NEAR, 0), -1)
    bot = np.full(MESSAGE, nowhere)
    bot[: NEAR + 1] = rows + np.append(np.arange(NEAR), 0)
    inputs = np.concatenate([top[:16], bot[:16], top[16:], bot[16:]])
    again = inputs.copy()
    again[[NEAR, 16 + NEAR]] = nowhere
    far_inputs = np.concatenate([inputs, again])
    far_low = np.arange(4 * MESSAGE) >= 2 * MESSAGE

    def matrix(sigma, centres, valid, inputs, use_low):
        high, low = two_parts(row_matrix(sigma, centres, inputs) * valid[:, None])
        return np.where(use_low[None, :], low.astype(np.float32), high.astype(np.float32)).astype(BF16)

    centres = np.arange(-PAD, rows + PAD)
    valid = ((centres >= -1) & (centres <= rows)).astype(np.float32)
    level = [matrix(s, centres, valid, own_inputs, own_low) for s in SIGMAS]
    rim = np.concatenate([np.arange(-1, RIM - 1), np.arange(rows + 1 - RIM, rows + 1)])
    halo = [matrix(s, rim, np.ones(rim.shape, np.float32), far_inputs, far_low) for s in SIGMAS]
    count = rows // 2 + 2 * (REACH + 1)
    index = np.arange(-(-count // 8) * 8)
    base = matrix(SIGMAS[-1], 2 * (index - REACH - 1), (index < count).astype(np.float32), own_inputs, own_low)
    strip_rows = -(-(rows // 4 + 2 * (REACH + 1)) // 16) * 16
    return np.concatenate(level), np.concatenate(halo), base, strip_rows


def coarse_constants(strip, padded):
    inputs = np.arange(padded) - REACH - 1
    centres = np.arange(-PAD, strip + PAD)
    valid = ((centres >= -1) & (centres <= strip)).astype(np.float32)
    parts = []
    for s in SIGMAS:
        high, low = two_parts(row_matrix(s, centres, inputs) * valid[:, None])
        parts.append(np.concatenate([high, high, low], axis=1))
    return np.concatenate(parts)


def joined(matrices):
    return np.concatenate(
        [np.pad(m.reshape(-1, m.shape[-1]).astype(np.float32), ((0, 0), (0, BLOCK - m.shape[-1]))) for m in matrices]
    ).astype(BF16)


def vmem_specs(count):
    return [pl.BlockSpec(memory_space=pltpu.VMEM) for _ in range(count)]


def far_specs(count):
    return [pl.BlockSpec(memory_space=pltpu.HBM) for _ in range(count)]


def limit(mib):
    return pltpu.CompilerParams(vmem_limit_bytes=mib * 2**20)


def like(value):
    return jax.ShapeDtypeStruct(value.shape, value.dtype)


def far(value):
    return pltpu.with_memory_space_constraint(jnp.asarray(value), pltpu.HBM)


def local(image):
    rows, cols = image.shape
    row_count = lax.axis_size("row")
    strip = rows // 4
    wide = cols + LANES
    tall = rows + 2 * PAD
    small = strip + 2 * PAD
    lh, lt, bm, strip_rows = fine_constants(rows)
    cw = coarse_constants(strip, strip_rows)
    bands = [column_weights(s, 1) for s in SIGMAS]
    wc, wl, we = (np.stack([b[i] for b in bands]) for i in range(3))
    early = far(joined([bm, *column_weights(SIGMAS[-1], 2)]))
    late = jnp.asarray(joined([wc, wl, we, lh, lt, cw]))
    base_rows = bm.shape[0]
    own_shape = jax.ShapeDtypeStruct((2 * rows, wide), BF16)
    message = jax.ShapeDtypeStruct((MESSAGE, wide), BF16)

    own, side, early = pl.pallas_call(
        pack_kernel,
        out_shape=(own_shape, jax.ShapeDtypeStruct((rows, LANES), F32), like(early)),
        in_specs=far_specs(2),
        out_specs=tuple(vmem_specs(3)),
        scratch_shapes=[pltpu.VMEM((rows, cols), F32), pltpu.SemaphoreType.DMA((2,))],
        compiler_params=limit(4),
        name="pack",
    )(far(image), early)
    side = lax.ppermute(side, "col", [(0, 1), (1, 0)])
    to_even, to_odd, base = pl.pallas_call(
        send_kernel,
        out_shape=(message, message, jax.ShapeDtypeStruct((base_rows, cols // 2 + LANES), F32)),
        in_specs=vmem_specs(2),
        out_specs=tuple(vmem_specs(3)),
        scratch_shapes=[
            pltpu.VMEM((base_rows, cols + 2 * LANES), BF16),
            pltpu.VMEM((base_rows, cols + 2 * LANES), BF16),
        ],
        compiler_params=limit(6),
        cost_estimate=pl.CostEstimate(flops=10**9, bytes_accessed=10**6, transcendentals=0),
        name="send",
    )(own, early)
    own, to_even, to_odd = pl.pallas_call(
        side_kernel,
        out_shape=(own_shape, message, message),
        in_specs=vmem_specs(4),
        out_specs=tuple(vmem_specs(3)),
        input_output_aliases={1: 0, 2: 1, 3: 2},
        compiler_params=limit(4),
        name="side",
    )(side, own, to_even, to_odd)

    def swap(value, first):
        pairs = [(i, i + 1) for i in range(first, row_count - 1, 2)]
        return lax.ppermute(value, "row", pairs + [(j, i) for i, j in pairs])

    even, odd = swap(to_even, 0), swap(to_odd, 1)

    fine_shapes = (
        jax.ShapeDtypeStruct((4, rows, cols), BF16),
        jax.ShapeDtypeStruct((2, rows, cols), BF16),
    )
    coarse_shapes = (
        jax.ShapeDtypeStruct((4, strip, cols), BF16),
        jax.ShapeDtypeStruct((2, strip, cols), BF16),
    )

    def scratch(count, height, seam):
        padded_cols = cols + 2 * LANES
        return [
            pltpu.VMEM((LEVELS, height, padded_cols), BF16),
            pltpu.VMEM((LEVELS, height, padded_cols), BF16),
            pltpu.VMEM((height, padded_cols + seam), F32),
            pltpu.VMEM((count, padded_cols), F32),
            pltpu.VMEM((count, padded_cols), F32),
        ]

    rim_tall = RIM + 2 * PAD
    dog_fine, hess_fine, rim = pl.pallas_call(
        inner_kernel,
        out_shape=(*fine_shapes, jax.ShapeDtypeStruct((4, 2 * rim_tall, cols + 2 * LANES), F32)),
        in_specs=vmem_specs(2),
        out_specs=tuple(vmem_specs(3)),
        scratch_shapes=scratch(tall, tall, BLOCK),
        compiler_params=limit(18),
        cost_estimate=pl.CostEstimate(flops=2 * 10**9, bytes_accessed=10**7, transcendentals=0),
        name="inner",
    )(own, late)

    keep, send = pl.pallas_call(
        functools.partial(base_kernel, row_count, rows // 2),
        out_shape=(
            jax.ShapeDtypeStruct((strip_rows, cols // 2 + LANES), F32),
            jax.ShapeDtypeStruct((strip_rows, cols // 2 + LANES), F32),
        ),
        in_specs=vmem_specs(3) + [pl.BlockSpec(memory_space=pl.ANY)],
        out_specs=tuple(vmem_specs(2)),
        scratch_shapes=[pltpu.VMEM((base_rows, LANES), F32)],
        compiler_params=limit(4),
        name="base",
    )(base, even, odd, rim)
    other = lax.ppermute(send, "col", [(0, 1), (1, 0)])
    dog_fine, hess_fine = pl.pallas_call(
        functools.partial(outer_kernel, row_count - 1),
        out_shape=fine_shapes,
        in_specs=vmem_specs(6),
        out_specs=tuple(vmem_specs(2)),
        scratch_shapes=scratch(2 * rim_tall, 2 * RIM, BLOCK),
        input_output_aliases={4: 0, 5: 1},
        compiler_params=limit(14),
        cost_estimate=pl.CostEstimate(flops=10**9, bytes_accessed=10**6, transcendentals=0),
        name="outer",
    )(even, odd, late, rim, dog_fine, hess_fine)

    return pl.pallas_call(
        functools.partial(coarse_kernel, row_count - 1),
        out_shape=fine_shapes + coarse_shapes,
        in_specs=vmem_specs(5),
        out_specs=tuple(far_specs(4)),
        scratch_shapes=[
            pltpu.VMEM((4, strip, cols), BF16),
            pltpu.VMEM((2, strip, cols), BF16),
            *scratch(small, small, 0),
            pltpu.SemaphoreType.DMA((4,)),
        ],
        compiler_params=limit(12),
        name="coarse",
    )(keep, other, dog_fine, hess_fine, late)


def solution(mesh):
    return jax.shard_map(
        local,
        mesh=mesh,
        in_specs=(P(("slab", "row"), "col"),),
        out_specs=(
            P(None, ("slab", "row"), "col"),
            P(None, ("slab", "row"), "col"),
            P(None, ("slab", "row", "col"), None),
            P(None, ("slab", "row", "col"), None),
        ),
        check_vma=False,
    )
```

```python
import functools

import jax
import jax.numpy as jnp
import numpy as np
from jax import lax
from jax.experimental import pallas as pl
from jax.experimental.pallas import tpu as pltpu
from jax.sharding import PartitionSpec as P

SIGMAS = [1.6 * 2.0 ** (k / 4.0) for k in range(5)]
LEVELS = len(SIGMAS)
REACH = 12
LANES = 128
BLOCK = 256
PAD = 8
RIM = 16
NEAR = REACH + 1
SPAN = 19
PART = 10
MESSAGE = NEAR + 1 + PART
BF16 = jnp.bfloat16
F32 = jnp.float32


def taps(sigma):
    offset = np.arange(2 * REACH + 1, dtype=np.float64) - REACH
    weights = np.exp(-offset * offset / (2.0 * sigma * sigma))
    return (weights / weights.sum()).astype(np.float32)


def two_parts(matrix):
    high = np.asarray(matrix, np.float32).astype(BF16)
    low = (np.asarray(matrix, np.float32) - high.astype(np.float32)).astype(BF16)
    return high, low


def tap_at(sigma, index):
    weights = taps(sigma)
    inside = (index >= 0) & (index <= 2 * REACH)
    return np.where(inside, weights[np.clip(index, 0, 2 * REACH)], np.float32(0.0))


def row_matrix(sigma, centres, inputs):
    return tap_at(sigma, inputs[None, :] - centres[:, None] + REACH)


def column_weights(sigma, step):
    width = BLOCK
    out = np.arange(BLOCK // step)[None, :] * step
    high, low = two_parts(tap_at(sigma, np.arange(width)[:, None] - out + REACH))
    lane = np.arange(LANES)[:, None]
    right = np.where(lane < REACH, tap_at(sigma, width + lane - out + REACH), 0.0)
    left = np.where(lane >= LANES - REACH, tap_at(sigma, lane - LANES - out + REACH), 0.0)
    edge_high, edge_low = two_parts(right + left)
    edge = np.concatenate([edge_high.astype(np.float32), edge_high.astype(np.float32)])
    edge[:LANES] += np.roll(edge_low.astype(np.float32), 32, axis=0)
    return high, low, edge.astype(BF16)


def split(value):
    high = value.astype(BF16)
    low = (value - high.astype(F32)).astype(BF16)
    return high, low


def mm(a, b):
    return jnp.dot(a, b, preferred_element_type=F32)


def edge_pair(high_left, high_right, low_left, low_right):
    lane = lax.broadcasted_iota(jnp.int32, high_left.shape, 1)
    eh = jnp.where(lane < LANES // 2, high_right, high_left)
    el = jnp.where(lane < LANES // 2, low_right, low_left)
    again = pltpu.roll(eh.astype(F32), 32, 1).astype(BF16)
    eh = jnp.where((lane >= 16) & (lane < 64), again, eh)
    return jnp.concatenate([eh, el], axis=1)


def edge_columns(high, low, at, width):
    left, right = slice(at - LANES, at), slice(at + width, at + width + LANES)
    return edge_pair(high[:, left], high[:, right], low[:, left], low[:, right])


def hess_tiles(d, top, rows, first_tile, count, gain, put):
    tall = rows + 2 * PAD
    lane = lax.broadcasted_iota(jnp.int32, (rows, LANES), 1)
    mid, slope, total = {}, {}, {}
    back, ahead = {}, {}

    def load(t):
        lanes = slice((first_tile + t + 1) * LANES, (first_tile + t + 2) * LANES)
        value = d[top : top + tall, lanes]
        up, down = pltpu.roll(value, 1, 0)[PAD : PAD + rows], pltpu.roll(value, tall - 1, 0)[PAD : PAD + rows]
        mid[t] = value[PAD : PAD + rows]
        slope[t], total[t] = down - up, up + down
        if t < count:
            back[t] = [pltpu.roll(v, 1, 1) for v in (mid[t], slope[t])]
        if t >= 0:
            ahead[t] = [pltpu.roll(v, LANES - 1, 1) for v in (mid[t], slope[t])]

    load(-1)
    load(0)
    for t in range(count):
        load(t + 1)
        before = [jnp.where(lane == 0, a, b) for a, b in zip(back[t - 1], back[t])]
        after = [jnp.where(lane == LANES - 1, a, b) for a, b in zip(ahead[t + 1], ahead[t])]
        twice = 2.0 * mid[t]
        dxx = after[0] + before[0] - twice
        dyy = total[t] - twice
        dxy = (after[1] - before[1]) * 0.25
        put(first_tile + t, (gain * (dxx * dyy - dxy * dxy)).astype(BF16))


def mesh_place():
    return lax.axis_index("row"), lax.axis_index("col")


def pack_kernel(x_hbm, early_hbm, x_ref, side_ref, early_ref, sems):
    copy = pltpu.make_async_copy(x_hbm, x_ref, sems.at[0])
    constants = pltpu.make_async_copy(early_hbm, early_ref, sems.at[1])
    copy.start()
    constants.start()
    _, col = mesh_place()
    cols = x_ref.shape[1]
    copy.wait()
    side_ref[...] = jnp.where(col == 0, x_ref[:, cols - LANES :], x_ref[:, :LANES])
    constants.wait()


def build_message(own_ref, part, rows, to):
    up_near = own_ref[:rows, to].astype(F32)[:NEAR]
    down_near = own_ref[:rows, to].astype(F32)[rows - NEAR :]
    up_low = own_ref[rows:, to].astype(F32)[:1]
    down_low = own_ref[rows:, to].astype(F32)[rows - 1 :]
    up = jnp.concatenate([up_near, up_low, part[0]], axis=0)
    down = jnp.concatenate([down_near, down_low, part[1]], axis=0)
    return up, down


def send_kernel(x_ref, early_ref, own_ref, even_ref, odd_ref, base_ref, bvh, bvl):
    row, col = mesh_place()
    rows, cols = x_ref.shape
    half = cols // 2
    base_rows = base_ref.shape[0]
    is_left = col == 0
    even = row % 2 == 0
    bm = early_ref[:base_rows, : 3 * rows]
    dc, dl, de = (early_ref[base_rows + i * BLOCK : base_rows + (i + 1) * BLOCK, : BLOCK // 2] for i in range(3))

    zero = jnp.zeros((base_rows, LANES), BF16)
    for ref in (bvh, bvl):
        ref[:, :LANES] = zero
        ref[:, LANES + cols :] = zero
    for at in range(0, cols, BLOCK):
        high, low = split(x_ref[:, at : at + BLOCK])
        own_ref[:rows, at : at + BLOCK] = high
        own_ref[rows:, at : at + BLOCK] = low
        value = mm(bm, jnp.concatenate([high, low, high], axis=0))
        to = slice(LANES + at, LANES + at + BLOCK)
        bvh[:, to], bvl[:, to] = split(value)
    first, last = slice(LANES, 2 * LANES), slice(cols, cols + LANES)
    pick = lambda ref: (
        jnp.where(is_left, ref[:, last].astype(F32), 0.0).astype(BF16),
        jnp.where(is_left, 0.0, ref[:, first].astype(F32)).astype(BF16),
    )
    beyond = edge_pair(*pick(bvh), *pick(bvl))
    group = 4
    for g in range(0, cols // BLOCK, group):
        ats = [LANES + BLOCK * (g + i) for i in range(group)]
        high = jnp.concatenate([bvh[:, at : at + BLOCK] for at in ats], axis=0)
        low = jnp.concatenate([bvl[:, at : at + BLOCK] for at in ats], axis=0)
        edge = jnp.concatenate([edge_columns(bvh, bvl, at, BLOCK) for at in ats], axis=0)
        value = mm(high, dc) + mm(low, dc) + mm(high, dl) + mm(edge, de)
        for i in range(group):
            base_ref[:, (g + i) * LANES : (g + i + 1) * LANES] = value[i * base_rows : (i + 1) * base_rows]
    base_ref[:, half:] = mm(beyond, de)

    first_up = REACH + 1 - 6
    first_down = REACH + 1 + SPAN
    for at in range(0, cols + LANES, LANES):
        to = slice(at, at + LANES)
        if at < cols:
            lanes = slice(at % half, at % half + LANES)
            skip = PART * (at // half)
            part = [base_ref[f + skip : f + skip + PART, lanes] for f in (first_up, first_down)]
        else:
            part = [
                base_ref[f : f + PART, half:] + pltpu.roll(base_ref[f + PART : f + 2 * PART, half:], LANES // 2, 1)
                for f in (first_up, first_down)
            ]
        up, down = build_message(own_ref, part, rows, to)
        if at == cols:
            index = lax.broadcasted_iota(jnp.int32, up.shape, 0)
            up = jnp.where(index > NEAR, up, 0.0)
            down = jnp.where(index > NEAR, down, 0.0)
        even_ref[:, to] = jnp.where(even, down, up).astype(BF16)
        odd_ref[:, to] = jnp.where(even, up, down).astype(BF16)


def side_kernel(side_ref, own_in, even_in, odd_in, own_ref, even_ref, odd_ref):
    row, _ = mesh_place()
    rows = own_ref.shape[0] // 2
    cols = own_ref.shape[1] - LANES
    even = row % 2 == 0
    high, low = split(side_ref[...])
    own_ref[:rows, cols:] = high
    own_ref[rows:, cols:] = low
    high, low = high.astype(F32), low.astype(F32)
    none = jnp.zeros((PART, LANES), F32)
    up = jnp.concatenate([high[:NEAR], low[:1], none], axis=0)
    down = jnp.concatenate([high[rows - NEAR :], low[rows - 1 :], none], axis=0)
    index = lax.broadcasted_iota(jnp.int32, up.shape, 0)
    for old, ref, a, b in ((even_in, even_ref, down, up), (odd_in, odd_ref, up, down)):
        kept = old[:, cols:].astype(F32)
        ref[:, cols:] = jnp.where(index > NEAR, kept, jnp.where(even, a, b)).astype(BF16)


def base_kernel(row_count, tile_base, base_ref, even_ref, odd_ref, _, keep_ref, send_ref, sum_ref):
    row, col = mesh_place()
    base_rows, wide = base_ref.shape
    half = wide - LANES
    count = keep_ref.shape[0]
    shift = tile_base // 2
    even = row % 2 == 0
    is_left = col == 0
    index = lax.broadcasted_iota(jnp.int32, (base_rows, LANES), 0)
    lane = lax.broadcasted_iota(jnp.int32, (PART, LANES), 1)
    outside = (lane >= LANES // 4) & (lane < 3 * LANES // 4)
    place = row * tile_base - REACH - 1 + index
    inside = (place >= 0) & (place < row_count * tile_base)
    first_bot = tile_base + REACH + 1 - 6

    def parts(ref_a, ref_b, at):
        def rows_of(lanes):
            a, b = ref_a[:, lanes].astype(F32), ref_b[:, lanes].astype(F32)
            return jnp.where(even, a, b)[NEAR + 1 :]

        if at < half:
            both = [rows_of(slice(at, at + LANES)), rows_of(slice(half + at, half + at + LANES))]
        else:
            value = rows_of(slice(2 * half, 2 * half + LANES))
            both = [jnp.where(outside, 0.0, v) for v in (value, pltpu.roll(value, LANES // 2, 1))]
        return jnp.concatenate([both[0], both[1][: SPAN - PART]], axis=0)

    for at in range(0, wide, LANES):
        to = slice(at, at + LANES)
        sum_ref[...] = base_ref[:, to]
        sum_ref[:SPAN, :] += parts(odd_ref, even_ref, at)
        sum_ref[first_bot : first_bot + SPAN, :] += parts(even_ref, odd_ref, at)
        total = jnp.where(inside, sum_ref[...], 0.0)
        keep_ref[:, to] = jnp.where(is_left, total[:count], total[shift : shift + count])
        send_ref[:, to] = jnp.where(is_left, total[shift : shift + count], total[:count])


def filter_columns(vh, vl, w_refs, group, cols, lev, emit, after_group, after_level):
    wc_ref, wl_ref, we_ref = w_refs
    tall = vh.shape[1]
    for s in range(LEVELS):
        band = slice(s * BLOCK, (s + 1) * BLOCK)
        for g in range(0, cols // BLOCK, group):
            ats = [LANES + BLOCK * (g + i) for i in range(group)]
            high = jnp.concatenate([vh[s, :, at : at + BLOCK] for at in ats], axis=0)
            low = jnp.concatenate([vl[s, :, at : at + BLOCK] for at in ats], axis=0)
            edge = jnp.concatenate([edge_columns(vh.at[s], vl.at[s], at, BLOCK) for at in ats], axis=0)
            value = (
                mm(high, wc_ref[band]) + mm(low, wc_ref[band]) + mm(high, wl_ref[band]) + mm(edge, we_ref[band])
            )
            for i, at in enumerate(ats):
                new = value[i * tall : (i + 1) * tall]
                if s > 0:
                    emit(s - 1, at, new - lev[:, at : at + BLOCK])
                if s + 1 < LEVELS:
                    lev[:, at : at + BLOCK] = new
            if s >= 3:
                after_group(s - 3, g * BLOCK // LANES, group * BLOCK // LANES)
        after_level(s)


def place_rows(vh, vl, rows_of, cols, is_left):
    tall = vh.shape[1]
    for at in range(0, cols, BLOCK):
        value = rows_of(slice(at, at + BLOCK))
        to = slice(LANES + at, LANES + at + BLOCK)
        for s in range(LEVELS):
            vh[s, :, to], vl[s, :, to] = split(value[s * tall : (s + 1) * tall])
    value = rows_of(slice(cols, cols + LANES))
    left, right = slice(0, LANES), slice(LANES + cols, 2 * LANES + cols)
    for s in range(LEVELS):
        part = value[s * tall : (s + 1) * tall]
        vh[s, :, left], vl[s, :, left] = split(jnp.where(is_left, 0.0, part))
        vh[s, :, right], vl[s, :, right] = split(jnp.where(is_left, part, 0.0))


def seam_filter(vh, vl, w_refs, cols, lev, is_left, emit):
    wc_ref, wl_ref, _ = w_refs
    start = pl.multiple_of(jnp.where(is_left, cols, 0), LANES)

    def seam(s):
        if s not in (1, 2, 3):
            return
        high = vh[s, :, pl.ds(start, BLOCK)]
        low = vl[s, :, pl.ds(start, BLOCK)]
        band = slice(s * BLOCK, (s + 1) * BLOCK)
        new = mm(high, wc_ref[band]) + mm(low, wc_ref[band]) + mm(high, wl_ref[band])
        if s > 1:
            d = new - lev[:, cols + 2 * LANES :]
            emit(s - 1, 0, jnp.where(is_left, 0.0, d[:, :LANES]))
            emit(s - 1, cols + LANES, jnp.where(is_left, d[:, LANES:], 0.0))
        if s < 3:
            lev[:, cols + 2 * LANES :] = new

    return seam


def band_refs(late_ref):
    size = LEVELS * BLOCK
    return [late_ref.at[i * size : (i + 1) * size] for i in range(3)]


def inner_kernel(own_ref, late_ref, dog_ref, hess_ref, rim_ref, vh, vl, lev, d1, d2):
    _, rows, cols = dog_ref.shape
    _, col = mesh_place()
    is_left = col == 0
    diffs = {1: d1, 2: d2}
    tall = rows + 2 * PAD
    mid_rows = rows - 2 * RIM
    rim_tall = RIM + 2 * PAD

    def rows_of(part):
        own = own_ref[:, part]
        return mm(lh, jnp.concatenate([own, own[:rows]], axis=0))

    def emit(k, at, d):
        to = slice(at, at + d.shape[1])
        rim_ref[k, :rim_tall, to] = d[:rim_tall]
        rim_ref[k, rim_tall:, to] = d[tall - rim_tall :]
        if 0 < at <= cols:
            mid = d[PAD + RIM : PAD + RIM + mid_rows]
            dog_ref[k, RIM : RIM + mid_rows, at - LANES : at - LANES + BLOCK] = (20.0 * mid).astype(BF16)
        if k in diffs:
            diffs[k][:, to] = d

    def after_group(m, first, count):
        def put(t, value):
            hess_ref[m, RIM : RIM + mid_rows, t * LANES : (t + 1) * LANES] = value

        hess_tiles(diffs[m + 1], RIM, mid_rows, first, count, 5000.0, put)

    first = 3 * LEVELS * BLOCK
    lh = late_ref[first : first + LEVELS * tall, : 3 * rows]
    place_rows(vh, vl, rows_of, cols, is_left)
    w_refs = band_refs(late_ref)
    seam = seam_filter(vh, vl, w_refs, cols, lev, is_left, emit)
    filter_columns(vh, vl, w_refs, 4, cols, lev, emit, after_group, seam)


def outer_kernel(last_row, even_ref, odd_ref, late_ref, rim_ref, dog_in, hess_in,
                 dog_ref, hess_ref, vh, vl, lev, d1, d2):
    _, rows, cols = dog_ref.shape
    row, col = mesh_place()
    is_left = col == 0
    even = row % 2 == 0
    diffs = {1: d1, 2: d2}
    rim_tall = RIM + 2 * PAD

    def rows_of(part):
        a, b = even_ref[:, part], odd_ref[:, part]
        bot, top = jnp.where(even, a, b), jnp.where(even, b, a)
        ends = jnp.concatenate([top[16:], bot[16:]], axis=0)
        stack = jnp.concatenate([top[:16], bot[:16], ends], axis=0)
        return mm(lt, jnp.concatenate([stack, stack], axis=0))

    def emit(k, at, d):
        to = slice(at, at + d.shape[1])
        zero = lambda count: jnp.zeros((count, d.shape[1]), F32)
        top = rim_ref[k, :rim_tall, to] + jnp.concatenate(
            [zero(PAD - 1), d[:RIM], zero(rim_tall - RIM - PAD + 1)], axis=0
        )
        bot = rim_ref[k, rim_tall:, to] + jnp.concatenate(
            [zero(rim_tall - RIM - PAD + 1), d[RIM:], zero(PAD - 1)], axis=0
        )
        if 0 < at <= cols:
            out = slice(at - LANES, at - LANES + BLOCK)
            dog_ref[k, :RIM, out] = (20.0 * top[PAD : PAD + RIM]).astype(BF16)
            dog_ref[k, rows - RIM :, out] = (20.0 * bot[PAD : PAD + RIM]).astype(BF16)
        if k in diffs:
            d = diffs[k]
            d[:PAD, to] = jnp.where(row == 0, 0.0, top[:PAD])
            d[PAD:rim_tall, to] = top[PAD:]
            d[rim_tall : 2 * rim_tall - PAD, to] = bot[: rim_tall - PAD]
            d[2 * rim_tall - PAD :, to] = jnp.where(row == last_row, 0.0, bot[rim_tall - PAD :])

    def after_group(m, first, count):
        for top, to in ((0, slice(0, RIM)), (rim_tall, slice(rows - RIM, rows))):

            def put(t, value):
                hess_ref[m, to, t * LANES : (t + 1) * LANES] = value

            hess_tiles(diffs[m + 1], top, RIM, first, count, 5000.0, put)

    first = 3 * LEVELS * BLOCK + LEVELS * (rows + 2 * PAD)
    lt = late_ref[first : first + LEVELS * 2 * RIM, : 4 * MESSAGE]
    place_rows(vh, vl, rows_of, cols, is_left)
    w_refs = band_refs(late_ref)
    seam = seam_filter(vh, vl, w_refs, cols, lev, is_left, emit)
    filter_columns(vh, vl, w_refs, 8, cols, lev, emit, after_group, seam)


def coarse_kernel(last_row, keep_ref, other_ref, fine_dog_ref, fine_hess_ref, late_ref,
                  fine_dog_hbm, fine_hess_hbm, dog_hbm, hess_hbm,
                  dog_ref, hess_ref, vh, vl, lev, d1, d2, sems):
    fine_copies = [
        pltpu.make_async_copy(fine_dog_ref, fine_dog_hbm, sems.at[0]),
        pltpu.make_async_copy(fine_hess_ref, fine_hess_hbm, sems.at[1]),
    ]
    for copy in fine_copies:
        copy.start()
    _, rows, cols = dog_ref.shape
    row, col = mesh_place()
    tall = rows + 2 * PAD
    diffs = {1: d1, 2: d2}
    is_left = col == 0
    half = cols // 2
    zero = jnp.zeros((tall, LANES), BF16)
    for s in range(LEVELS):
        for ref in (vh, vl):
            ref[s, :, :LANES] = zero
            ref[s, :, LANES + cols :] = zero
    zero = jnp.zeros((tall, LANES), F32)
    for d in (d1, d2):
        d[:, :LANES] = zero
        d[:, LANES + cols :] = zero

    strip_rows = keep_ref.shape[0]
    lh = late_ref[late_ref.shape[0] - LEVELS * tall :, : 3 * strip_rows]
    for at in range(0, cols, BLOCK):
        source = slice(at % half, at % half + BLOCK)
        first = is_left if at < half else jnp.logical_not(is_left)
        value = jnp.where(first, keep_ref[:, source], other_ref[:, source])
        if at in (half - BLOCK, half):
            extra = jnp.where(first, other_ref[:, half:], keep_ref[:, half:])
            none = jnp.zeros(extra.shape, F32)
            value = value + jnp.concatenate([none, extra] if at < half else [extra, none], axis=1)
        high, low = split(value)
        stack = jnp.concatenate([high, low, high], axis=0)
        value = mm(lh, stack)
        to = slice(LANES + at, LANES + at + BLOCK)
        for s in range(LEVELS):
            vh[s, :, to], vl[s, :, to] = split(value[s * tall : (s + 1) * tall])

    def emit(k, at, d):
        dog_ref[k, :, at - LANES : at - LANES + BLOCK] = (80.0 * d[PAD : PAD + rows]).astype(BF16)
        if k in diffs:
            to = slice(at, at + BLOCK)
            diffs[k][:PAD, to] = jnp.where((row == 0) & (col == 0), 0.0, d[:PAD])
            diffs[k][PAD : PAD + rows, to] = d[PAD : PAD + rows]
            diffs[k][PAD + rows :, to] = jnp.where((row == last_row) & (col == 1), 0.0, d[PAD + rows :])

    def after_group(m, first, count):
        def put(t, value):
            hess_ref[m, :, t * LANES : (t + 1) * LANES] = value

        hess_tiles(diffs[m + 1], 0, rows, first, count, 200000.0, put)

    filter_columns(vh, vl, band_refs(late_ref), 8, cols, lev, emit, after_group, lambda s: None)
    copies = [
        pltpu.make_async_copy(dog_ref, dog_hbm, sems.at[2]),
        pltpu.make_async_copy(hess_ref, hess_hbm, sems.at[3]),
    ]
    for copy in copies:
        copy.start()
    for copy in fine_copies + copies:
        copy.wait()


def fine_constants(rows):
    own = np.arange(rows)
    own_inputs = np.concatenate([own, own, own])
    own_low = np.arange(3 * rows) >= 2 * rows
    nowhere = -1000
    top = np.full(MESSAGE, nowhere)
    top[: NEAR + 1] = np.append(np.arange(-NEAR, 0), -1)
    bot = np.full(MESSAGE, nowhere)
    bot[: NEAR + 1] = rows + np.append(np.arange(NEAR), 0)
    inputs = np.concatenate([top[:16], bot[:16], top[16:], bot[16:]])
    again = inputs.copy()
    again[[NEAR, 16 + NEAR]] = nowhere
    far_inputs = np.concatenate([inputs, again])
    far_low = np.arange(4 * MESSAGE) >= 2 * MESSAGE

    def matrix(sigma, centres, valid, inputs, use_low):
        high, low = two_parts(row_matrix(sigma, centres, inputs) * valid[:, None])
        return np.where(use_low[None, :], low.astype(np.float32), high.astype(np.float32)).astype(BF16)

    centres = np.arange(-PAD, rows + PAD)
    valid = ((centres >= -1) & (centres <= rows)).astype(np.float32)
    level = [matrix(s, centres, valid, own_inputs, own_low) for s in SIGMAS]
    rim = np.concatenate([np.arange(-1, RIM - 1), np.arange(rows + 1 - RIM, rows + 1)])
    halo = [matrix(s, rim, np.ones(rim.shape, np.float32), far_inputs, far_low) for s in SIGMAS]
    count = rows // 2 + 2 * (REACH + 1)
    index = np.arange(-(-count // 8) * 8)
    base = matrix(SIGMAS[-1], 2 * (index - REACH - 1), (index < count).astype(np.float32), own_inputs, own_low)
    strip_rows = -(-(rows // 4 + 2 * (REACH + 1)) // 16) * 16
    return np.concatenate(level), np.concatenate(halo), base, strip_rows


def coarse_constants(strip, padded):
    inputs = np.arange(padded) - REACH - 1
    centres = np.arange(-PAD, strip + PAD)
    valid = ((centres >= -1) & (centres <= strip)).astype(np.float32)
    parts = []
    for s in SIGMAS:
        high, low = two_parts(row_matrix(s, centres, inputs) * valid[:, None])
        parts.append(np.concatenate([high, high, low], axis=1))
    return np.concatenate(parts)


def joined(matrices, columns=BLOCK):
    return np.concatenate(
        [np.pad(m.reshape(-1, m.shape[-1]).astype(np.float32), ((0, 0), (0, columns - m.shape[-1]))) for m in matrices]
    ).astype(BF16)


def vmem_specs(count):
    return [pl.BlockSpec(memory_space=pltpu.VMEM) for _ in range(count)]


def far_specs(count):
    return [pl.BlockSpec(memory_space=pltpu.HBM) for _ in range(count)]


def limit(mib):
    return pltpu.CompilerParams(vmem_limit_bytes=mib * 2**20)


def like(value):
    return jax.ShapeDtypeStruct(value.shape, value.dtype)


def far(value):
    return pltpu.with_memory_space_constraint(jnp.asarray(value), pltpu.HBM)


def local(image):
    rows, cols = image.shape
    row_count = lax.axis_size("row")
    strip = rows // 4
    wide = cols + LANES
    tall = rows + 2 * PAD
    small = strip + 2 * PAD
    lh, lt, bm, strip_rows = fine_constants(rows)
    cw = coarse_constants(strip, strip_rows)
    bands = [column_weights(s, 1) for s in SIGMAS]
    wc, wl, we = (np.stack([b[i] for b in bands]) for i in range(3))
    early = far(joined([bm, *column_weights(SIGMAS[-1], 2)]))
    late = jnp.asarray(joined([wc, wl, we, lh, lt, cw]))
    base_rows = bm.shape[0]
    own_shape = jax.ShapeDtypeStruct((2 * rows, wide), BF16)
    message = jax.ShapeDtypeStruct((MESSAGE, wide), BF16)

    tile, side, early = pl.pallas_call(
        pack_kernel,
        out_shape=(like(image), jax.ShapeDtypeStruct((rows, LANES), F32), like(early)),
        in_specs=far_specs(2),
        out_specs=tuple(vmem_specs(3)),
        scratch_shapes=[pltpu.SemaphoreType.DMA((2,))],
        compiler_params=limit(4),
        name="pack",
    )(far(image), early)
    side = lax.ppermute(side, "col", [(0, 1), (1, 0)])
    own, to_even, to_odd, base = pl.pallas_call(
        send_kernel,
        out_shape=(own_shape, message, message, jax.ShapeDtypeStruct((base_rows, cols // 2 + LANES), F32)),
        in_specs=vmem_specs(2),
        out_specs=tuple(vmem_specs(4)),
        scratch_shapes=[
            pltpu.VMEM((base_rows, cols + 2 * LANES), BF16),
            pltpu.VMEM((base_rows, cols + 2 * LANES), BF16),
        ],
        compiler_params=limit(6),
        cost_estimate=pl.CostEstimate(flops=10**9, bytes_accessed=10**6, transcendentals=0),
        name="send",
    )(tile, early)
    own, to_even, to_odd = pl.pallas_call(
        side_kernel,
        out_shape=(own_shape, message, message),
        in_specs=vmem_specs(4),
        out_specs=tuple(vmem_specs(3)),
        input_output_aliases={1: 0, 2: 1, 3: 2},
        compiler_params=limit(4),
        name="side",
    )(side, own, to_even, to_odd)

    def swap(value, first):
        pairs = [(i, i + 1) for i in range(first, row_count - 1, 2)]
        return lax.ppermute(value, "row", pairs + [(j, i) for i, j in pairs])

    even, odd = swap(to_even, 0), swap(to_odd, 1)

    fine_shapes = (
        jax.ShapeDtypeStruct((4, rows, cols), BF16),
        jax.ShapeDtypeStruct((2, rows, cols), BF16),
    )
    coarse_shapes = (
        jax.ShapeDtypeStruct((4, strip, cols), BF16),
        jax.ShapeDtypeStruct((2, strip, cols), BF16),
    )

    def scratch(count, height, seam):
        padded_cols = cols + 2 * LANES
        return [
            pltpu.VMEM((LEVELS, height, padded_cols), BF16),
            pltpu.VMEM((LEVELS, height, padded_cols), BF16),
            pltpu.VMEM((height, padded_cols + seam), F32),
            pltpu.VMEM((count, padded_cols), F32),
            pltpu.VMEM((count, padded_cols), F32),
        ]

    rim_tall = RIM + 2 * PAD
    dog_fine, hess_fine, rim = pl.pallas_call(
        inner_kernel,
        out_shape=(*fine_shapes, jax.ShapeDtypeStruct((4, 2 * rim_tall, cols + 2 * LANES), F32)),
        in_specs=vmem_specs(2),
        out_specs=tuple(vmem_specs(3)),
        scratch_shapes=scratch(tall, tall, BLOCK),
        compiler_params=limit(18),
        cost_estimate=pl.CostEstimate(flops=2 * 10**9, bytes_accessed=10**7, transcendentals=0),
        name="inner",
    )(own, late)

    keep, send = pl.pallas_call(
        functools.partial(base_kernel, row_count, rows // 2),
        out_shape=(
            jax.ShapeDtypeStruct((strip_rows, cols // 2 + LANES), F32),
            jax.ShapeDtypeStruct((strip_rows, cols // 2 + LANES), F32),
        ),
        in_specs=vmem_specs(3) + [pl.BlockSpec(memory_space=pl.ANY)],
        out_specs=tuple(vmem_specs(2)),
        scratch_shapes=[pltpu.VMEM((base_rows, LANES), F32)],
        compiler_params=limit(4),
        name="base",
    )(base, even, odd, rim)
    other = lax.ppermute(send, "col", [(0, 1), (1, 0)])
    dog_fine, hess_fine = pl.pallas_call(
        functools.partial(outer_kernel, row_count - 1),
        out_shape=fine_shapes,
        in_specs=vmem_specs(6),
        out_specs=tuple(vmem_specs(2)),
        scratch_shapes=scratch(2 * rim_tall, 2 * RIM, BLOCK),
        input_output_aliases={4: 0, 5: 1},
        compiler_params=limit(14),
        cost_estimate=pl.CostEstimate(flops=10**9, bytes_accessed=10**6, transcendentals=0),
        name="outer",
    )(even, odd, late, rim, dog_fine, hess_fine)

    return pl.pallas_call(
        functools.partial(coarse_kernel, row_count - 1),
        out_shape=fine_shapes + coarse_shapes,
        in_specs=vmem_specs(5),
        out_specs=tuple(far_specs(4)),
        scratch_shapes=[
            pltpu.VMEM((4, strip, cols), BF16),
            pltpu.VMEM((2, strip, cols), BF16),
            *scratch(small, small, 0),
            pltpu.SemaphoreType.DMA((4,)),
        ],
        compiler_params=limit(12),
        name="coarse",
    )(keep, other, dog_fine, hess_fine, late)


def solution(mesh):
    return jax.shard_map(
        local,
        mesh=mesh,
        in_specs=(P(("slab", "row"), "col"),),
        out_specs=(
            P(None, ("slab", "row"), "col"),
            P(None, ("slab", "row"), "col"),
            P(None, ("slab", "row", "col"), None),
            P(None, ("slab", "row", "col"), None),
        ),
        check_vma=False,
    )
```

```python
import functools

import jax
import jax.numpy as jnp
import numpy as np
from jax import lax
from jax.experimental import pallas as pl
from jax.experimental.pallas import tpu as pltpu
from jax.sharding import PartitionSpec as P

SIGMAS = [1.6 * 2.0 ** (k / 4.0) for k in range(5)]
LEVELS = len(SIGMAS)
REACH = 12
LANES = 128
BLOCK = 256
PAD = 8
RIM = 16
NEAR = REACH + 1
SPAN = 19
PART = 10
MESSAGE = NEAR + 1 + PART
BF16 = jnp.bfloat16
F32 = jnp.float32


def taps(sigma):
    offset = np.arange(2 * REACH + 1, dtype=np.float64) - REACH
    weights = np.exp(-offset * offset / (2.0 * sigma * sigma))
    return (weights / weights.sum()).astype(np.float32)


def two_parts(matrix):
    high = np.asarray(matrix, np.float32).astype(BF16)
    low = (np.asarray(matrix, np.float32) - high.astype(np.float32)).astype(BF16)
    return high, low


def tap_at(sigma, index):
    weights = taps(sigma)
    inside = (index >= 0) & (index <= 2 * REACH)
    return np.where(inside, weights[np.clip(index, 0, 2 * REACH)], np.float32(0.0))


def row_matrix(sigma, centres, inputs):
    return tap_at(sigma, inputs[None, :] - centres[:, None] + REACH)


def column_weights(sigma, step):
    width = BLOCK
    out = np.arange(BLOCK // step)[None, :] * step
    high, low = two_parts(tap_at(sigma, np.arange(width)[:, None] - out + REACH))
    lane = np.arange(LANES)[:, None]
    right = np.where(lane < REACH, tap_at(sigma, width + lane - out + REACH), 0.0)
    left = np.where(lane >= LANES - REACH, tap_at(sigma, lane - LANES - out + REACH), 0.0)
    edge_high, edge_low = two_parts(right + left)
    edge = np.concatenate([edge_high.astype(np.float32), edge_high.astype(np.float32)])
    edge[:LANES] += np.roll(edge_low.astype(np.float32), 32, axis=0)
    return high, low, edge.astype(BF16)


def split(value):
    high = value.astype(BF16)
    low = (value - high.astype(F32)).astype(BF16)
    return high, low


def mm(a, b):
    return jnp.dot(a, b, preferred_element_type=F32)


def edge_pair(high_left, high_right, low_left, low_right):
    lane = lax.broadcasted_iota(jnp.int32, high_left.shape, 1)
    eh = jnp.where(lane < LANES // 2, high_right, high_left)
    el = jnp.where(lane < LANES // 2, low_right, low_left)
    again = pltpu.roll(eh.astype(F32), 32, 1).astype(BF16)
    eh = jnp.where((lane >= 16) & (lane < 64), again, eh)
    return jnp.concatenate([eh, el], axis=1)


def edge_columns(high, low, at, width):
    left, right = slice(at - LANES, at), slice(at + width, at + width + LANES)
    return edge_pair(high[:, left], high[:, right], low[:, left], low[:, right])


def hess_tiles(d, top, rows, first_tile, count, gain, put):
    tall = rows + 2 * PAD
    lane = lax.broadcasted_iota(jnp.int32, (rows, LANES), 1)
    mid, slope, total = {}, {}, {}
    back, ahead = {}, {}

    def load(t):
        lanes = slice((first_tile + t + 1) * LANES, (first_tile + t + 2) * LANES)
        value = d[top : top + tall, lanes]
        up, down = pltpu.roll(value, 1, 0)[PAD : PAD + rows], pltpu.roll(value, tall - 1, 0)[PAD : PAD + rows]
        mid[t] = value[PAD : PAD + rows]
        slope[t], total[t] = down - up, up + down
        if t < count:
            back[t] = [pltpu.roll(v, 1, 1) for v in (mid[t], slope[t])]
        if t >= 0:
            ahead[t] = [pltpu.roll(v, LANES - 1, 1) for v in (mid[t], slope[t])]

    load(-1)
    load(0)
    for t in range(count):
        load(t + 1)
        before = [jnp.where(lane == 0, a, b) for a, b in zip(back[t - 1], back[t])]
        after = [jnp.where(lane == LANES - 1, a, b) for a, b in zip(ahead[t + 1], ahead[t])]
        twice = 2.0 * mid[t]
        dxx = after[0] + before[0] - twice
        dyy = total[t] - twice
        dxy = (after[1] - before[1]) * 0.25
        put(first_tile + t, (gain * (dxx * dyy - dxy * dxy)).astype(BF16))


def mesh_place():
    return lax.axis_index("row"), lax.axis_index("col")


def border_kernel(x_hbm, side_ref, sem):
    _, col = mesh_place()
    start = pl.multiple_of(jnp.where(col == 0, x_hbm.shape[1] - LANES, 0), LANES)
    copy = pltpu.make_async_copy(x_hbm.at[:, pl.ds(start, LANES)], side_ref, sem)
    copy.start()
    copy.wait()


def build_message(own_ref, part, rows, to):
    up_near = own_ref[:rows, to].astype(F32)[:NEAR]
    down_near = own_ref[:rows, to].astype(F32)[rows - NEAR :]
    up_low = own_ref[rows:, to].astype(F32)[:1]
    down_low = own_ref[rows:, to].astype(F32)[rows - 1 :]
    up = jnp.concatenate([up_near, up_low, part[0]], axis=0)
    down = jnp.concatenate([down_near, down_low, part[1]], axis=0)
    return up, down


def send_kernel(x_ref, early_ref, own_ref, even_ref, odd_ref, base_ref, bvh, bvl):
    row, col = mesh_place()
    rows, cols = x_ref.shape
    half = cols // 2
    base_rows = base_ref.shape[0]
    is_left = col == 0
    even = row % 2 == 0
    bm = early_ref[:base_rows, : 3 * rows]
    dc, dl, de = (early_ref[base_rows + i * BLOCK : base_rows + (i + 1) * BLOCK, : BLOCK // 2] for i in range(3))

    zero = jnp.zeros((base_rows, LANES), BF16)
    for ref in (bvh, bvl):
        ref[:, :LANES] = zero
        ref[:, LANES + cols :] = zero
    for at in range(0, cols, BLOCK):
        high, low = split(x_ref[:, at : at + BLOCK])
        own_ref[:rows, at : at + BLOCK] = high
        own_ref[rows:, at : at + BLOCK] = low
        value = mm(bm, jnp.concatenate([high, low, high], axis=0))
        to = slice(LANES + at, LANES + at + BLOCK)
        bvh[:, to], bvl[:, to] = split(value)
    first, last = slice(LANES, 2 * LANES), slice(cols, cols + LANES)
    pick = lambda ref: (
        jnp.where(is_left, ref[:, last].astype(F32), 0.0).astype(BF16),
        jnp.where(is_left, 0.0, ref[:, first].astype(F32)).astype(BF16),
    )
    beyond = edge_pair(*pick(bvh), *pick(bvl))
    group = 4
    for g in range(0, cols // BLOCK, group):
        ats = [LANES + BLOCK * (g + i) for i in range(group)]
        high = jnp.concatenate([bvh[:, at : at + BLOCK] for at in ats], axis=0)
        low = jnp.concatenate([bvl[:, at : at + BLOCK] for at in ats], axis=0)
        edge = jnp.concatenate([edge_columns(bvh, bvl, at, BLOCK) for at in ats], axis=0)
        value = mm(high, dc) + mm(low, dc) + mm(high, dl) + mm(edge, de)
        for i in range(group):
            base_ref[:, (g + i) * LANES : (g + i + 1) * LANES] = value[i * base_rows : (i + 1) * base_rows]
    base_ref[:, half:] = mm(beyond, de)

    first_up = REACH + 1 - 6
    first_down = REACH + 1 + SPAN
    for at in range(0, cols + LANES, LANES):
        to = slice(at, at + LANES)
        if at < cols:
            lanes = slice(at % half, at % half + LANES)
            skip = PART * (at // half)
            part = [base_ref[f + skip : f + skip + PART, lanes] for f in (first_up, first_down)]
        else:
            part = [
                base_ref[f : f + PART, half:] + pltpu.roll(base_ref[f + PART : f + 2 * PART, half:], LANES // 2, 1)
                for f in (first_up, first_down)
            ]
        up, down = build_message(own_ref, part, rows, to)
        if at == cols:
            index = lax.broadcasted_iota(jnp.int32, up.shape, 0)
            up = jnp.where(index > NEAR, up, 0.0)
            down = jnp.where(index > NEAR, down, 0.0)
        even_ref[:, to] = jnp.where(even, down, up).astype(BF16)
        odd_ref[:, to] = jnp.where(even, up, down).astype(BF16)


def side_kernel(side_ref, own_in, even_in, odd_in, own_ref, even_ref, odd_ref):
    row, _ = mesh_place()
    rows = own_ref.shape[0] // 2
    cols = own_ref.shape[1] - LANES
    even = row % 2 == 0
    high, low = split(side_ref[...])
    own_ref[:rows, cols:] = high
    own_ref[rows:, cols:] = low
    high, low = high.astype(F32), low.astype(F32)
    none = jnp.zeros((PART, LANES), F32)
    up = jnp.concatenate([high[:NEAR], low[:1], none], axis=0)
    down = jnp.concatenate([high[rows - NEAR :], low[rows - 1 :], none], axis=0)
    index = lax.broadcasted_iota(jnp.int32, up.shape, 0)
    for old, ref, a, b in ((even_in, even_ref, down, up), (odd_in, odd_ref, up, down)):
        kept = old[:, cols:].astype(F32)
        ref[:, cols:] = jnp.where(index > NEAR, kept, jnp.where(even, a, b)).astype(BF16)


def base_kernel(row_count, tile_base, base_ref, even_ref, odd_ref, _, keep_ref, send_ref, sum_ref):
    row, col = mesh_place()
    base_rows, wide = base_ref.shape
    half = wide - LANES
    count = keep_ref.shape[0]
    shift = tile_base // 2
    even = row % 2 == 0
    is_left = col == 0
    index = lax.broadcasted_iota(jnp.int32, (base_rows, LANES), 0)
    lane = lax.broadcasted_iota(jnp.int32, (PART, LANES), 1)
    outside = (lane >= LANES // 4) & (lane < 3 * LANES // 4)
    place = row * tile_base - REACH - 1 + index
    inside = (place >= 0) & (place < row_count * tile_base)
    first_bot = tile_base + REACH + 1 - 6

    def parts(ref_a, ref_b, at):
        def rows_of(lanes):
            a, b = ref_a[:, lanes].astype(F32), ref_b[:, lanes].astype(F32)
            return jnp.where(even, a, b)[NEAR + 1 :]

        if at < half:
            both = [rows_of(slice(at, at + LANES)), rows_of(slice(half + at, half + at + LANES))]
        else:
            value = rows_of(slice(2 * half, 2 * half + LANES))
            both = [jnp.where(outside, 0.0, v) for v in (value, pltpu.roll(value, LANES // 2, 1))]
        return jnp.concatenate([both[0], both[1][: SPAN - PART]], axis=0)

    for at in range(0, wide, LANES):
        to = slice(at, at + LANES)
        sum_ref[...] = base_ref[:, to]
        sum_ref[:SPAN, :] += parts(odd_ref, even_ref, at)
        sum_ref[first_bot : first_bot + SPAN, :] += parts(even_ref, odd_ref, at)
        total = jnp.where(inside, sum_ref[...], 0.0)
        keep_ref[:, to] = jnp.where(is_left, total[:count], total[shift : shift + count])
        send_ref[:, to] = jnp.where(is_left, total[shift : shift + count], total[:count])


def filter_columns(vh, vl, w_refs, group, cols, lev, emit, after_group, after_level):
    wc_ref, wl_ref, we_ref = w_refs
    tall = vh.shape[1]
    for s in range(LEVELS):
        band = slice(s * BLOCK, (s + 1) * BLOCK)
        for g in range(0, cols // BLOCK, group):
            ats = [LANES + BLOCK * (g + i) for i in range(group)]
            high = jnp.concatenate([vh[s, :, at : at + BLOCK] for at in ats], axis=0)
            low = jnp.concatenate([vl[s, :, at : at + BLOCK] for at in ats], axis=0)
            edge = jnp.concatenate([edge_columns(vh.at[s], vl.at[s], at, BLOCK) for at in ats], axis=0)
            value = (
                mm(high, wc_ref[band]) + mm(low, wc_ref[band]) + mm(high, wl_ref[band]) + mm(edge, we_ref[band])
            )
            for i, at in enumerate(ats):
                new = value[i * tall : (i + 1) * tall]
                if s > 0:
                    emit(s - 1, at, new - lev[:, at : at + BLOCK])
                if s + 1 < LEVELS:
                    lev[:, at : at + BLOCK] = new
            if s >= 3:
                after_group(s - 3, g * BLOCK // LANES, group * BLOCK // LANES)
        after_level(s)


def place_rows(vh, vl, rows_of, cols, is_left):
    tall = vh.shape[1]
    for at in range(0, cols, BLOCK):
        value = rows_of(slice(at, at + BLOCK))
        to = slice(LANES + at, LANES + at + BLOCK)
        for s in range(LEVELS):
            vh[s, :, to], vl[s, :, to] = split(value[s * tall : (s + 1) * tall])
    value = rows_of(slice(cols, cols + LANES))
    left, right = slice(0, LANES), slice(LANES + cols, 2 * LANES + cols)
    for s in range(LEVELS):
        part = value[s * tall : (s + 1) * tall]
        vh[s, :, left], vl[s, :, left] = split(jnp.where(is_left, 0.0, part))
        vh[s, :, right], vl[s, :, right] = split(jnp.where(is_left, part, 0.0))


def seam_filter(vh, vl, w_refs, cols, lev, is_left, emit):
    wc_ref, wl_ref, _ = w_refs
    start = pl.multiple_of(jnp.where(is_left, cols, 0), LANES)

    def seam(s):
        if s not in (1, 2, 3):
            return
        high = vh[s, :, pl.ds(start, BLOCK)]
        low = vl[s, :, pl.ds(start, BLOCK)]
        band = slice(s * BLOCK, (s + 1) * BLOCK)
        new = mm(high, wc_ref[band]) + mm(low, wc_ref[band]) + mm(high, wl_ref[band])
        if s > 1:
            d = new - lev[:, cols + 2 * LANES :]
            emit(s - 1, 0, jnp.where(is_left, 0.0, d[:, :LANES]))
            emit(s - 1, cols + LANES, jnp.where(is_left, d[:, LANES:], 0.0))
        if s < 3:
            lev[:, cols + 2 * LANES :] = new

    return seam


def band_refs(late_ref):
    size = LEVELS * BLOCK
    return [late_ref.at[i * size : (i + 1) * size] for i in range(3)]


def inner_kernel(own_ref, late_ref, dog_ref, hess_ref, rim_ref, vh, vl, lev, d1, d2):
    _, rows, cols = dog_ref.shape
    _, col = mesh_place()
    is_left = col == 0
    diffs = {1: d1, 2: d2}
    tall = rows + 2 * PAD
    mid_rows = rows - 2 * RIM
    rim_tall = RIM + 2 * PAD

    def rows_of(part):
        own = own_ref[:, part]
        return mm(lh, jnp.concatenate([own, own[:rows]], axis=0))

    def emit(k, at, d):
        to = slice(at, at + d.shape[1])
        rim_ref[k, :rim_tall, to] = d[:rim_tall]
        rim_ref[k, rim_tall:, to] = d[tall - rim_tall :]
        if 0 < at <= cols:
            mid = d[PAD + RIM : PAD + RIM + mid_rows]
            dog_ref[k, RIM : RIM + mid_rows, at - LANES : at - LANES + BLOCK] = (20.0 * mid).astype(BF16)
        if k in diffs:
            diffs[k][:, to] = d

    def after_group(m, first, count):
        def put(t, value):
            hess_ref[m, RIM : RIM + mid_rows, t * LANES : (t + 1) * LANES] = value

        hess_tiles(diffs[m + 1], RIM, mid_rows, first, count, 5000.0, put)

    first = 3 * LEVELS * BLOCK
    lh = late_ref[first : first + LEVELS * tall, : 3 * rows]
    place_rows(vh, vl, rows_of, cols, is_left)
    w_refs = band_refs(late_ref)
    seam = seam_filter(vh, vl, w_refs, cols, lev, is_left, emit)
    filter_columns(vh, vl, w_refs, 4, cols, lev, emit, after_group, seam)


def outer_kernel(last_row, even_ref, odd_ref, late_ref, rim_ref, dog_in, hess_in,
                 dog_ref, hess_ref, vh, vl, lev, d1, d2):
    _, rows, cols = dog_ref.shape
    row, col = mesh_place()
    is_left = col == 0
    even = row % 2 == 0
    diffs = {1: d1, 2: d2}
    rim_tall = RIM + 2 * PAD

    def rows_of(part):
        a, b = even_ref[:, part], odd_ref[:, part]
        bot, top = jnp.where(even, a, b), jnp.where(even, b, a)
        ends = jnp.concatenate([top[16:], bot[16:]], axis=0)
        stack = jnp.concatenate([top[:16], bot[:16], ends], axis=0)
        return mm(lt, jnp.concatenate([stack, stack], axis=0))

    def emit(k, at, d):
        to = slice(at, at + d.shape[1])
        zero = lambda count: jnp.zeros((count, d.shape[1]), F32)
        top = rim_ref[k, :rim_tall, to] + jnp.concatenate(
            [zero(PAD - 1), d[:RIM], zero(rim_tall - RIM - PAD + 1)], axis=0
        )
        bot = rim_ref[k, rim_tall:, to] + jnp.concatenate(
            [zero(rim_tall - RIM - PAD + 1), d[RIM:], zero(PAD - 1)], axis=0
        )
        if 0 < at <= cols:
            out = slice(at - LANES, at - LANES + BLOCK)
            dog_ref[k, :RIM, out] = (20.0 * top[PAD : PAD + RIM]).astype(BF16)
            dog_ref[k, rows - RIM :, out] = (20.0 * bot[PAD : PAD + RIM]).astype(BF16)
        if k in diffs:
            d = diffs[k]
            d[:PAD, to] = jnp.where(row == 0, 0.0, top[:PAD])
            d[PAD:rim_tall, to] = top[PAD:]
            d[rim_tall : 2 * rim_tall - PAD, to] = bot[: rim_tall - PAD]
            d[2 * rim_tall - PAD :, to] = jnp.where(row == last_row, 0.0, bot[rim_tall - PAD :])

    def after_group(m, first, count):
        for top, to in ((0, slice(0, RIM)), (rim_tall, slice(rows - RIM, rows))):

            def put(t, value):
                hess_ref[m, to, t * LANES : (t + 1) * LANES] = value

            hess_tiles(diffs[m + 1], top, RIM, first, count, 5000.0, put)

    first = 3 * LEVELS * BLOCK + LEVELS * (rows + 2 * PAD)
    lt = late_ref[first : first + LEVELS * 2 * RIM, : 4 * MESSAGE]
    place_rows(vh, vl, rows_of, cols, is_left)
    w_refs = band_refs(late_ref)
    seam = seam_filter(vh, vl, w_refs, cols, lev, is_left, emit)
    filter_columns(vh, vl, w_refs, 8, cols, lev, emit, after_group, seam)


def coarse_kernel(last_row, keep_ref, other_ref, fine_dog_ref, fine_hess_ref, late_ref,
                  fine_dog_hbm, fine_hess_hbm, dog_hbm, hess_hbm,
                  dog_ref, hess_ref, vh, vl, lev, d1, d2, sems):
    fine_copies = [
        pltpu.make_async_copy(fine_dog_ref, fine_dog_hbm, sems.at[0]),
        pltpu.make_async_copy(fine_hess_ref, fine_hess_hbm, sems.at[1]),
    ]
    for copy in fine_copies:
        copy.start()
    _, rows, cols = dog_ref.shape
    row, col = mesh_place()
    tall = rows + 2 * PAD
    diffs = {1: d1, 2: d2}
    is_left = col == 0
    half = cols // 2
    zero = jnp.zeros((tall, LANES), BF16)
    for s in range(LEVELS):
        for ref in (vh, vl):
            ref[s, :, :LANES] = zero
            ref[s, :, LANES + cols :] = zero
    zero = jnp.zeros((tall, LANES), F32)
    for d in (d1, d2):
        d[:, :LANES] = zero
        d[:, LANES + cols :] = zero

    strip_rows = keep_ref.shape[0]
    lh = late_ref[late_ref.shape[0] - LEVELS * tall :, : 3 * strip_rows]
    for at in range(0, cols, BLOCK):
        source = slice(at % half, at % half + BLOCK)
        first = is_left if at < half else jnp.logical_not(is_left)
        value = jnp.where(first, keep_ref[:, source], other_ref[:, source])
        if at in (half - BLOCK, half):
            extra = jnp.where(first, other_ref[:, half:], keep_ref[:, half:])
            none = jnp.zeros(extra.shape, F32)
            value = value + jnp.concatenate([none, extra] if at < half else [extra, none], axis=1)
        high, low = split(value)
        stack = jnp.concatenate([high, low, high], axis=0)
        value = mm(lh, stack)
        to = slice(LANES + at, LANES + at + BLOCK)
        for s in range(LEVELS):
            vh[s, :, to], vl[s, :, to] = split(value[s * tall : (s + 1) * tall])

    def emit(k, at, d):
        dog_ref[k, :, at - LANES : at - LANES + BLOCK] = (80.0 * d[PAD : PAD + rows]).astype(BF16)
        if k in diffs:
            to = slice(at, at + BLOCK)
            diffs[k][:PAD, to] = jnp.where((row == 0) & (col == 0), 0.0, d[:PAD])
            diffs[k][PAD : PAD + rows, to] = d[PAD : PAD + rows]
            diffs[k][PAD + rows :, to] = jnp.where((row == last_row) & (col == 1), 0.0, d[PAD + rows :])

    def after_group(m, first, count):
        def put(t, value):
            hess_ref[m, :, t * LANES : (t + 1) * LANES] = value

        hess_tiles(diffs[m + 1], 0, rows, first, count, 200000.0, put)

    filter_columns(vh, vl, band_refs(late_ref), 8, cols, lev, emit, after_group, lambda s: None)
    copies = [
        pltpu.make_async_copy(dog_ref, dog_hbm, sems.at[2]),
        pltpu.make_async_copy(hess_ref, hess_hbm, sems.at[3]),
    ]
    for copy in copies:
        copy.start()
    for copy in fine_copies + copies:
        copy.wait()


def fine_constants(rows):
    own = np.arange(rows)
    own_inputs = np.concatenate([own, own, own])
    own_low = np.arange(3 * rows) >= 2 * rows
    nowhere = -1000
    top = np.full(MESSAGE, nowhere)
    top[: NEAR + 1] = np.append(np.arange(-NEAR, 0), -1)
    bot = np.full(MESSAGE, nowhere)
    bot[: NEAR + 1] = rows + np.append(np.arange(NEAR), 0)
    inputs = np.concatenate([top[:16], bot[:16], top[16:], bot[16:]])
    again = inputs.copy()
    again[[NEAR, 16 + NEAR]] = nowhere
    far_inputs = np.concatenate([inputs, again])
    far_low = np.arange(4 * MESSAGE) >= 2 * MESSAGE

    def matrix(sigma, centres, valid, inputs, use_low):
        high, low = two_parts(row_matrix(sigma, centres, inputs) * valid[:, None])
        return np.where(use_low[None, :], low.astype(np.float32), high.astype(np.float32)).astype(BF16)

    centres = np.arange(-PAD, rows + PAD)
    valid = ((centres >= -1) & (centres <= rows)).astype(np.float32)
    level = [matrix(s, centres, valid, own_inputs, own_low) for s in SIGMAS]
    rim = np.concatenate([np.arange(-1, RIM - 1), np.arange(rows + 1 - RIM, rows + 1)])
    halo = [matrix(s, rim, np.ones(rim.shape, np.float32), far_inputs, far_low) for s in SIGMAS]
    count = rows // 2 + 2 * (REACH + 1)
    index = np.arange(-(-count // 8) * 8)
    base = matrix(SIGMAS[-1], 2 * (index - REACH - 1), (index < count).astype(np.float32), own_inputs, own_low)
    strip_rows = -(-(rows // 4 + 2 * (REACH + 1)) // 16) * 16
    return np.concatenate(level), np.concatenate(halo), base, strip_rows


def coarse_constants(strip, padded):
    inputs = np.arange(padded) - REACH - 1
    centres = np.arange(-PAD, strip + PAD)
    valid = ((centres >= -1) & (centres <= strip)).astype(np.float32)
    parts = []
    for s in SIGMAS:
        high, low = two_parts(row_matrix(s, centres, inputs) * valid[:, None])
        parts.append(np.concatenate([high, high, low], axis=1))
    return np.concatenate(parts)


def joined(matrices, columns=BLOCK):
    return np.concatenate(
        [np.pad(m.reshape(-1, m.shape[-1]).astype(np.float32), ((0, 0), (0, columns - m.shape[-1]))) for m in matrices]
    ).astype(BF16)


def vmem_specs(count):
    return [pl.BlockSpec(memory_space=pltpu.VMEM) for _ in range(count)]


def far_specs(count):
    return [pl.BlockSpec(memory_space=pltpu.HBM) for _ in range(count)]


def limit(mib):
    return pltpu.CompilerParams(vmem_limit_bytes=mib * 2**20)


def like(value):
    return jax.ShapeDtypeStruct(value.shape, value.dtype)


def far(value):
    return pltpu.with_memory_space_constraint(jnp.asarray(value), pltpu.HBM)


def local(image):
    rows, cols = image.shape
    row_count = lax.axis_size("row")
    strip = rows // 4
    wide = cols + LANES
    tall = rows + 2 * PAD
    small = strip + 2 * PAD
    lh, lt, bm, strip_rows = fine_constants(rows)
    cw = coarse_constants(strip, strip_rows)
    bands = [column_weights(s, 1) for s in SIGMAS]
    wc, wl, we = (np.stack([b[i] for b in bands]) for i in range(3))
    early = jnp.asarray(joined([bm, *column_weights(SIGMAS[-1], 2)]))
    late = jnp.asarray(joined([wc, wl, we, lh, lt, cw]))
    base_rows = bm.shape[0]
    own_shape = jax.ShapeDtypeStruct((2 * rows, wide), BF16)
    message = jax.ShapeDtypeStruct((MESSAGE, wide), BF16)

    side = pl.pallas_call(
        border_kernel,
        out_shape=jax.ShapeDtypeStruct((rows, LANES), F32),
        in_specs=far_specs(1),
        out_specs=vmem_specs(1)[0],
        scratch_shapes=[pltpu.SemaphoreType.DMA],
        compiler_params=limit(1),
        cost_estimate=pl.CostEstimate(flops=2 * 10**9, bytes_accessed=10**7, transcendentals=0),
        name="border",
    )(far(image))
    side = lax.ppermute(side, "col", [(0, 1), (1, 0)])
    own, to_even, to_odd, base = pl.pallas_call(
        send_kernel,
        out_shape=(own_shape, message, message, jax.ShapeDtypeStruct((base_rows, cols // 2 + LANES), F32)),
        in_specs=vmem_specs(2),
        out_specs=tuple(vmem_specs(4)),
        scratch_shapes=[
            pltpu.VMEM((base_rows, cols + 2 * LANES), BF16),
            pltpu.VMEM((base_rows, cols + 2 * LANES), BF16),
        ],
        compiler_params=limit(6),
        cost_estimate=pl.CostEstimate(flops=10**9, bytes_accessed=10**6, transcendentals=0),
        name="send",
    )(image, early)
    own, to_even, to_odd = pl.pallas_call(
        side_kernel,
        out_shape=(own_shape, message, message),
        in_specs=vmem_specs(4),
        out_specs=tuple(vmem_specs(3)),
        input_output_aliases={1: 0, 2: 1, 3: 2},
        compiler_params=limit(4),
        name="side",
    )(side, own, to_even, to_odd)

    def swap(value, first):
        pairs = [(i, i + 1) for i in range(first, row_count - 1, 2)]
        return lax.ppermute(value, "row", pairs + [(j, i) for i, j in pairs])

    even, odd = swap(to_even, 0), swap(to_odd, 1)

    fine_shapes = (
        jax.ShapeDtypeStruct((4, rows, cols), BF16),
        jax.ShapeDtypeStruct((2, rows, cols), BF16),
    )
    coarse_shapes = (
        jax.ShapeDtypeStruct((4, strip, cols), BF16),
        jax.ShapeDtypeStruct((2, strip, cols), BF16),
    )

    def scratch(count, height, seam):
        padded_cols = cols + 2 * LANES
        return [
            pltpu.VMEM((LEVELS, height, padded_cols), BF16),
            pltpu.VMEM((LEVELS, height, padded_cols), BF16),
            pltpu.VMEM((height, padded_cols + seam), F32),
            pltpu.VMEM((count, padded_cols), F32),
            pltpu.VMEM((count, padded_cols), F32),
        ]

    rim_tall = RIM + 2 * PAD
    dog_fine, hess_fine, rim = pl.pallas_call(
        inner_kernel,
        out_shape=(*fine_shapes, jax.ShapeDtypeStruct((4, 2 * rim_tall, cols + 2 * LANES), F32)),
        in_specs=vmem_specs(2),
        out_specs=tuple(vmem_specs(3)),
        scratch_shapes=scratch(tall, tall, BLOCK),
        compiler_params=limit(18),
        cost_estimate=pl.CostEstimate(flops=2 * 10**9, bytes_accessed=10**7, transcendentals=0),
        name="inner",
    )(own, late)

    keep, send = pl.pallas_call(
        functools.partial(base_kernel, row_count, rows // 2),
        out_shape=(
            jax.ShapeDtypeStruct((strip_rows, cols // 2 + LANES), F32),
            jax.ShapeDtypeStruct((strip_rows, cols // 2 + LANES), F32),
        ),
        in_specs=vmem_specs(3) + [pl.BlockSpec(memory_space=pl.ANY)],
        out_specs=tuple(vmem_specs(2)),
        scratch_shapes=[pltpu.VMEM((base_rows, LANES), F32)],
        compiler_params=limit(4),
        name="base",
    )(base, even, odd, rim)
    other = lax.ppermute(send, "col", [(0, 1), (1, 0)])
    dog_fine, hess_fine = pl.pallas_call(
        functools.partial(outer_kernel, row_count - 1),
        out_shape=fine_shapes,
        in_specs=vmem_specs(6),
        out_specs=tuple(vmem_specs(2)),
        scratch_shapes=scratch(2 * rim_tall, 2 * RIM, BLOCK),
        input_output_aliases={4: 0, 5: 1},
        compiler_params=limit(14),
        cost_estimate=pl.CostEstimate(flops=10**9, bytes_accessed=10**6, transcendentals=0),
        name="outer",
    )(even, odd, late, rim, dog_fine, hess_fine)

    return pl.pallas_call(
        functools.partial(coarse_kernel, row_count - 1),
        out_shape=fine_shapes + coarse_shapes,
        in_specs=vmem_specs(5),
        out_specs=tuple(far_specs(4)),
        scratch_shapes=[
            pltpu.VMEM((4, strip, cols), BF16),
            pltpu.VMEM((2, strip, cols), BF16),
            *scratch(small, small, 0),
            pltpu.SemaphoreType.DMA((4,)),
        ],
        compiler_params=limit(12),
        name="coarse",
    )(keep, other, dog_fine, hess_fine, late)


def solution(mesh):
    return jax.shard_map(
        local,
        mesh=mesh,
        in_specs=(P(("slab", "row"), "col"),),
        out_specs=(
            P(None, ("slab", "row"), "col"),
            P(None, ("slab", "row"), "col"),
            P(None, ("slab", "row", "col"), None),
            P(None, ("slab", "row", "col"), None),
        ),
        check_vma=False,
    )
```

```python
import functools

import jax
import jax.numpy as jnp
import numpy as np
from jax import lax
from jax.experimental import pallas as pl
from jax.experimental.pallas import tpu as pltpu
from jax.sharding import PartitionSpec as P

SIGMAS = [1.6 * 2.0 ** (k / 4.0) for k in range(5)]
LEVELS = len(SIGMAS)
REACH = 12
LANES = 128
BLOCK = 256
PAD = 8
RIM = 16
NEAR = REACH + 1
SPAN = 19
PART = 10
MESSAGE = NEAR + 1 + PART
BF16 = jnp.bfloat16
F32 = jnp.float32


def taps(sigma):
    offset = np.arange(2 * REACH + 1, dtype=np.float64) - REACH
    weights = np.exp(-offset * offset / (2.0 * sigma * sigma))
    return (weights / weights.sum()).astype(np.float32)


def two_parts(matrix):
    high = np.asarray(matrix, np.float32).astype(BF16)
    low = (np.asarray(matrix, np.float32) - high.astype(np.float32)).astype(BF16)
    return high, low


def tap_at(sigma, index):
    weights = taps(sigma)
    inside = (index >= 0) & (index <= 2 * REACH)
    return np.where(inside, weights[np.clip(index, 0, 2 * REACH)], np.float32(0.0))


def row_matrix(sigma, centres, inputs):
    return tap_at(sigma, inputs[None, :] - centres[:, None] + REACH)


def column_weights(sigma, step):
    width = BLOCK
    out = np.arange(BLOCK // step)[None, :] * step
    high, low = two_parts(tap_at(sigma, np.arange(width)[:, None] - out + REACH))
    lane = np.arange(LANES)[:, None]
    right = np.where(lane < REACH, tap_at(sigma, width + lane - out + REACH), 0.0)
    left = np.where(lane >= LANES - REACH, tap_at(sigma, lane - LANES - out + REACH), 0.0)
    edge_high, edge_low = two_parts(right + left)
    edge = np.concatenate([edge_high.astype(np.float32), edge_high.astype(np.float32)])
    edge[:LANES] += np.roll(edge_low.astype(np.float32), 32, axis=0)
    return high, low, edge.astype(BF16)


def split(value):
    high = value.astype(BF16)
    low = (value - high.astype(F32)).astype(BF16)
    return high, low


def mm(a, b):
    return jnp.dot(a, b, preferred_element_type=F32)


def edge_pair(high_left, high_right, low_left, low_right):
    lane = lax.broadcasted_iota(jnp.int32, high_left.shape, 1)
    eh = jnp.where(lane < LANES // 2, high_right, high_left)
    el = jnp.where(lane < LANES // 2, low_right, low_left)
    again = pltpu.roll(eh.astype(F32), 32, 1).astype(BF16)
    eh = jnp.where((lane >= 16) & (lane < 64), again, eh)
    return jnp.concatenate([eh, el], axis=1)


def edge_columns(high, low, at, width):
    left, right = slice(at - LANES, at), slice(at + width, at + width + LANES)
    return edge_pair(high[:, left], high[:, right], low[:, left], low[:, right])


def hess_tiles(d, top, rows, first_tile, count, gain, put):
    tall = rows + 2 * PAD
    lane = lax.broadcasted_iota(jnp.int32, (rows, LANES), 1)
    mid, slope, total = {}, {}, {}
    back, ahead = {}, {}

    def load(t):
        lanes = slice((first_tile + t + 1) * LANES, (first_tile + t + 2) * LANES)
        value = d[top : top + tall, lanes]
        up, down = pltpu.roll(value, 1, 0)[PAD : PAD + rows], pltpu.roll(value, tall - 1, 0)[PAD : PAD + rows]
        mid[t] = value[PAD : PAD + rows]
        slope[t], total[t] = down - up, up + down
        if t < count:
            back[t] = [pltpu.roll(v, 1, 1) for v in (mid[t], slope[t])]
        if t >= 0:
            ahead[t] = [pltpu.roll(v, LANES - 1, 1) for v in (mid[t], slope[t])]

    load(-1)
    load(0)
    for t in range(count):
        load(t + 1)
        before = [jnp.where(lane == 0, a, b) for a, b in zip(back[t - 1], back[t])]
        after = [jnp.where(lane == LANES - 1, a, b) for a, b in zip(ahead[t + 1], ahead[t])]
        twice = 2.0 * mid[t]
        dxx = after[0] + before[0] - twice
        dyy = total[t] - twice
        dxy = (after[1] - before[1]) * 0.25
        put(first_tile + t, (gain * (dxx * dyy - dxy * dxy)).astype(BF16))


def mesh_place():
    return lax.axis_index("row"), lax.axis_index("col")


def border_kernel(x_hbm, side_ref, sem):
    _, col = mesh_place()
    start = pl.multiple_of(jnp.where(col == 0, x_hbm.shape[1] - LANES, 0), LANES)
    copy = pltpu.make_async_copy(x_hbm.at[:, pl.ds(start, LANES)], side_ref, sem)
    copy.start()
    copy.wait()


def build_message(own_ref, part, rows, to):
    up_near = own_ref[:rows, to].astype(F32)[:NEAR]
    down_near = own_ref[:rows, to].astype(F32)[rows - NEAR :]
    up_low = own_ref[rows:, to].astype(F32)[:1]
    down_low = own_ref[rows:, to].astype(F32)[rows - 1 :]
    up = jnp.concatenate([up_near, up_low, part[0]], axis=0)
    down = jnp.concatenate([down_near, down_low, part[1]], axis=0)
    return up, down


def send_kernel(x_ref, early_ref, own_ref, even_ref, odd_ref, base_ref, bvh, bvl):
    row, col = mesh_place()
    rows, cols = x_ref.shape
    half = cols // 2
    base_rows = base_ref.shape[0]
    is_left = col == 0
    even = row % 2 == 0
    bm = early_ref[:base_rows, : 3 * rows]
    dc, dl, de = (early_ref[base_rows + i * BLOCK : base_rows + (i + 1) * BLOCK, : BLOCK // 2] for i in range(3))

    zero = jnp.zeros((base_rows, LANES), BF16)
    for ref in (bvh, bvl):
        ref[:, :LANES] = zero
        ref[:, LANES + cols :] = zero
    for at in range(0, cols, BLOCK):
        high, low = split(x_ref[:, at : at + BLOCK])
        own_ref[:rows, at : at + BLOCK] = high
        own_ref[rows:, at : at + BLOCK] = low
        value = mm(bm, jnp.concatenate([high, low, high], axis=0))
        to = slice(LANES + at, LANES + at + BLOCK)
        bvh[:, to], bvl[:, to] = split(value)
    first, last = slice(LANES, 2 * LANES), slice(cols, cols + LANES)
    pick = lambda ref: (
        jnp.where(is_left, ref[:, last].astype(F32), 0.0).astype(BF16),
        jnp.where(is_left, 0.0, ref[:, first].astype(F32)).astype(BF16),
    )
    beyond = edge_pair(*pick(bvh), *pick(bvl))
    group = 4
    for g in range(0, cols // BLOCK, group):
        ats = [LANES + BLOCK * (g + i) for i in range(group)]
        high = jnp.concatenate([bvh[:, at : at + BLOCK] for at in ats], axis=0)
        low = jnp.concatenate([bvl[:, at : at + BLOCK] for at in ats], axis=0)
        edge = jnp.concatenate([edge_columns(bvh, bvl, at, BLOCK) for at in ats], axis=0)
        value = mm(high, dc) + mm(low, dc) + mm(high, dl) + mm(edge, de)
        for i in range(group):
            base_ref[:, (g + i) * LANES : (g + i + 1) * LANES] = value[i * base_rows : (i + 1) * base_rows]
    base_ref[:, half:] = mm(beyond, de)

    first_up = REACH + 1 - 6
    first_down = REACH + 1 + SPAN
    for at in range(0, cols + LANES, LANES):
        to = slice(at, at + LANES)
        if at < cols:
            lanes = slice(at % half, at % half + LANES)
            skip = PART * (at // half)
            part = [base_ref[f + skip : f + skip + PART, lanes] for f in (first_up, first_down)]
        else:
            part = [
                base_ref[f : f + PART, half:] + pltpu.roll(base_ref[f + PART : f + 2 * PART, half:], LANES // 2, 1)
                for f in (first_up, first_down)
            ]
        up, down = build_message(own_ref, part, rows, to)
        if at == cols:
            index = lax.broadcasted_iota(jnp.int32, up.shape, 0)
            up = jnp.where(index > NEAR, up, 0.0)
            down = jnp.where(index > NEAR, down, 0.0)
        even_ref[:, to] = jnp.where(even, down, up).astype(BF16)
        odd_ref[:, to] = jnp.where(even, up, down).astype(BF16)


def side_kernel(side_ref, own_in, even_in, odd_in, own_ref, even_ref, odd_ref):
    row, _ = mesh_place()
    rows = own_ref.shape[0] // 2
    cols = own_ref.shape[1] - LANES
    even = row % 2 == 0
    high, low = split(side_ref[...])
    own_ref[:rows, cols:] = high
    own_ref[rows:, cols:] = low
    high, low = high.astype(F32), low.astype(F32)
    none = jnp.zeros((PART, LANES), F32)
    up = jnp.concatenate([high[:NEAR], low[:1], none], axis=0)
    down = jnp.concatenate([high[rows - NEAR :], low[rows - 1 :], none], axis=0)
    index = lax.broadcasted_iota(jnp.int32, up.shape, 0)
    for old, ref, a, b in ((even_in, even_ref, down, up), (odd_in, odd_ref, up, down)):
        kept = old[:, cols:].astype(F32)
        ref[:, cols:] = jnp.where(index > NEAR, kept, jnp.where(even, a, b)).astype(BF16)


def base_kernel(row_count, tile_base, base_ref, even_ref, odd_ref, _, keep_ref, send_ref, sum_ref):
    row, col = mesh_place()
    base_rows, wide = base_ref.shape
    half = wide - LANES
    count = keep_ref.shape[0]
    shift = tile_base // 2
    even = row % 2 == 0
    is_left = col == 0
    index = lax.broadcasted_iota(jnp.int32, (base_rows, LANES), 0)
    lane = lax.broadcasted_iota(jnp.int32, (PART, LANES), 1)
    outside = (lane >= LANES // 4) & (lane < 3 * LANES // 4)
    place = row * tile_base - REACH - 1 + index
    inside = (place >= 0) & (place < row_count * tile_base)
    first_bot = tile_base + REACH + 1 - 6

    def parts(ref_a, ref_b, at):
        def rows_of(lanes):
            a, b = ref_a[:, lanes].astype(F32), ref_b[:, lanes].astype(F32)
            return jnp.where(even, a, b)[NEAR + 1 :]

        if at < half:
            both = [rows_of(slice(at, at + LANES)), rows_of(slice(half + at, half + at + LANES))]
        else:
            value = rows_of(slice(2 * half, 2 * half + LANES))
            both = [jnp.where(outside, 0.0, v) for v in (value, pltpu.roll(value, LANES // 2, 1))]
        return jnp.concatenate([both[0], both[1][: SPAN - PART]], axis=0)

    for at in range(0, wide, LANES):
        to = slice(at, at + LANES)
        sum_ref[...] = base_ref[:, to]
        sum_ref[:SPAN, :] += parts(odd_ref, even_ref, at)
        sum_ref[first_bot : first_bot + SPAN, :] += parts(even_ref, odd_ref, at)
        total = jnp.where(inside, sum_ref[...], 0.0)
        keep_ref[:, to] = jnp.where(is_left, total[:count], total[shift : shift + count])
        send_ref[:, to] = jnp.where(is_left, total[shift : shift + count], total[:count])


def filter_columns(vh, vl, w_refs, group, cols, lev, emit, after_group, after_level):
    wc_ref, wl_ref, we_ref = w_refs
    tall = vh.shape[1]
    for s in range(LEVELS):
        band = slice(s * BLOCK, (s + 1) * BLOCK)
        for g in range(0, cols // BLOCK, group):
            ats = [LANES + BLOCK * (g + i) for i in range(group)]
            high = jnp.concatenate([vh[s, :, at : at + BLOCK] for at in ats], axis=0)
            low = jnp.concatenate([vl[s, :, at : at + BLOCK] for at in ats], axis=0)
            edge = jnp.concatenate([edge_columns(vh.at[s], vl.at[s], at, BLOCK) for at in ats], axis=0)
            value = (
                mm(high, wc_ref[band]) + mm(low, wc_ref[band]) + mm(high, wl_ref[band]) + mm(edge, we_ref[band])
            )
            for i, at in enumerate(ats):
                new = value[i * tall : (i + 1) * tall]
                if s > 0:
                    emit(s - 1, at, new - lev[:, at : at + BLOCK])
                if s + 1 < LEVELS:
                    lev[:, at : at + BLOCK] = new
            if s >= 3:
                after_group(s - 3, g * BLOCK // LANES, group * BLOCK // LANES)
        after_level(s)


def place_rows(vh, vl, rows_of, cols, is_left):
    tall = vh.shape[1]
    for at in range(0, cols, BLOCK):
        value = rows_of(slice(at, at + BLOCK))
        to = slice(LANES + at, LANES + at + BLOCK)
        for s in range(LEVELS):
            vh[s, :, to], vl[s, :, to] = split(value[s * tall : (s + 1) * tall])
    value = rows_of(slice(cols, cols + LANES))
    left, right = slice(0, LANES), slice(LANES + cols, 2 * LANES + cols)
    for s in range(LEVELS):
        part = value[s * tall : (s + 1) * tall]
        vh[s, :, left], vl[s, :, left] = split(jnp.where(is_left, 0.0, part))
        vh[s, :, right], vl[s, :, right] = split(jnp.where(is_left, part, 0.0))


def seam_filter(vh, vl, w_refs, cols, lev, is_left, emit):
    wc_ref, wl_ref, _ = w_refs
    start = pl.multiple_of(jnp.where(is_left, cols, 0), LANES)

    def seam(s):
        if s not in (1, 2, 3):
            return
        high = vh[s, :, pl.ds(start, BLOCK)]
        low = vl[s, :, pl.ds(start, BLOCK)]
        band = slice(s * BLOCK, (s + 1) * BLOCK)
        new = mm(high, wc_ref[band]) + mm(low, wc_ref[band]) + mm(high, wl_ref[band])
        if s > 1:
            d = new - lev[:, cols + 2 * LANES :]
            emit(s - 1, 0, jnp.where(is_left, 0.0, d[:, :LANES]))
            emit(s - 1, cols + LANES, jnp.where(is_left, d[:, LANES:], 0.0))
        if s < 3:
            lev[:, cols + 2 * LANES :] = new

    return seam


def band_refs(late_ref):
    size = LEVELS * BLOCK
    return [late_ref.at[i * size : (i + 1) * size] for i in range(3)]


def inner_kernel(own_ref, late_ref, dog_ref, hess_ref, rim_ref, vh, vl, lev, d1, d2):
    _, rows, cols = dog_ref.shape
    _, col = mesh_place()
    is_left = col == 0
    diffs = {1: d1, 2: d2}
    tall = rows + 2 * PAD
    mid_rows = rows - 2 * RIM
    rim_tall = RIM + 2 * PAD

    def rows_of(part):
        own = own_ref[:, part]
        return mm(lh, jnp.concatenate([own, own[:rows]], axis=0))

    def emit(k, at, d):
        to = slice(at, at + d.shape[1])
        rim_ref[k, :rim_tall, to] = d[:rim_tall]
        rim_ref[k, rim_tall:, to] = d[tall - rim_tall :]
        if 0 < at <= cols:
            mid = d[PAD + RIM : PAD + RIM + mid_rows]
            dog_ref[k, RIM : RIM + mid_rows, at - LANES : at - LANES + BLOCK] = (20.0 * mid).astype(BF16)
        if k in diffs:
            diffs[k][:, to] = d

    def after_group(m, first, count):
        def put(t, value):
            hess_ref[m, RIM : RIM + mid_rows, t * LANES : (t + 1) * LANES] = value

        hess_tiles(diffs[m + 1], RIM, mid_rows, first, count, 5000.0, put)

    first = 3 * LEVELS * BLOCK
    lh = late_ref[first : first + LEVELS * tall, : 3 * rows]
    place_rows(vh, vl, rows_of, cols, is_left)
    w_refs = band_refs(late_ref)
    seam = seam_filter(vh, vl, w_refs, cols, lev, is_left, emit)
    filter_columns(vh, vl, w_refs, 4, cols, lev, emit, after_group, seam)


def outer_kernel(last_row, one_hop, message_ref, late_ref, rim_ref, dog_in, hess_in, dog_ref, hess_ref, *scratch):
    row, _ = mesh_place()
    from_above = (row % 2 == 1) if one_hop else (row % 2 == 0)
    for above in (True, False):

        @pl.when(from_above if above else jnp.logical_not(from_above))
        def _():
            outer_side(last_row, above, message_ref, late_ref, rim_ref, dog_ref, hess_ref, *scratch)


def outer_side(last_row, above, message_ref, late_ref, rim_ref, dog_ref, hess_ref, vh, vl, lev, d1, d2):
    _, rows, cols = dog_ref.shape
    row, col = mesh_place()
    is_left = col == 0
    diffs = {1: d1, 2: d2}
    rim_tall = RIM + 2 * PAD
    skip = PAD - 1 if above else PAD + 1
    first = 0 if above else rim_tall
    outs = slice(0, RIM) if above else slice(rows - RIM, rows)
    height = LEVELS * RIM
    start = 3 * LEVELS * BLOCK + LEVELS * (rows + 2 * PAD) + (0 if above else 2 * height)
    lt_high = late_ref[start : start + height, :MESSAGE]
    lt_low = late_ref[start + height : start + 2 * height, :MESSAGE]

    def rows_of(part):
        return mm(lt_high, message_ref[:, part]) + mm(lt_low, message_ref[:, part])

    def emit(k, at, d):
        to = slice(at, at + d.shape[1])
        zero = lambda count: jnp.zeros((count, d.shape[1]), F32)
        total = rim_ref[k, first : first + rim_tall, to] + jnp.concatenate(
            [zero(skip), d, zero(rim_tall - RIM - skip)], axis=0
        )
        if 0 < at <= cols:
            dog_ref[k, outs, at - LANES : at - LANES + BLOCK] = (20.0 * total[PAD : PAD + RIM]).astype(BF16)
        if k in diffs:
            d = diffs[k]
            if above:
                d[:PAD, to] = jnp.where(row == 0, 0.0, total[:PAD])
                d[PAD:, to] = total[PAD:]
            else:
                d[: rim_tall - PAD, to] = total[: rim_tall - PAD]
                d[rim_tall - PAD :, to] = jnp.where(row == last_row, 0.0, total[rim_tall - PAD :])

    def after_group(m, tile, count):
        def put(t, value):
            hess_ref[m, outs, t * LANES : (t + 1) * LANES] = value

        hess_tiles(diffs[m + 1], 0, RIM, tile, count, 5000.0, put)

    place_rows(vh, vl, rows_of, cols, is_left)
    w_refs = band_refs(late_ref)
    seam = seam_filter(vh, vl, w_refs, cols, lev, is_left, emit)
    filter_columns(vh, vl, w_refs, 8, cols, lev, emit, after_group, seam)


def coarse_kernel(last_row, keep_ref, other_ref, fine_dog_ref, fine_hess_ref, late_ref,
                  fine_dog_hbm, fine_hess_hbm, dog_hbm, hess_hbm,
                  dog_ref, hess_ref, vh, vl, lev, d1, d2, sems):
    fine_copies = [
        pltpu.make_async_copy(fine_dog_ref, fine_dog_hbm, sems.at[0]),
        pltpu.make_async_copy(fine_hess_ref, fine_hess_hbm, sems.at[1]),
    ]
    for copy in fine_copies:
        copy.start()
    _, rows, cols = dog_ref.shape
    row, col = mesh_place()
    tall = rows + 2 * PAD
    diffs = {1: d1, 2: d2}
    is_left = col == 0
    half = cols // 2
    zero = jnp.zeros((tall, LANES), BF16)
    for s in range(LEVELS):
        for ref in (vh, vl):
            ref[s, :, :LANES] = zero
            ref[s, :, LANES + cols :] = zero
    zero = jnp.zeros((tall, LANES), F32)
    for d in (d1, d2):
        d[:, :LANES] = zero
        d[:, LANES + cols :] = zero

    strip_rows = keep_ref.shape[0]
    lh = late_ref[late_ref.shape[0] - LEVELS * tall :, : 3 * strip_rows]
    for at in range(0, cols, BLOCK):
        source = slice(at % half, at % half + BLOCK)
        first = is_left if at < half else jnp.logical_not(is_left)
        value = jnp.where(first, keep_ref[:, source], other_ref[:, source])
        if at in (half - BLOCK, half):
            extra = jnp.where(first, other_ref[:, half:], keep_ref[:, half:])
            none = jnp.zeros(extra.shape, F32)
            value = value + jnp.concatenate([none, extra] if at < half else [extra, none], axis=1)
        high, low = split(value)
        stack = jnp.concatenate([high, low, high], axis=0)
        value = mm(lh, stack)
        to = slice(LANES + at, LANES + at + BLOCK)
        for s in range(LEVELS):
            vh[s, :, to], vl[s, :, to] = split(value[s * tall : (s + 1) * tall])

    def emit(k, at, d):
        dog_ref[k, :, at - LANES : at - LANES + BLOCK] = (80.0 * d[PAD : PAD + rows]).astype(BF16)
        if k in diffs:
            to = slice(at, at + BLOCK)
            diffs[k][:PAD, to] = jnp.where((row == 0) & (col == 0), 0.0, d[:PAD])
            diffs[k][PAD : PAD + rows, to] = d[PAD : PAD + rows]
            diffs[k][PAD + rows :, to] = jnp.where((row == last_row) & (col == 1), 0.0, d[PAD + rows :])

    dog_copy = pltpu.make_async_copy(dog_ref, dog_hbm, sems.at[2])
    hess_copies = [pltpu.make_async_copy(hess_ref.at[m], hess_hbm.at[m], sems.at[3 + m]) for m in range(2)]

    def after_group(m, first, count):
        def put(t, value):
            hess_ref[m, :, t * LANES : (t + 1) * LANES] = value

        if m == 1:
            dog_copy.start()
        hess_tiles(diffs[m + 1], 0, rows, first, count, 200000.0, put)
        hess_copies[m].start()

    filter_columns(vh, vl, band_refs(late_ref), 8, cols, lev, emit, after_group, lambda s: None)
    for copy in fine_copies + [dog_copy] + hess_copies:
        copy.wait()


def fine_constants(rows):
    own = np.arange(rows)
    own_inputs = np.concatenate([own, own, own])
    own_low = np.arange(3 * rows) >= 2 * rows
    nowhere = -1000
    top = np.full(MESSAGE, nowhere)
    top[: NEAR + 1] = np.append(np.arange(-NEAR, 0), -1)
    bot = np.full(MESSAGE, nowhere)
    bot[: NEAR + 1] = rows + np.append(np.arange(NEAR), 0)
    def matrix(sigma, centres, valid, inputs, use_low):
        high, low = two_parts(row_matrix(sigma, centres, inputs) * valid[:, None])
        return np.where(use_low[None, :], low.astype(np.float32), high.astype(np.float32)).astype(BF16)

    centres = np.arange(-PAD, rows + PAD)
    valid = ((centres >= -1) & (centres <= rows)).astype(np.float32)
    level = [matrix(s, centres, valid, own_inputs, own_low) for s in SIGMAS]
    halo = []
    for inputs, rim in ((top, np.arange(-1, RIM - 1)), (bot, np.arange(rows + 1 - RIM, rows + 1))):
        again = inputs.copy()
        again[NEAR] = nowhere
        for rows_in, use_low in ((inputs, False), (again, True)):
            part = np.full(MESSAGE, use_low)
            halo += [matrix(s, rim, np.ones(RIM, np.float32), rows_in, part) for s in SIGMAS]
    count = rows // 2 + 2 * (REACH + 1)
    index = np.arange(-(-count // 8) * 8)
    base = matrix(SIGMAS[-1], 2 * (index - REACH - 1), (index < count).astype(np.float32), own_inputs, own_low)
    strip_rows = -(-(rows // 4 + 2 * (REACH + 1)) // 16) * 16
    return np.concatenate(level), np.concatenate(halo), base, strip_rows


def coarse_constants(strip, padded):
    inputs = np.arange(padded) - REACH - 1
    centres = np.arange(-PAD, strip + PAD)
    valid = ((centres >= -1) & (centres <= strip)).astype(np.float32)
    parts = []
    for s in SIGMAS:
        high, low = two_parts(row_matrix(s, centres, inputs) * valid[:, None])
        parts.append(np.concatenate([high, high, low], axis=1))
    return np.concatenate(parts)


def joined(matrices, columns=BLOCK):
    return np.concatenate(
        [np.pad(m.reshape(-1, m.shape[-1]).astype(np.float32), ((0, 0), (0, columns - m.shape[-1]))) for m in matrices]
    ).astype(BF16)


def vmem_specs(count):
    return [pl.BlockSpec(memory_space=pltpu.VMEM) for _ in range(count)]


def far_specs(count):
    return [pl.BlockSpec(memory_space=pltpu.HBM) for _ in range(count)]


def limit(mib):
    return pltpu.CompilerParams(vmem_limit_bytes=mib * 2**20)


def like(value):
    return jax.ShapeDtypeStruct(value.shape, value.dtype)


def far(value):
    return pltpu.with_memory_space_constraint(jnp.asarray(value), pltpu.HBM)


def local(image):
    rows, cols = image.shape
    row_count = lax.axis_size("row")
    strip = rows // 4
    wide = cols + LANES
    tall = rows + 2 * PAD
    small = strip + 2 * PAD
    lh, lt, bm, strip_rows = fine_constants(rows)
    cw = coarse_constants(strip, strip_rows)
    bands = [column_weights(s, 1) for s in SIGMAS]
    wc, wl, we = (np.stack([b[i] for b in bands]) for i in range(3))
    early = jnp.asarray(joined([bm, *column_weights(SIGMAS[-1], 2)]))
    late = jnp.asarray(joined([wc, wl, we, lh, lt, cw]))
    base_rows = bm.shape[0]
    own_shape = jax.ShapeDtypeStruct((2 * rows, wide), BF16)
    message = jax.ShapeDtypeStruct((MESSAGE, wide), BF16)

    side = pl.pallas_call(
        border_kernel,
        out_shape=jax.ShapeDtypeStruct((rows, LANES), F32),
        in_specs=far_specs(1),
        out_specs=vmem_specs(1)[0],
        scratch_shapes=[pltpu.SemaphoreType.DMA],
        compiler_params=limit(1),
        cost_estimate=pl.CostEstimate(flops=2 * 10**9, bytes_accessed=10**7, transcendentals=0),
        name="border",
    )(far(image))
    side = lax.ppermute(side, "col", [(0, 1), (1, 0)])
    own, to_even, to_odd, base = pl.pallas_call(
        send_kernel,
        out_shape=(own_shape, message, message, jax.ShapeDtypeStruct((base_rows, cols // 2 + LANES), F32)),
        in_specs=vmem_specs(2),
        out_specs=tuple(vmem_specs(4)),
        scratch_shapes=[
            pltpu.VMEM((base_rows, cols + 2 * LANES), BF16),
            pltpu.VMEM((base_rows, cols + 2 * LANES), BF16),
        ],
        compiler_params=limit(6),
        cost_estimate=pl.CostEstimate(flops=10**9, bytes_accessed=10**6, transcendentals=0),
        name="send",
    )(image, early)
    own, to_even, to_odd = pl.pallas_call(
        side_kernel,
        out_shape=(own_shape, message, message),
        in_specs=vmem_specs(4),
        out_specs=tuple(vmem_specs(3)),
        input_output_aliases={1: 0, 2: 1, 3: 2},
        compiler_params=limit(4),
        name="side",
    )(side, own, to_even, to_odd)

    def swap(value, first):
        pairs = [(i, i + 1) for i in range(first, row_count - 1, 2)]
        return lax.ppermute(value, "row", pairs + [(j, i) for i, j in pairs])

    even, odd = swap(to_even, 0), swap(to_odd, 1)

    fine_shapes = (
        jax.ShapeDtypeStruct((4, rows, cols), BF16),
        jax.ShapeDtypeStruct((2, rows, cols), BF16),
    )
    coarse_shapes = (
        jax.ShapeDtypeStruct((4, strip, cols), BF16),
        jax.ShapeDtypeStruct((2, strip, cols), BF16),
    )

    def scratch(count, height, seam):
        padded_cols = cols + 2 * LANES
        return [
            pltpu.VMEM((LEVELS, height, padded_cols), BF16),
            pltpu.VMEM((LEVELS, height, padded_cols), BF16),
            pltpu.VMEM((height, padded_cols + seam), F32),
            pltpu.VMEM((count, padded_cols), F32),
            pltpu.VMEM((count, padded_cols), F32),
        ]

    rim_tall = RIM + 2 * PAD
    dog_fine, hess_fine, rim = pl.pallas_call(
        inner_kernel,
        out_shape=(*fine_shapes, jax.ShapeDtypeStruct((4, 2 * rim_tall, cols + 2 * LANES), F32)),
        in_specs=vmem_specs(2),
        out_specs=tuple(vmem_specs(3)),
        scratch_shapes=scratch(tall, tall, BLOCK),
        compiler_params=limit(18),
        cost_estimate=pl.CostEstimate(flops=2 * 10**9, bytes_accessed=10**7, transcendentals=0),
        name="inner",
    )(own, late)

    def finish(one_hop, message, dog, hess):
        return pl.pallas_call(
            functools.partial(outer_kernel, row_count - 1, one_hop),
            out_shape=fine_shapes,
            in_specs=vmem_specs(5),
            out_specs=tuple(vmem_specs(2)),
            scratch_shapes=scratch(rim_tall, RIM, BLOCK),
            input_output_aliases={3: 0, 4: 1},
            compiler_params=limit(12),
            cost_estimate=pl.CostEstimate(flops=10**9, bytes_accessed=10**6, transcendentals=0),
            name="outer",
        )(message, late, rim, dog, hess)

    dog_fine, hess_fine = finish(True, even, dog_fine, hess_fine)

    keep, send = pl.pallas_call(
        functools.partial(base_kernel, row_count, rows // 2),
        out_shape=(
            jax.ShapeDtypeStruct((strip_rows, cols // 2 + LANES), F32),
            jax.ShapeDtypeStruct((strip_rows, cols // 2 + LANES), F32),
        ),
        in_specs=vmem_specs(3) + [pl.BlockSpec(memory_space=pl.ANY)],
        out_specs=tuple(vmem_specs(2)),
        scratch_shapes=[pltpu.VMEM((base_rows, LANES), F32)],
        compiler_params=limit(4),
        name="base",
    )(base, even, odd, hess_fine)
    other = lax.ppermute(send, "col", [(0, 1), (1, 0)])
    dog_fine, hess_fine = finish(False, odd, dog_fine, hess_fine)

    return pl.pallas_call(
        functools.partial(coarse_kernel, row_count - 1),
        out_shape=fine_shapes + coarse_shapes,
        in_specs=vmem_specs(5),
        out_specs=tuple(far_specs(4)),
        scratch_shapes=[
            pltpu.VMEM((4, strip, cols), BF16),
            pltpu.VMEM((2, strip, cols), BF16),
            *scratch(small, small, 0),
            pltpu.SemaphoreType.DMA((5,)),
        ],
        compiler_params=limit(12),
        name="coarse",
    )(keep, other, dog_fine, hess_fine, late)


def solution(mesh):
    return jax.shard_map(
        local,
        mesh=mesh,
        in_specs=(P(("slab", "row"), "col"),),
        out_specs=(
            P(None, ("slab", "row"), "col"),
            P(None, ("slab", "row"), "col"),
            P(None, ("slab", "row", "col"), None),
            P(None, ("slab", "row", "col"), None),
        ),
        check_vma=False,
    )
```

```python
import functools

import jax
import jax.numpy as jnp
import numpy as np
from jax import lax
from jax.experimental import pallas as pl
from jax.experimental.pallas import tpu as pltpu
from jax.sharding import PartitionSpec as P

SIGMAS = [1.6 * 2.0 ** (k / 4.0) for k in range(5)]
LEVELS = len(SIGMAS)
REACH = 12
LANES = 128
BLOCK = 256
PAD = 8
RIM = 16
NEAR = REACH + 1
SPAN = 19
PART = 10
MESSAGE = NEAR + 1 + PART
BF16 = jnp.bfloat16
F32 = jnp.float32


def taps(sigma):
    offset = np.arange(2 * REACH + 1, dtype=np.float64) - REACH
    weights = np.exp(-offset * offset / (2.0 * sigma * sigma))
    return (weights / weights.sum()).astype(np.float32)


def two_parts(matrix):
    high = np.asarray(matrix, np.float32).astype(BF16)
    low = (np.asarray(matrix, np.float32) - high.astype(np.float32)).astype(BF16)
    return high, low


def tap_at(sigma, index):
    weights = taps(sigma)
    inside = (index >= 0) & (index <= 2 * REACH)
    return np.where(inside, weights[np.clip(index, 0, 2 * REACH)], np.float32(0.0))


def row_matrix(sigma, centres, inputs):
    return tap_at(sigma, inputs[None, :] - centres[:, None] + REACH)


def column_weights(sigma, step):
    width = BLOCK
    out = np.arange(BLOCK // step)[None, :] * step
    high, low = two_parts(tap_at(sigma, np.arange(width)[:, None] - out + REACH))
    lane = np.arange(LANES)[:, None]
    right = np.where(lane < REACH, tap_at(sigma, width + lane - out + REACH), 0.0)
    left = np.where(lane >= LANES - REACH, tap_at(sigma, lane - LANES - out + REACH), 0.0)
    edge_high, edge_low = two_parts(right + left)
    edge = np.concatenate([edge_high.astype(np.float32), edge_high.astype(np.float32)])
    edge[:LANES] += np.roll(edge_low.astype(np.float32), 32, axis=0)
    return high, low, edge.astype(BF16)


def split(value):
    high = value.astype(BF16)
    low = (value - high.astype(F32)).astype(BF16)
    return high, low


def mm(a, b):
    return jnp.dot(a, b, preferred_element_type=F32)


def edge_pair(high_left, high_right, low_left, low_right):
    lane = lax.broadcasted_iota(jnp.int32, high_left.shape, 1)
    eh = jnp.where(lane < LANES // 2, high_right, high_left)
    el = jnp.where(lane < LANES // 2, low_right, low_left)
    again = pltpu.roll(eh.astype(F32), 32, 1).astype(BF16)
    eh = jnp.where((lane >= 16) & (lane < 64), again, eh)
    return jnp.concatenate([eh, el], axis=1)


def edge_columns(high, low, at, width):
    left, right = slice(at - LANES, at), slice(at + width, at + width + LANES)
    return edge_pair(high[:, left], high[:, right], low[:, left], low[:, right])


def hess_tiles(d, top, rows, first_tile, count, gain, put):
    tall = rows + 2 * PAD
    lane = lax.broadcasted_iota(jnp.int32, (rows, LANES), 1)
    mid, slope, total = {}, {}, {}
    back, ahead = {}, {}

    def load(t):
        lanes = slice((first_tile + t + 1) * LANES, (first_tile + t + 2) * LANES)
        value = d[top : top + tall, lanes]
        up, down = pltpu.roll(value, 1, 0)[PAD : PAD + rows], pltpu.roll(value, tall - 1, 0)[PAD : PAD + rows]
        mid[t] = value[PAD : PAD + rows]
        slope[t], total[t] = down - up, up + down
        if t < count:
            back[t] = [pltpu.roll(v, 1, 1) for v in (mid[t], slope[t])]
        if t >= 0:
            ahead[t] = [pltpu.roll(v, LANES - 1, 1) for v in (mid[t], slope[t])]

    load(-1)
    load(0)
    for t in range(count):
        load(t + 1)
        before = [jnp.where(lane == 0, a, b) for a, b in zip(back[t - 1], back[t])]
        after = [jnp.where(lane == LANES - 1, a, b) for a, b in zip(ahead[t + 1], ahead[t])]
        twice = 2.0 * mid[t]
        dxx = after[0] + before[0] - twice
        dyy = total[t] - twice
        dxy = (after[1] - before[1]) * 0.25
        put(first_tile + t, (gain * (dxx * dyy - dxy * dxy)).astype(BF16))


def mesh_place():
    return lax.axis_index("row"), lax.axis_index("col")


def border_kernel(x_hbm, side_ref, sem):
    _, col = mesh_place()
    start = pl.multiple_of(jnp.where(col == 0, x_hbm.shape[1] - LANES, 0), LANES)
    copy = pltpu.make_async_copy(x_hbm.at[:, pl.ds(start, LANES)], side_ref, sem)
    copy.start()
    copy.wait()


def build_message(own_ref, part, rows, to):
    up_near = own_ref[:rows, to].astype(F32)[:NEAR]
    down_near = own_ref[:rows, to].astype(F32)[rows - NEAR :]
    up_low = own_ref[rows:, to].astype(F32)[:1]
    down_low = own_ref[rows:, to].astype(F32)[rows - 1 :]
    up = jnp.concatenate([up_near, up_low, part[0]], axis=0)
    down = jnp.concatenate([down_near, down_low, part[1]], axis=0)
    return up, down


def send_kernel(x_ref, early_ref, own_ref, even_ref, odd_ref, base_ref, bvh, bvl):
    row, col = mesh_place()
    rows, cols = x_ref.shape
    half = cols // 2
    base_rows = base_ref.shape[0]
    is_left = col == 0
    even = row % 2 == 0
    bm = early_ref[:base_rows, : 3 * rows]
    dc, dl, de = (early_ref[base_rows + i * BLOCK : base_rows + (i + 1) * BLOCK, : BLOCK // 2] for i in range(3))

    zero = jnp.zeros((base_rows, LANES), BF16)
    for ref in (bvh, bvl):
        ref[:, :LANES] = zero
        ref[:, LANES + cols :] = zero
    for at in range(0, cols, BLOCK):
        high, low = split(x_ref[:, at : at + BLOCK])
        own_ref[:rows, at : at + BLOCK] = high
        own_ref[rows:, at : at + BLOCK] = low
        value = mm(bm, jnp.concatenate([high, low, high], axis=0))
        to = slice(LANES + at, LANES + at + BLOCK)
        bvh[:, to], bvl[:, to] = split(value)
    first, last = slice(LANES, 2 * LANES), slice(cols, cols + LANES)
    pick = lambda ref: (
        jnp.where(is_left, ref[:, last].astype(F32), 0.0).astype(BF16),
        jnp.where(is_left, 0.0, ref[:, first].astype(F32)).astype(BF16),
    )
    beyond = edge_pair(*pick(bvh), *pick(bvl))
    group = 4
    for g in range(0, cols // BLOCK, group):
        ats = [LANES + BLOCK * (g + i) for i in range(group)]
        high = jnp.concatenate([bvh[:, at : at + BLOCK] for at in ats], axis=0)
        low = jnp.concatenate([bvl[:, at : at + BLOCK] for at in ats], axis=0)
        edge = jnp.concatenate([edge_columns(bvh, bvl, at, BLOCK) for at in ats], axis=0)
        value = mm(high, dc) + mm(low, dc) + mm(high, dl) + mm(edge, de)
        for i in range(group):
            base_ref[:, (g + i) * LANES : (g + i + 1) * LANES] = value[i * base_rows : (i + 1) * base_rows]
    base_ref[:, half:] = mm(beyond, de)

    first_up = REACH + 1 - 6
    first_down = REACH + 1 + SPAN
    for at in range(0, cols + LANES, LANES):
        to = slice(at, at + LANES)
        if at < cols:
            lanes = slice(at % half, at % half + LANES)
            skip = PART * (at // half)
            part = [base_ref[f + skip : f + skip + PART, lanes] for f in (first_up, first_down)]
        else:
            part = [
                base_ref[f : f + PART, half:] + pltpu.roll(base_ref[f + PART : f + 2 * PART, half:], LANES // 2, 1)
                for f in (first_up, first_down)
            ]
        up, down = build_message(own_ref, part, rows, to)
        if at == cols:
            index = lax.broadcasted_iota(jnp.int32, up.shape, 0)
            up = jnp.where(index > NEAR, up, 0.0)
            down = jnp.where(index > NEAR, down, 0.0)
        even_ref[:, to] = jnp.where(even, down, up).astype(BF16)
        odd_ref[:, to] = jnp.where(even, up, down).astype(BF16)


def side_kernel(side_ref, own_in, even_in, odd_in, own_ref, even_ref, odd_ref):
    row, _ = mesh_place()
    rows = own_ref.shape[0] // 2
    cols = own_ref.shape[1] - LANES
    even = row % 2 == 0
    high, low = split(side_ref[...])
    own_ref[:rows, cols:] = high
    own_ref[rows:, cols:] = low
    high, low = high.astype(F32), low.astype(F32)
    none = jnp.zeros((PART, LANES), F32)
    up = jnp.concatenate([high[:NEAR], low[:1], none], axis=0)
    down = jnp.concatenate([high[rows - NEAR :], low[rows - 1 :], none], axis=0)
    index = lax.broadcasted_iota(jnp.int32, up.shape, 0)
    for old, ref, a, b in ((even_in, even_ref, down, up), (odd_in, odd_ref, up, down)):
        kept = old[:, cols:].astype(F32)
        ref[:, cols:] = jnp.where(index > NEAR, kept, jnp.where(even, a, b)).astype(BF16)


def base_kernel(row_count, tile_base, base_ref, even_ref, odd_ref, _, keep_ref, send_ref, sum_ref):
    row, col = mesh_place()
    base_rows, wide = base_ref.shape
    half = wide - LANES
    count = keep_ref.shape[0]
    shift = tile_base // 2
    even = row % 2 == 0
    is_left = col == 0
    index = lax.broadcasted_iota(jnp.int32, (base_rows, LANES), 0)
    lane = lax.broadcasted_iota(jnp.int32, (PART, LANES), 1)
    outside = (lane >= LANES // 4) & (lane < 3 * LANES // 4)
    place = row * tile_base - REACH - 1 + index
    inside = (place >= 0) & (place < row_count * tile_base)
    first_bot = tile_base + REACH + 1 - 6

    def parts(ref_a, ref_b, at):
        def rows_of(lanes):
            a, b = ref_a[:, lanes].astype(F32), ref_b[:, lanes].astype(F32)
            return jnp.where(even, a, b)[NEAR + 1 :]

        if at < half:
            both = [rows_of(slice(at, at + LANES)), rows_of(slice(half + at, half + at + LANES))]
        else:
            value = rows_of(slice(2 * half, 2 * half + LANES))
            both = [jnp.where(outside, 0.0, v) for v in (value, pltpu.roll(value, LANES // 2, 1))]
        return jnp.concatenate([both[0], both[1][: SPAN - PART]], axis=0)

    for at in range(0, wide, LANES):
        to = slice(at, at + LANES)
        sum_ref[...] = base_ref[:, to]
        sum_ref[:SPAN, :] += parts(odd_ref, even_ref, at)
        sum_ref[first_bot : first_bot + SPAN, :] += parts(even_ref, odd_ref, at)
        total = jnp.where(inside, sum_ref[...], 0.0)
        keep_ref[:, to] = jnp.where(is_left, total[:count], total[shift : shift + count])
        send_ref[:, to] = jnp.where(is_left, total[shift : shift + count], total[:count])


def filter_columns(vh, vl, w_refs, group, cols, lev, emit, after_group, after_level):
    wc_ref, wl_ref, we_ref = w_refs
    tall = vh.shape[1]
    for s in range(LEVELS):
        band = slice(s * BLOCK, (s + 1) * BLOCK)
        for g in range(0, cols // BLOCK, group):
            ats = [LANES + BLOCK * (g + i) for i in range(group)]
            high = jnp.concatenate([vh[s, :, at : at + BLOCK] for at in ats], axis=0)
            low = jnp.concatenate([vl[s, :, at : at + BLOCK] for at in ats], axis=0)
            edge = jnp.concatenate([edge_columns(vh.at[s], vl.at[s], at, BLOCK) for at in ats], axis=0)
            value = (
                mm(high, wc_ref[band]) + mm(low, wc_ref[band]) + mm(high, wl_ref[band]) + mm(edge, we_ref[band])
            )
            for i, at in enumerate(ats):
                new = value[i * tall : (i + 1) * tall]
                if s > 0:
                    emit(s - 1, at, new - lev[:, at : at + BLOCK])
                if s + 1 < LEVELS:
                    lev[:, at : at + BLOCK] = new
            if s >= 3:
                after_group(s - 3, g * BLOCK // LANES, group * BLOCK // LANES)
        after_level(s)


def place_rows(vh, vl, rows_of, cols, is_left):
    tall = vh.shape[1]
    for at in range(0, cols, BLOCK):
        value = rows_of(slice(at, at + BLOCK))
        to = slice(LANES + at, LANES + at + BLOCK)
        for s in range(LEVELS):
            vh[s, :, to], vl[s, :, to] = split(value[s * tall : (s + 1) * tall])
    value = rows_of(slice(cols, cols + LANES))
    left, right = slice(0, LANES), slice(LANES + cols, 2 * LANES + cols)
    for s in range(LEVELS):
        part = value[s * tall : (s + 1) * tall]
        vh[s, :, left], vl[s, :, left] = split(jnp.where(is_left, 0.0, part))
        vh[s, :, right], vl[s, :, right] = split(jnp.where(is_left, part, 0.0))


def seam_filter(vh, vl, w_refs, cols, lev, is_left, emit):
    wc_ref, wl_ref, _ = w_refs
    start = pl.multiple_of(jnp.where(is_left, cols, 0), LANES)

    def seam(s):
        if s not in (1, 2, 3):
            return
        high = vh[s, :, pl.ds(start, BLOCK)]
        low = vl[s, :, pl.ds(start, BLOCK)]
        band = slice(s * BLOCK, (s + 1) * BLOCK)
        new = mm(high, wc_ref[band]) + mm(low, wc_ref[band]) + mm(high, wl_ref[band])
        if s > 1:
            d = new - lev[:, cols + 2 * LANES :]
            emit(s - 1, 0, jnp.where(is_left, 0.0, d[:, :LANES]))
            emit(s - 1, cols + LANES, jnp.where(is_left, d[:, LANES:], 0.0))
        if s < 3:
            lev[:, cols + 2 * LANES :] = new

    return seam


def band_refs(late_ref):
    size = LEVELS * BLOCK
    return [late_ref.at[i * size : (i + 1) * size] for i in range(3)]


def inner_kernel(own_ref, late_ref, dog_ref, hess_ref, rim_ref, vh, vl, lev, d1, d2):
    _, rows, cols = dog_ref.shape
    _, col = mesh_place()
    is_left = col == 0
    diffs = {1: d1, 2: d2}
    mid_rows = rows - 2 * RIM
    rim_tall = RIM + PAD

    def rows_of(part):
        own = own_ref[:, part]
        return mm(lh, jnp.concatenate([own, own[:rows]], axis=0))

    def emit(k, at, d):
        to = slice(at, at + d.shape[1])
        rim_ref[k, :rim_tall, to] = d[:rim_tall]
        rim_ref[k, rim_tall:, to] = d[rows - rim_tall :]
        if 0 < at <= cols:
            mid = d[RIM : RIM + mid_rows]
            dog_ref[k, RIM : RIM + mid_rows, at - LANES : at - LANES + BLOCK] = (20.0 * mid).astype(BF16)
        if k in diffs:
            diffs[k][:, to] = d

    def after_group(m, first, count):
        def put(t, value):
            hess_ref[m, RIM : RIM + mid_rows, t * LANES : (t + 1) * LANES] = value

        hess_tiles(diffs[m + 1], RIM - PAD, mid_rows, first, count, 5000.0, put)

    first = 3 * LEVELS * BLOCK
    lh = late_ref[first : first + LEVELS * rows, : 3 * rows]
    place_rows(vh, vl, rows_of, cols, is_left)
    w_refs = band_refs(late_ref)
    seam = seam_filter(vh, vl, w_refs, cols, lev, is_left, emit)
    filter_columns(vh, vl, w_refs, 4, cols, lev, emit, after_group, seam)


def outer_kernel(last_row, one_hop, message_ref, own_ref, late_ref, rim_ref, dog_in, hess_in, dog_ref, hess_ref, *scratch):
    row, _ = mesh_place()
    from_above = (row % 2 == 1) if one_hop else (row % 2 == 0)
    for above in (True, False):

        @pl.when(from_above if above else jnp.logical_not(from_above))
        def _():
            outer_side(last_row, above, message_ref, own_ref, late_ref, rim_ref, dog_ref, hess_ref, *scratch)


def outer_side(last_row, above, message_ref, own_ref, late_ref, rim_ref, dog_ref, hess_ref, vh, vl, lev, d1, d2):
    _, rows, cols = dog_ref.shape
    row, col = mesh_place()
    is_left = col == 0
    diffs = {1: d1, 2: d2}
    rim_tall = RIM + 2 * PAD
    skip = PAD - 1 if above else PAD + 1
    outs = slice(0, RIM) if above else slice(rows - RIM, rows)
    height = LEVELS * RIM
    start = 3 * LEVELS * BLOCK + LEVELS * rows + (0 if above else 2 * height)
    lt_high = late_ref[start : start + height, : 3 * RIM + MESSAGE]
    lt_low = late_ref[start + height : start + 2 * height, :MESSAGE]
    own_first = 0 if above else rows - RIM

    def rows_of(part):
        message = message_ref[:, part]
        high = own_ref[own_first : own_first + RIM, part]
        low = own_ref[rows + own_first : rows + own_first + RIM, part]
        return mm(lt_high, jnp.concatenate([high, low, high, message], axis=0)) + mm(lt_low, message)

    def emit(k, at, d):
        to = slice(at, at + d.shape[1])
        zero = lambda count: jnp.zeros((count, d.shape[1]), F32)
        total = jnp.concatenate([zero(skip), d, zero(rim_tall - RIM - skip)], axis=0)
        if above:
            total = jnp.concatenate([total[:PAD], total[PAD:] + rim_ref[k, : rim_tall - PAD, to]], axis=0)
        else:
            own = total[: rim_tall - PAD] + rim_ref[k, rim_tall - PAD :, to]
            total = jnp.concatenate([own, total[rim_tall - PAD :]], axis=0)
        if 0 < at <= cols:
            dog_ref[k, outs, at - LANES : at - LANES + BLOCK] = (20.0 * total[PAD : PAD + RIM]).astype(BF16)
        if k in diffs:
            d = diffs[k]
            if above:
                d[:PAD, to] = jnp.where(row == 0, 0.0, total[:PAD])
                d[PAD:, to] = total[PAD:]
            else:
                d[: rim_tall - PAD, to] = total[: rim_tall - PAD]
                d[rim_tall - PAD :, to] = jnp.where(row == last_row, 0.0, total[rim_tall - PAD :])

    def after_group(m, tile, count):
        def put(t, value):
            hess_ref[m, outs, t * LANES : (t + 1) * LANES] = value

        hess_tiles(diffs[m + 1], 0, RIM, tile, count, 5000.0, put)

    place_rows(vh, vl, rows_of, cols, is_left)
    w_refs = band_refs(late_ref)
    seam = seam_filter(vh, vl, w_refs, cols, lev, is_left, emit)
    filter_columns(vh, vl, w_refs, 8, cols, lev, emit, after_group, seam)


def coarse_kernel(last_row, keep_ref, other_ref, fine_dog_ref, fine_hess_ref, late_ref,
                  fine_dog_hbm, fine_hess_hbm, dog_hbm, hess_hbm,
                  dog_ref, hess_ref, vh, vl, lev, d1, d2, sems):
    fine_copies = [
        pltpu.make_async_copy(fine_dog_ref, fine_dog_hbm, sems.at[0]),
        pltpu.make_async_copy(fine_hess_ref, fine_hess_hbm, sems.at[1]),
    ]
    for copy in fine_copies:
        copy.start()
    _, rows, cols = dog_ref.shape
    row, col = mesh_place()
    tall = rows + 2 * PAD
    diffs = {1: d1, 2: d2}
    is_left = col == 0
    half = cols // 2
    zero = jnp.zeros((tall, LANES), BF16)
    for s in range(LEVELS):
        for ref in (vh, vl):
            ref[s, :, :LANES] = zero
            ref[s, :, LANES + cols :] = zero
    zero = jnp.zeros((tall, LANES), F32)
    for d in (d1, d2):
        d[:, :LANES] = zero
        d[:, LANES + cols :] = zero

    strip_rows = keep_ref.shape[0]
    lh = late_ref[late_ref.shape[0] - LEVELS * tall :, : 3 * strip_rows]
    for at in range(0, cols, BLOCK):
        source = slice(at % half, at % half + BLOCK)
        first = is_left if at < half else jnp.logical_not(is_left)
        value = jnp.where(first, keep_ref[:, source], other_ref[:, source])
        if at in (half - BLOCK, half):
            extra = jnp.where(first, other_ref[:, half:], keep_ref[:, half:])
            none = jnp.zeros(extra.shape, F32)
            value = value + jnp.concatenate([none, extra] if at < half else [extra, none], axis=1)
        high, low = split(value)
        stack = jnp.concatenate([high, low, high], axis=0)
        value = mm(lh, stack)
        to = slice(LANES + at, LANES + at + BLOCK)
        for s in range(LEVELS):
            vh[s, :, to], vl[s, :, to] = split(value[s * tall : (s + 1) * tall])

    def emit(k, at, d):
        dog_ref[k, :, at - LANES : at - LANES + BLOCK] = (80.0 * d[PAD : PAD + rows]).astype(BF16)
        if k in diffs:
            to = slice(at, at + BLOCK)
            diffs[k][:PAD, to] = jnp.where((row == 0) & (col == 0), 0.0, d[:PAD])
            diffs[k][PAD : PAD + rows, to] = d[PAD : PAD + rows]
            diffs[k][PAD + rows :, to] = jnp.where((row == last_row) & (col == 1), 0.0, d[PAD + rows :])

    dog_copy = pltpu.make_async_copy(dog_ref, dog_hbm, sems.at[2])
    hess_copies = [pltpu.make_async_copy(hess_ref.at[m], hess_hbm.at[m], sems.at[3 + m]) for m in range(2)]

    def after_group(m, first, count):
        def put(t, value):
            hess_ref[m, :, t * LANES : (t + 1) * LANES] = value

        if m == 1:
            dog_copy.start()
        hess_tiles(diffs[m + 1], 0, rows, first, count, 200000.0, put)
        hess_copies[m].start()

    filter_columns(vh, vl, band_refs(late_ref), 8, cols, lev, emit, after_group, lambda s: None)
    for copy in fine_copies + [dog_copy] + hess_copies:
        copy.wait()


def fine_constants(rows):
    own = np.arange(rows)
    own_inputs = np.concatenate([own, own, own])
    own_low = np.arange(3 * rows) >= 2 * rows
    nowhere = -1000
    top = np.full(MESSAGE, nowhere)
    top[: NEAR + 1] = np.append(np.arange(-NEAR, 0), -1)
    bot = np.full(MESSAGE, nowhere)
    bot[: NEAR + 1] = rows + np.append(np.arange(NEAR), 0)
    def matrix(sigma, centres, valid, inputs, use_low):
        high, low = two_parts(row_matrix(sigma, centres, inputs) * valid[:, None])
        return np.where(use_low[None, :], low.astype(np.float32), high.astype(np.float32)).astype(BF16)

    level = [matrix(s, own, np.ones(rows, np.float32), own_inputs, own_low) for s in SIGMAS]
    halo = []
    for inputs, rim, near_own, outer in (
        (top, np.arange(-1, RIM - 1), own[:RIM], 0),
        (bot, np.arange(rows + 1 - RIM, rows + 1), own[rows - RIM :], RIM - 1),
    ):
        ones = np.ones(RIM, np.float32)
        alone = (np.arange(RIM) == outer).astype(np.float32)
        triple = np.concatenate([near_own, near_own, near_own])
        triple_low = np.arange(3 * RIM) >= 2 * RIM
        again = inputs.copy()
        again[NEAR] = nowhere
        for s in SIGMAS:
            beside = matrix(s, rim, alone, triple, triple_low).astype(np.float32)
            beyond = matrix(s, rim, ones, inputs, np.zeros(MESSAGE, bool)).astype(np.float32)
            halo.append(np.concatenate([beside, beyond], axis=1))
        for s in SIGMAS:
            low = matrix(s, rim, ones, again, np.ones(MESSAGE, bool)).astype(np.float32)
            halo.append(np.pad(low, ((0, 0), (0, 3 * RIM))))
    count = rows // 2 + 2 * (REACH + 1)
    index = np.arange(-(-count // 8) * 8)
    base = matrix(SIGMAS[-1], 2 * (index - REACH - 1), (index < count).astype(np.float32), own_inputs, own_low)
    strip_rows = -(-(rows // 4 + 2 * (REACH + 1)) // 16) * 16
    return np.concatenate(level), np.concatenate(halo), base, strip_rows


def coarse_constants(strip, padded):
    inputs = np.arange(padded) - REACH - 1
    centres = np.arange(-PAD, strip + PAD)
    valid = ((centres >= -1) & (centres <= strip)).astype(np.float32)
    parts = []
    for s in SIGMAS:
        high, low = two_parts(row_matrix(s, centres, inputs) * valid[:, None])
        parts.append(np.concatenate([high, high, low], axis=1))
    return np.concatenate(parts)


def joined(matrices, columns=BLOCK):
    return np.concatenate(
        [np.pad(m.reshape(-1, m.shape[-1]).astype(np.float32), ((0, 0), (0, columns - m.shape[-1]))) for m in matrices]
    ).astype(BF16)


def vmem_specs(count):
    return [pl.BlockSpec(memory_space=pltpu.VMEM) for _ in range(count)]


def far_specs(count):
    return [pl.BlockSpec(memory_space=pltpu.HBM) for _ in range(count)]


def limit(mib):
    return pltpu.CompilerParams(vmem_limit_bytes=mib * 2**20)


def like(value):
    return jax.ShapeDtypeStruct(value.shape, value.dtype)


def far(value):
    return pltpu.with_memory_space_constraint(jnp.asarray(value), pltpu.HBM)


def local(image):
    rows, cols = image.shape
    row_count = lax.axis_size("row")
    strip = rows // 4
    wide = cols + LANES
    small = strip + 2 * PAD
    lh, lt, bm, strip_rows = fine_constants(rows)
    cw = coarse_constants(strip, strip_rows)
    bands = [column_weights(s, 1) for s in SIGMAS]
    wc, wl, we = (np.stack([b[i] for b in bands]) for i in range(3))
    early = jnp.asarray(joined([bm, *column_weights(SIGMAS[-1], 2)]))
    late = jnp.asarray(joined([wc, wl, we, lh, lt, cw]))
    base_rows = bm.shape[0]
    own_shape = jax.ShapeDtypeStruct((2 * rows, wide), BF16)
    message = jax.ShapeDtypeStruct((MESSAGE, wide), BF16)

    side = pl.pallas_call(
        border_kernel,
        out_shape=jax.ShapeDtypeStruct((rows, LANES), F32),
        in_specs=far_specs(1),
        out_specs=vmem_specs(1)[0],
        scratch_shapes=[pltpu.SemaphoreType.DMA],
        compiler_params=limit(1),
        cost_estimate=pl.CostEstimate(flops=2 * 10**9, bytes_accessed=10**7, transcendentals=0),
        name="border",
    )(far(image))
    side = lax.ppermute(side, "col", [(0, 1), (1, 0)])
    own, to_even, to_odd, base = pl.pallas_call(
        send_kernel,
        out_shape=(own_shape, message, message, jax.ShapeDtypeStruct((base_rows, cols // 2 + LANES), F32)),
        in_specs=vmem_specs(2),
        out_specs=tuple(vmem_specs(4)),
        scratch_shapes=[
            pltpu.VMEM((base_rows, cols + 2 * LANES), BF16),
            pltpu.VMEM((base_rows, cols + 2 * LANES), BF16),
        ],
        compiler_params=limit(6),
        cost_estimate=pl.CostEstimate(flops=10**9, bytes_accessed=10**6, transcendentals=0),
        name="send",
    )(image, early)
    own, to_even, to_odd = pl.pallas_call(
        side_kernel,
        out_shape=(own_shape, message, message),
        in_specs=vmem_specs(4),
        out_specs=tuple(vmem_specs(3)),
        input_output_aliases={1: 0, 2: 1, 3: 2},
        compiler_params=limit(4),
        name="side",
    )(side, own, to_even, to_odd)

    def swap(value, first):
        pairs = [(i, i + 1) for i in range(first, row_count - 1, 2)]
        return lax.ppermute(value, "row", pairs + [(j, i) for i, j in pairs])

    even, odd = swap(to_even, 0), swap(to_odd, 1)

    fine_shapes = (
        jax.ShapeDtypeStruct((4, rows, cols), BF16),
        jax.ShapeDtypeStruct((2, rows, cols), BF16),
    )
    coarse_shapes = (
        jax.ShapeDtypeStruct((4, strip, cols), BF16),
        jax.ShapeDtypeStruct((2, strip, cols), BF16),
    )

    def scratch(count, height, seam):
        padded_cols = cols + 2 * LANES
        return [
            pltpu.VMEM((LEVELS, height, padded_cols), BF16),
            pltpu.VMEM((LEVELS, height, padded_cols), BF16),
            pltpu.VMEM((height, padded_cols + seam), F32),
            pltpu.VMEM((count, padded_cols), F32),
            pltpu.VMEM((count, padded_cols), F32),
        ]

    rim_tall = RIM + 2 * PAD
    dog_fine, hess_fine, rim = pl.pallas_call(
        inner_kernel,
        out_shape=(*fine_shapes, jax.ShapeDtypeStruct((4, 2 * (RIM + PAD), cols + 2 * LANES), F32)),
        in_specs=vmem_specs(2),
        out_specs=tuple(vmem_specs(3)),
        scratch_shapes=scratch(rows, rows, BLOCK),
        compiler_params=limit(18),
        cost_estimate=pl.CostEstimate(flops=2 * 10**9, bytes_accessed=10**7, transcendentals=0),
        name="inner",
    )(own, late)

    def finish(one_hop, message, dog, hess):
        return pl.pallas_call(
            functools.partial(outer_kernel, row_count - 1, one_hop),
            out_shape=fine_shapes,
            in_specs=vmem_specs(6),
            out_specs=tuple(vmem_specs(2)),
            scratch_shapes=scratch(rim_tall, RIM, BLOCK),
            input_output_aliases={4: 0, 5: 1},
            compiler_params=limit(12),
            cost_estimate=pl.CostEstimate(flops=10**9, bytes_accessed=10**6, transcendentals=0),
            name="outer",
        )(message, own, late, rim, dog, hess)

    dog_fine, hess_fine = finish(True, even, dog_fine, hess_fine)

    keep, send = pl.pallas_call(
        functools.partial(base_kernel, row_count, rows // 2),
        out_shape=(
            jax.ShapeDtypeStruct((strip_rows, cols // 2 + LANES), F32),
            jax.ShapeDtypeStruct((strip_rows, cols // 2 + LANES), F32),
        ),
        in_specs=vmem_specs(3) + [pl.BlockSpec(memory_space=pl.ANY)],
        out_specs=tuple(vmem_specs(2)),
        scratch_shapes=[pltpu.VMEM((base_rows, LANES), F32)],
        compiler_params=limit(4),
        name="base",
    )(base, even, odd, hess_fine)
    other = lax.ppermute(send, "col", [(0, 1), (1, 0)])
    dog_fine, hess_fine = finish(False, odd, dog_fine, hess_fine)

    return pl.pallas_call(
        functools.partial(coarse_kernel, row_count - 1),
        out_shape=fine_shapes + coarse_shapes,
        in_specs=vmem_specs(5),
        out_specs=tuple(far_specs(4)),
        scratch_shapes=[
            pltpu.VMEM((4, strip, cols), BF16),
            pltpu.VMEM((2, strip, cols), BF16),
            *scratch(small, small, 0),
            pltpu.SemaphoreType.DMA((5,)),
        ],
        compiler_params=limit(12),
        name="coarse",
    )(keep, other, dog_fine, hess_fine, late)


def solution(mesh):
    return jax.shard_map(
        local,
        mesh=mesh,
        in_specs=(P(("slab", "row"), "col"),),
        out_specs=(
            P(None, ("slab", "row"), "col"),
            P(None, ("slab", "row"), "col"),
            P(None, ("slab", "row", "col"), None),
            P(None, ("slab", "row", "col"), None),
        ),
        check_vma=False,
    )
```

```python
import functools

import jax
import jax.numpy as jnp
import numpy as np
from jax import lax
from jax.experimental import pallas as pl
from jax.experimental.pallas import tpu as pltpu
from jax.sharding import PartitionSpec as P


SIGMAS = [1.6 * 2.0 ** (k / 4.0) for k in range(5)]
LEVELS = len(SIGMAS)
REACH = 12
LANES = 128
BLOCK = 256
PAD = 8
RIM = 16
NEAR = REACH + 1
SPAN = 19
PART = 10
MESSAGE = NEAR + 1 + PART
BF16 = jnp.bfloat16
F32 = jnp.float32


def taps(sigma):
    offset = np.arange(2 * REACH + 1, dtype=np.float64) - REACH
    weights = np.exp(-offset * offset / (2.0 * sigma * sigma))
    return (weights / weights.sum()).astype(np.float32)


def two_parts(matrix):
    high = np.asarray(matrix, np.float32).astype(BF16)
    low = (np.asarray(matrix, np.float32) - high.astype(np.float32)).astype(BF16)
    return high, low


def tap_at(sigma, index):
    weights = taps(sigma)
    inside = (index >= 0) & (index <= 2 * REACH)
    return np.where(inside, weights[np.clip(index, 0, 2 * REACH)], np.float32(0.0))


def row_matrix(sigma, centres, inputs):
    return tap_at(sigma, inputs[None, :] - centres[:, None] + REACH)


def column_weights(sigma, step):
    width = BLOCK
    out = np.arange(BLOCK // step)[None, :] * step
    high, low = two_parts(tap_at(sigma, np.arange(width)[:, None] - out + REACH))
    lane = np.arange(LANES)[:, None]
    right = np.where(lane < REACH, tap_at(sigma, width + lane - out + REACH), 0.0)
    left = np.where(lane >= LANES - REACH, tap_at(sigma, lane - LANES - out + REACH), 0.0)
    edge_high, edge_low = two_parts(right + left)
    edge = np.concatenate([edge_high.astype(np.float32), edge_high.astype(np.float32)])
    edge[:LANES] += np.roll(edge_low.astype(np.float32), 32, axis=0)
    return high, low, edge.astype(BF16)


def split(value):
    high = value.astype(BF16)
    low = (value - high.astype(F32)).astype(BF16)
    return high, low


def mm(a, b):
    return jnp.dot(a, b, preferred_element_type=F32)


def edge_pair(high_left, high_right, low_left, low_right):
    lane = lax.broadcasted_iota(jnp.int32, high_left.shape, 1)
    eh = jnp.where(lane < LANES // 2, high_right, high_left)
    el = jnp.where(lane < LANES // 2, low_right, low_left)
    again = pltpu.roll(eh.astype(F32), 32, 1).astype(BF16)
    eh = jnp.where((lane >= 16) & (lane < 64), again, eh)
    return jnp.concatenate([eh, el], axis=1)


def edge_columns(high, low, at, width):
    left, right = slice(at - LANES, at), slice(at + width, at + width + LANES)
    return edge_pair(high[:, left], high[:, right], low[:, left], low[:, right])


def hess_tiles(d, top, rows, first_tile, count, gain, put):
    tall = rows + 2 * PAD
    lane = lax.broadcasted_iota(jnp.int32, (rows, LANES), 1)
    mid, slope, total = {}, {}, {}
    back, ahead = {}, {}

    def load(t):
        lanes = slice((first_tile + t + 1) * LANES, (first_tile + t + 2) * LANES)
        value = d[top : top + tall, lanes]
        up, down = pltpu.roll(value, 1, 0)[PAD : PAD + rows], pltpu.roll(value, tall - 1, 0)[PAD : PAD + rows]
        mid[t] = value[PAD : PAD + rows]
        slope[t], total[t] = down - up, up + down
        if t < count:
            back[t] = [pltpu.roll(v, 1, 1) for v in (mid[t], slope[t])]
        if t >= 0:
            ahead[t] = [pltpu.roll(v, LANES - 1, 1) for v in (mid[t], slope[t])]

    load(-1)
    load(0)
    for t in range(count):
        load(t + 1)
        before = [jnp.where(lane == 0, a, b) for a, b in zip(back[t - 1], back[t])]
        after = [jnp.where(lane == LANES - 1, a, b) for a, b in zip(ahead[t + 1], ahead[t])]
        twice = 2.0 * mid[t]
        dxx = after[0] + before[0] - twice
        dyy = total[t] - twice
        dxy = (after[1] - before[1]) * 0.25
        put(first_tile + t, (gain * (dxx * dyy - dxy * dxy)).astype(BF16))


def mesh_place():
    return lax.axis_index("row"), lax.axis_index("col")


def border_kernel(x_hbm, side_ref, sem):
    _, col = mesh_place()
    start = pl.multiple_of(jnp.where(col == 0, x_hbm.shape[1] - LANES, 0), LANES)
    copy = pltpu.make_async_copy(x_hbm.at[:, pl.ds(start, LANES)], side_ref, sem)
    copy.start()
    copy.wait()


def build_message(own_ref, part, rows, to):
    up_near = own_ref[:rows, to].astype(F32)[:NEAR]
    down_near = own_ref[:rows, to].astype(F32)[rows - NEAR :]
    up_low = own_ref[rows:, to].astype(F32)[:1]
    down_low = own_ref[rows:, to].astype(F32)[rows - 1 :]
    up = jnp.concatenate([up_near, up_low, part[0]], axis=0)
    down = jnp.concatenate([down_near, down_low, part[1]], axis=0)
    return up, down


def send_kernel(x_ref, early_ref, own_ref, even_ref, odd_ref, base_ref, bvh, bvl):
    row, col = mesh_place()
    rows, cols = x_ref.shape
    half = cols // 2
    base_rows = base_ref.shape[0]
    is_left = col == 0
    even = row % 2 == 0
    bm = early_ref[:base_rows, : 3 * rows]
    dc, dl, de = (early_ref[base_rows + i * BLOCK : base_rows + (i + 1) * BLOCK, : BLOCK // 2] for i in range(3))

    zero = jnp.zeros((base_rows, LANES), BF16)
    for ref in (bvh, bvl):
        ref[:, :LANES] = zero
        ref[:, LANES + cols :] = zero
    for at in range(0, cols, BLOCK):
        high, low = split(x_ref[:, at : at + BLOCK])
        own_ref[:rows, at : at + BLOCK] = high
        own_ref[rows:, at : at + BLOCK] = low
        value = mm(bm, jnp.concatenate([high, low, high], axis=0))
        to = slice(LANES + at, LANES + at + BLOCK)
        bvh[:, to], bvl[:, to] = split(value)
    first, last = slice(LANES, 2 * LANES), slice(cols, cols + LANES)
    pick = lambda ref: (
        jnp.where(is_left, ref[:, last].astype(F32), 0.0).astype(BF16),
        jnp.where(is_left, 0.0, ref[:, first].astype(F32)).astype(BF16),
    )
    beyond = edge_pair(*pick(bvh), *pick(bvl))
    group = 4
    for g in range(0, cols // BLOCK, group):
        ats = [LANES + BLOCK * (g + i) for i in range(group)]
        high = jnp.concatenate([bvh[:, at : at + BLOCK] for at in ats], axis=0)
        low = jnp.concatenate([bvl[:, at : at + BLOCK] for at in ats], axis=0)
        edge = jnp.concatenate([edge_columns(bvh, bvl, at, BLOCK) for at in ats], axis=0)
        value = mm(high, dc) + mm(low, dc) + mm(high, dl) + mm(edge, de)
        for i in range(group):
            base_ref[:, (g + i) * LANES : (g + i + 1) * LANES] = value[i * base_rows : (i + 1) * base_rows]
    base_ref[:, half:] = mm(beyond, de)

    first_up = REACH + 1 - 6
    first_down = REACH + 1 + SPAN
    for at in range(0, cols + LANES, LANES):
        to = slice(at, at + LANES)
        if at < cols:
            lanes = slice(at % half, at % half + LANES)
            skip = PART * (at // half)
            part = [base_ref[f + skip : f + skip + PART, lanes] for f in (first_up, first_down)]
        else:
            part = [
                base_ref[f : f + PART, half:] + pltpu.roll(base_ref[f + PART : f + 2 * PART, half:], LANES // 2, 1)
                for f in (first_up, first_down)
            ]
        up, down = build_message(own_ref, part, rows, to)
        if at == cols:
            index = lax.broadcasted_iota(jnp.int32, up.shape, 0)
            up = jnp.where(index > NEAR, up, 0.0)
            down = jnp.where(index > NEAR, down, 0.0)
        even_ref[:, to] = jnp.where(even, down, up).astype(BF16)
        odd_ref[:, to] = jnp.where(even, up, down).astype(BF16)


def side_kernel(side_ref, own_in, even_in, odd_in, own_ref, even_ref, odd_ref):
    row, _ = mesh_place()
    rows = own_ref.shape[0] // 2
    cols = own_ref.shape[1] - LANES
    even = row % 2 == 0
    high, low = split(side_ref[...])
    own_ref[:rows, cols:] = high
    own_ref[rows:, cols:] = low
    high, low = high.astype(F32), low.astype(F32)
    none = jnp.zeros((PART, LANES), F32)
    up = jnp.concatenate([high[:NEAR], low[:1], none], axis=0)
    down = jnp.concatenate([high[rows - NEAR :], low[rows - 1 :], none], axis=0)
    index = lax.broadcasted_iota(jnp.int32, up.shape, 0)
    for old, ref, a, b in ((even_in, even_ref, down, up), (odd_in, odd_ref, up, down)):
        kept = old[:, cols:].astype(F32)
        ref[:, cols:] = jnp.where(index > NEAR, kept, jnp.where(even, a, b)).astype(BF16)


def base_kernel(row_count, tile_base, base_ref, even_ref, _, keep_ref, send_ref, sum_ref):
    row, col = mesh_place()
    base_rows, wide = base_ref.shape
    half = wide - LANES
    count = keep_ref.shape[0]
    shift = tile_base // 2
    even = row % 2 == 0
    is_left = col == 0
    index = lax.broadcasted_iota(jnp.int32, (base_rows, LANES), 0)
    place = row * tile_base - REACH - 1 + index
    inside = (place >= 0) & (place < row_count * tile_base)
    first_bot = tile_base + REACH + 1 - 6
    for at in range(0, wide, LANES):
        to = slice(at, at + LANES)
        if at < half:
            both = [even_ref[:, lanes].astype(F32) for lanes in (to, slice(half + at, half + at + LANES))]
        else:
            both = unpack_extra(even_ref[:, 2 * half :].astype(F32))
        part = jnp.concatenate([both[0][NEAR + 1 :], both[1][NEAR + 1 : NEAR + 1 + SPAN - PART]], axis=0)
        sum_ref[...] = base_ref[:, to]
        sum_ref[:SPAN, :] += jnp.where(even, 0.0, part)
        sum_ref[first_bot : first_bot + SPAN, :] += jnp.where(even, part, 0.0)
        total = jnp.where(inside, sum_ref[...], 0.0)
        keep_ref[:, to] = jnp.where(is_left, total[:count], total[shift : shift + count])
        send_ref[:, to] = jnp.where(is_left, total[shift : shift + count], total[:count])


def unpack_extra(value):
    lane = lax.broadcasted_iota(jnp.int32, value.shape, 1)
    outside = (lane >= LANES // 4) & (lane < 3 * LANES // 4)
    return [jnp.where(outside, 0.0, v) for v in (value, pltpu.roll(value, LANES // 2, 1))]


def filter_columns(vh, vl, w_refs, group, cols, lev, emit, after_group, after_level):
    wc_ref, wl_ref, we_ref = w_refs
    tall = vh.shape[1]
    for s in range(LEVELS):
        band = slice(s * BLOCK, (s + 1) * BLOCK)
        for g in range(0, cols // BLOCK, group):
            ats = [LANES + BLOCK * (g + i) for i in range(group)]
            high = jnp.concatenate([vh[s, :, at : at + BLOCK] for at in ats], axis=0)
            low = jnp.concatenate([vl[s, :, at : at + BLOCK] for at in ats], axis=0)
            edge = jnp.concatenate([edge_columns(vh.at[s], vl.at[s], at, BLOCK) for at in ats], axis=0)
            value = (
                mm(high, wc_ref[band]) + mm(low, wc_ref[band]) + mm(high, wl_ref[band]) + mm(edge, we_ref[band])
            )
            for i, at in enumerate(ats):
                new = value[i * tall : (i + 1) * tall]
                if s > 0:
                    emit(s - 1, at, new - lev[:, at : at + BLOCK])
                if s + 1 < LEVELS:
                    lev[:, at : at + BLOCK] = new
            if s >= 3:
                after_group(s - 3, g * BLOCK // LANES, group * BLOCK // LANES)
        after_level(s)


def place_rows(vh, vl, rows_of, cols, is_left):
    tall = vh.shape[1]
    for at in range(0, cols, BLOCK):
        value = rows_of(slice(at, at + BLOCK))
        to = slice(LANES + at, LANES + at + BLOCK)
        for s in range(LEVELS):
            vh[s, :, to], vl[s, :, to] = split(value[s * tall : (s + 1) * tall])
    value = rows_of(slice(cols, cols + LANES))
    left, right = slice(0, LANES), slice(LANES + cols, 2 * LANES + cols)
    for s in range(LEVELS):
        part = value[s * tall : (s + 1) * tall]
        vh[s, :, left], vl[s, :, left] = split(jnp.where(is_left, 0.0, part))
        vh[s, :, right], vl[s, :, right] = split(jnp.where(is_left, part, 0.0))


def seam_filter(vh, vl, w_refs, cols, lev, is_left, emit):
    wc_ref, wl_ref, _ = w_refs
    start = pl.multiple_of(jnp.where(is_left, cols, 0), LANES)

    def seam(s):
        if s not in (1, 2, 3):
            return
        high = vh[s, :, pl.ds(start, BLOCK)]
        low = vl[s, :, pl.ds(start, BLOCK)]
        band = slice(s * BLOCK, (s + 1) * BLOCK)
        new = mm(high, wc_ref[band]) + mm(low, wc_ref[band]) + mm(high, wl_ref[band])
        if s > 1:
            d = new - lev[:, cols + 2 * LANES :]
            emit(s - 1, 0, jnp.where(is_left, 0.0, d[:, :LANES]))
            emit(s - 1, cols + LANES, jnp.where(is_left, d[:, LANES:], 0.0))
        if s < 3:
            lev[:, cols + 2 * LANES :] = new

    return seam


def band_refs(late_ref):
    size = LEVELS * BLOCK
    return [late_ref.at[i * size : (i + 1) * size] for i in range(3)]


def inner_kernel(own_ref, late_ref, dog_ref, hess_ref, rim_ref, vh, vl, lev, d1, d2):
    _, rows, cols = dog_ref.shape
    _, col = mesh_place()
    is_left = col == 0
    diffs = {1: d1, 2: d2}
    mid_rows = rows - 2 * RIM
    rim_tall = RIM + PAD

    def rows_of(part):
        own = own_ref[:, part]
        return mm(lh, jnp.concatenate([own, own[:rows]], axis=0))

    def emit(k, at, d):
        to = slice(at, at + d.shape[1])
        rim_ref[k, :rim_tall, to] = d[:rim_tall]
        rim_ref[k, rim_tall:, to] = d[rows - rim_tall :]
        if 0 < at <= cols:
            mid = d[RIM : RIM + mid_rows]
            dog_ref[k, RIM : RIM + mid_rows, at - LANES : at - LANES + BLOCK] = (20.0 * mid).astype(BF16)
        if k in diffs:
            diffs[k][:, to] = d

    def after_group(m, first, count):
        def put(t, value):
            hess_ref[m, RIM : RIM + mid_rows, t * LANES : (t + 1) * LANES] = value

        hess_tiles(diffs[m + 1], RIM - PAD, mid_rows, first, count, 5000.0, put)

    first = 3 * LEVELS * BLOCK
    lh = late_ref[first : first + LEVELS * rows, : 3 * rows]
    place_rows(vh, vl, rows_of, cols, is_left)
    w_refs = band_refs(late_ref)
    seam = seam_filter(vh, vl, w_refs, cols, lev, is_left, emit)
    filter_columns(vh, vl, w_refs, 4, cols, lev, emit, after_group, seam)


def outer_kernel(last_row, one_hop, message_ref, own_ref, late_ref, rim_ref, dog_in, hess_in, dog_ref, hess_ref, *scratch):
    row, _ = mesh_place()
    from_above = (row % 2 == 1) if one_hop else (row % 2 == 0)
    for above in (True, False):

        @pl.when(from_above if above else jnp.logical_not(from_above))
        def _():
            outer_side(last_row, above, message_ref, own_ref, late_ref, rim_ref, dog_ref, hess_ref, *scratch)


def outer_side(last_row, above, message_ref, own_ref, late_ref, rim_ref, dog_ref, hess_ref, vh, vl, lev, d1, d2):
    _, rows, cols = dog_ref.shape
    row, col = mesh_place()
    is_left = col == 0
    diffs = {1: d1, 2: d2}
    rim_tall = RIM + 2 * PAD
    skip = PAD - 1 if above else PAD + 1
    outs = slice(0, RIM) if above else slice(rows - RIM, rows)
    height = LEVELS * RIM
    start = 3 * LEVELS * BLOCK + LEVELS * rows + (0 if above else 2 * height)
    lt_high = late_ref[start : start + height, : 3 * RIM + MESSAGE]
    lt_low = late_ref[start + height : start + 2 * height, :MESSAGE]
    own_first = 0 if above else rows - RIM

    def rows_of(part):
        message = message_ref[:, part]
        high = own_ref[own_first : own_first + RIM, part]
        low = own_ref[rows + own_first : rows + own_first + RIM, part]
        return mm(lt_high, jnp.concatenate([high, low, high, message], axis=0)) + mm(lt_low, message)

    def emit(k, at, d):
        to = slice(at, at + d.shape[1])
        zero = lambda count: jnp.zeros((count, d.shape[1]), F32)
        total = jnp.concatenate([zero(skip), d, zero(rim_tall - RIM - skip)], axis=0)
        if above:
            total = jnp.concatenate([total[:PAD], total[PAD:] + rim_ref[k, : rim_tall - PAD, to]], axis=0)
        else:
            own = total[: rim_tall - PAD] + rim_ref[k, rim_tall - PAD :, to]
            total = jnp.concatenate([own, total[rim_tall - PAD :]], axis=0)
        if 0 < at <= cols:
            dog_ref[k, outs, at - LANES : at - LANES + BLOCK] = (20.0 * total[PAD : PAD + RIM]).astype(BF16)
        if k in diffs:
            d = diffs[k]
            if above:
                d[:PAD, to] = jnp.where(row == 0, 0.0, total[:PAD])
                d[PAD:, to] = total[PAD:]
            else:
                d[: rim_tall - PAD, to] = total[: rim_tall - PAD]
                d[rim_tall - PAD :, to] = jnp.where(row == last_row, 0.0, total[rim_tall - PAD :])

    def after_group(m, tile, count):
        def put(t, value):
            hess_ref[m, outs, t * LANES : (t + 1) * LANES] = value

        hess_tiles(diffs[m + 1], 0, RIM, tile, count, 5000.0, put)

    place_rows(vh, vl, rows_of, cols, is_left)
    w_refs = band_refs(late_ref)
    seam = seam_filter(vh, vl, w_refs, cols, lev, is_left, emit)
    filter_columns(vh, vl, w_refs, 8, cols, lev, emit, after_group, seam)


def coarse_kernel(last_row, keep_ref, other_ref, odd_ref, odd_other_ref, fine_dog_ref, fine_hess_ref, late_ref,
                  fine_dog_hbm, fine_hess_hbm, dog_hbm, hess_hbm,
                  dog_ref, hess_ref, vh, vl, lev, d1, d2, sems):
    fine_copies = [
        pltpu.make_async_copy(fine_dog_ref, fine_dog_hbm, sems.at[0]),
        pltpu.make_async_copy(fine_hess_ref, fine_hess_hbm, sems.at[1]),
    ]
    for copy in fine_copies:
        copy.start()
    _, rows, cols = dog_ref.shape
    row, col = mesh_place()
    tall = rows + 2 * PAD
    diffs = {1: d1, 2: d2}
    is_left = col == 0
    half = cols // 2
    zero = jnp.zeros((tall, LANES), BF16)
    for s in range(LEVELS):
        for ref in (vh, vl):
            ref[s, :, :LANES] = zero
            ref[s, :, LANES + cols :] = zero
    zero = jnp.zeros((tall, LANES), F32)
    for d in (d1, d2):
        d[:, :LANES] = zero
        d[:, LANES + cols :] = zero

    strip_rows = keep_ref.shape[0]
    height = LEVELS * tall
    variant = 2 * (row % 2) + col
    start = pl.multiple_of(late_ref.shape[0] - 4 * height + variant * height, 16)
    lh = late_ref[pl.ds(start, height), : 3 * strip_rows + 4 * MESSAGE]
    lp = lh[:, 3 * strip_rows :]
    for at in range(0, cols, BLOCK):
        source = slice(at % half, at % half + BLOCK)
        second = slice(half + at % half, half + at % half + BLOCK)
        first = is_left if at < half else jnp.logical_not(is_left)
        value = jnp.where(first, keep_ref[:, source], other_ref[:, source])
        message = [jnp.where(first, odd_ref[:, lanes], odd_other_ref[:, lanes]) for lanes in (source, second)]
        at_seam = at in (half - BLOCK, half)
        if at_seam:
            join = lambda v: jnp.concatenate(
                [jnp.zeros(v.shape, v.dtype), v] if at < half else [v, jnp.zeros(v.shape, v.dtype)], axis=1
            )
            value = value + join(jnp.where(first, other_ref[:, half:], keep_ref[:, half:]))
            extra = jnp.where(first, odd_other_ref[:, cols:], odd_ref[:, cols:]).astype(F32)
            extra = [v.astype(BF16) for v in unpack_extra(extra)]
        high, low = split(value)
        stack = jnp.concatenate([high, low, high, *message, *message], axis=0)
        value = mm(lh, stack)
        if at_seam:
            value = value + join(mm(lp, jnp.concatenate([*extra, *extra], axis=0)))
        to = slice(LANES + at, LANES + at + BLOCK)
        for s in range(LEVELS):
            vh[s, :, to], vl[s, :, to] = split(value[s * tall : (s + 1) * tall])

    def emit(k, at, d):
        dog_ref[k, :, at - LANES : at - LANES + BLOCK] = (80.0 * d[PAD : PAD + rows]).astype(BF16)
        if k in diffs:
            to = slice(at, at + BLOCK)
            diffs[k][:PAD, to] = jnp.where((row == 0) & (col == 0), 0.0, d[:PAD])
            diffs[k][PAD : PAD + rows, to] = d[PAD : PAD + rows]
            diffs[k][PAD + rows :, to] = jnp.where((row == last_row) & (col == 1), 0.0, d[PAD + rows :])

    dog_copy = pltpu.make_async_copy(dog_ref, dog_hbm, sems.at[2])
    hess_copies = [pltpu.make_async_copy(hess_ref.at[m], hess_hbm.at[m], sems.at[3 + m]) for m in range(2)]

    def after_group(m, first, count):
        def put(t, value):
            hess_ref[m, :, t * LANES : (t + 1) * LANES] = value

        if m == 1:
            dog_copy.start()
        hess_tiles(diffs[m + 1], 0, rows, first, count, 200000.0, put)
        hess_copies[m].start()

    filter_columns(vh, vl, band_refs(late_ref), 8, cols, lev, emit, after_group, lambda s: None)
    for copy in fine_copies + [dog_copy] + hess_copies:
        copy.wait()


def fine_constants(rows):
    own = np.arange(rows)
    own_inputs = np.concatenate([own, own, own])
    own_low = np.arange(3 * rows) >= 2 * rows
    nowhere = -1000
    top = np.full(MESSAGE, nowhere)
    top[: NEAR + 1] = np.append(np.arange(-NEAR, 0), -1)
    bot = np.full(MESSAGE, nowhere)
    bot[: NEAR + 1] = rows + np.append(np.arange(NEAR), 0)

    def matrix(sigma, centres, valid, inputs, use_low):
        high, low = two_parts(row_matrix(sigma, centres, inputs) * valid[:, None])
        return np.where(use_low[None, :], low.astype(np.float32), high.astype(np.float32)).astype(BF16)

    level = [matrix(s, own, np.ones(rows, np.float32), own_inputs, own_low) for s in SIGMAS]
    halo = []
    for inputs, rim, near_own, outer in (
        (top, np.arange(-1, RIM - 1), own[:RIM], 0),
        (bot, np.arange(rows + 1 - RIM, rows + 1), own[rows - RIM :], RIM - 1),
    ):
        ones = np.ones(RIM, np.float32)
        alone = (np.arange(RIM) == outer).astype(np.float32)
        triple = np.concatenate([near_own, near_own, near_own])
        triple_low = np.arange(3 * RIM) >= 2 * RIM
        again = inputs.copy()
        again[NEAR] = nowhere
        for s in SIGMAS:
            beside = matrix(s, rim, alone, triple, triple_low).astype(np.float32)
            beyond = matrix(s, rim, ones, inputs, np.zeros(MESSAGE, bool)).astype(np.float32)
            halo.append(np.concatenate([beside, beyond], axis=1))
        for s in SIGMAS:
            low = matrix(s, rim, ones, again, np.ones(MESSAGE, bool)).astype(np.float32)
            halo.append(np.pad(low, ((0, 0), (0, 3 * RIM))))
    count = rows // 2 + 2 * (REACH + 1)
    index = np.arange(-(-count // 8) * 8)
    base = matrix(SIGMAS[-1], 2 * (index - REACH - 1), (index < count).astype(np.float32), own_inputs, own_low)
    strip_rows = -(-(rows // 4 + 2 * (REACH + 1)) // 16) * 16
    return np.concatenate(level), np.concatenate(halo), base, strip_rows


def coarse_constants(strip, padded):
    inputs = np.arange(padded) - REACH - 1
    centres = np.arange(-PAD, strip + PAD)
    valid = ((centres >= -1) & (centres <= strip)).astype(np.float32)
    variants = []
    for parity in range(2):
        for core in range(2):
            first = (2 * strip + REACH + 1 - 6) * parity - strip * core - REACH - 1
            message = np.full(2 * MESSAGE, -1000)
            message[NEAR + 1 : MESSAGE] = first + np.arange(PART)
            message[MESSAGE + NEAR + 1 : 2 * MESSAGE - 1] = first + np.arange(PART, SPAN)
            for s in SIGMAS:
                high, low = two_parts(row_matrix(s, centres, inputs) * valid[:, None])
                more_high, more_low = two_parts(row_matrix(s, centres, message) * valid[:, None])
                variants.append(np.concatenate([high, high, low, more_high, more_low], axis=1))
    return np.concatenate(variants)


def joined(matrices, columns=BLOCK):
    return np.concatenate(
        [np.pad(m.reshape(-1, m.shape[-1]).astype(np.float32), ((0, 0), (0, columns - m.shape[-1]))) for m in matrices]
    ).astype(BF16)


def vmem_specs(count):
    return [pl.BlockSpec(memory_space=pltpu.VMEM) for _ in range(count)]


def far_specs(count):
    return [pl.BlockSpec(memory_space=pltpu.HBM) for _ in range(count)]


def limit(mib):
    return pltpu.CompilerParams(vmem_limit_bytes=mib * 2**20)


def far(value):
    return pltpu.with_memory_space_constraint(jnp.asarray(value), pltpu.HBM)


def local(image):
    rows, cols = image.shape
    row_count = lax.axis_size("row")
    strip = rows // 4
    wide = cols + LANES
    small = strip + 2 * PAD
    lh, lt, bm, strip_rows = fine_constants(rows)
    cw = coarse_constants(strip, strip_rows)
    bands = [column_weights(s, 1) for s in SIGMAS]
    wc, wl, we = (np.stack([b[i] for b in bands]) for i in range(3))
    early = jnp.asarray(joined([bm, *column_weights(SIGMAS[-1], 2)]))
    late = jnp.asarray(joined([wc, wl, we, lh, lt, cw]))
    base_rows = bm.shape[0]
    own_shape = jax.ShapeDtypeStruct((2 * rows, wide), BF16)
    message = jax.ShapeDtypeStruct((MESSAGE, wide), BF16)

    side = pl.pallas_call(
        border_kernel,
        out_shape=jax.ShapeDtypeStruct((rows, LANES), F32),
        in_specs=far_specs(1),
        out_specs=vmem_specs(1)[0],
        scratch_shapes=[pltpu.SemaphoreType.DMA],
        compiler_params=limit(1),
        cost_estimate=pl.CostEstimate(flops=2 * 10**9, bytes_accessed=10**7, transcendentals=0),
        name="border",
    )(far(image))
    side = lax.ppermute(side, "col", [(0, 1), (1, 0)])
    own, to_even, to_odd, base = pl.pallas_call(
        send_kernel,
        out_shape=(own_shape, message, message, jax.ShapeDtypeStruct((base_rows, cols // 2 + LANES), F32)),
        in_specs=vmem_specs(2),
        out_specs=tuple(vmem_specs(4)),
        scratch_shapes=[
            pltpu.VMEM((base_rows, cols + 2 * LANES), BF16),
            pltpu.VMEM((base_rows, cols + 2 * LANES), BF16),
        ],
        compiler_params=limit(6),
        cost_estimate=pl.CostEstimate(flops=10**9, bytes_accessed=10**6, transcendentals=0),
        name="send",
    )(image, early)
    own, to_even, to_odd = pl.pallas_call(
        side_kernel,
        out_shape=(own_shape, message, message),
        in_specs=vmem_specs(4),
        out_specs=tuple(vmem_specs(3)),
        input_output_aliases={1: 0, 2: 1, 3: 2},
        compiler_params=limit(4),
        name="side",
    )(side, own, to_even, to_odd)

    def swap(value, first):
        pairs = [(i, i + 1) for i in range(first, row_count - 1, 2)]
        return lax.ppermute(value, "row", pairs + [(j, i) for i, j in pairs])

    even = swap(to_even, 0)
    odd = swap(to_odd, 1)

    fine_shapes = (
        jax.ShapeDtypeStruct((4, rows, cols), BF16),
        jax.ShapeDtypeStruct((2, rows, cols), BF16),
    )
    coarse_shapes = (
        jax.ShapeDtypeStruct((4, strip, cols), BF16),
        jax.ShapeDtypeStruct((2, strip, cols), BF16),
    )

    def scratch(count, height, seam):
        padded_cols = cols + 2 * LANES
        return [
            pltpu.VMEM((LEVELS, height, padded_cols), BF16),
            pltpu.VMEM((LEVELS, height, padded_cols), BF16),
            pltpu.VMEM((height, padded_cols + seam), F32),
            pltpu.VMEM((count, padded_cols), F32),
            pltpu.VMEM((count, padded_cols), F32),
        ]

    rim_tall = RIM + 2 * PAD
    dog_fine, hess_fine, rim = pl.pallas_call(
        inner_kernel,
        out_shape=(*fine_shapes, jax.ShapeDtypeStruct((4, 2 * (RIM + PAD), cols + 2 * LANES), F32)),
        in_specs=vmem_specs(2),
        out_specs=tuple(vmem_specs(3)),
        scratch_shapes=scratch(rows, rows, BLOCK),
        compiler_params=limit(18),
        cost_estimate=pl.CostEstimate(flops=2 * 10**9, bytes_accessed=10**7, transcendentals=0),
        name="inner",
    )(own, late)

    def finish(one_hop, message, dog, hess):
        return pl.pallas_call(
            functools.partial(outer_kernel, row_count - 1, one_hop),
            out_shape=fine_shapes,
            in_specs=vmem_specs(6),
            out_specs=tuple(vmem_specs(2)),
            scratch_shapes=scratch(rim_tall, RIM, BLOCK),
            input_output_aliases={4: 0, 5: 1},
            compiler_params=limit(12),
            cost_estimate=pl.CostEstimate(flops=10**9, bytes_accessed=10**6, transcendentals=0),
            name="outer",
        )(message, own, late, rim, dog, hess)

    dog_fine, hess_fine = finish(True, even, dog_fine, hess_fine)

    keep, send = pl.pallas_call(
        functools.partial(base_kernel, row_count, rows // 2),
        out_shape=(
            jax.ShapeDtypeStruct((strip_rows, cols // 2 + LANES), F32),
            jax.ShapeDtypeStruct((strip_rows, cols // 2 + LANES), F32),
        ),
        in_specs=vmem_specs(2) + [pl.BlockSpec(memory_space=pl.ANY)],
        out_specs=tuple(vmem_specs(2)),
        scratch_shapes=[pltpu.VMEM((base_rows, LANES), F32)],
        compiler_params=limit(4),
        name="base",
    )(base, even, rim)
    other = lax.ppermute(send, "col", [(0, 1), (1, 0)])
    odd_other = lax.ppermute(odd, "col", [(0, 1), (1, 0)])
    dog_fine, hess_fine = finish(False, odd, dog_fine, hess_fine)

    return pl.pallas_call(
        functools.partial(coarse_kernel, row_count - 1),
        out_shape=fine_shapes + coarse_shapes,
        in_specs=vmem_specs(7),
        out_specs=tuple(far_specs(4)),
        scratch_shapes=[
            pltpu.VMEM((4, strip, cols), BF16),
            pltpu.VMEM((2, strip, cols), BF16),
            *scratch(small, small, 0),
            pltpu.SemaphoreType.DMA((5,)),
        ],
        compiler_params=limit(12),
        name="coarse",
    )(keep, other, odd, odd_other, dog_fine, hess_fine, late)


def solution(mesh):
    return jax.shard_map(
        local,
        mesh=mesh,
        in_specs=(P(("slab", "row"), "col"),),
        out_specs=(
            P(None, ("slab", "row"), "col"),
            P(None, ("slab", "row"), "col"),
            P(None, ("slab", "row", "col"), None),
            P(None, ("slab", "row", "col"), None),
        ),
        check_vma=False,
    )
```

```python
import functools

import jax
import jax.numpy as jnp
import numpy as np
from jax import lax
from jax.experimental import pallas as pl
from jax.experimental.pallas import tpu as pltpu
from jax.sharding import PartitionSpec as P


SIGMAS = [1.6 * 2.0 ** (k / 4.0) for k in range(5)]
LEVELS = len(SIGMAS)
ORDER = (1, 2, 3, 0, 4)
REACH = 12
LANES = 128
BLOCK = 256
PAD = 8
RIM = 16
NEAR = REACH + 1
SPAN = 19
PART = 10
MESSAGE = NEAR + 1 + PART
BF16 = jnp.bfloat16
F32 = jnp.float32


def taps(sigma):
    offset = np.arange(2 * REACH + 1, dtype=np.float64) - REACH
    weights = np.exp(-offset * offset / (2.0 * sigma * sigma))
    return (weights / weights.sum()).astype(np.float32)


def two_parts(matrix):
    high = np.asarray(matrix, np.float32).astype(BF16)
    low = (np.asarray(matrix, np.float32) - high.astype(np.float32)).astype(BF16)
    return high, low


def tap_at(sigma, index):
    weights = taps(sigma)
    inside = (index >= 0) & (index <= 2 * REACH)
    return np.where(inside, weights[np.clip(index, 0, 2 * REACH)], np.float32(0.0))


def row_matrix(sigma, centres, inputs):
    return tap_at(sigma, inputs[None, :] - centres[:, None] + REACH)


def column_weights(sigma, step):
    width = BLOCK
    out = np.arange(BLOCK // step)[None, :] * step
    high, low = two_parts(tap_at(sigma, np.arange(width)[:, None] - out + REACH))
    lane = np.arange(LANES)[:, None]
    right = np.where(lane < REACH, tap_at(sigma, width + lane - out + REACH), 0.0)
    left = np.where(lane >= LANES - REACH, tap_at(sigma, lane - LANES - out + REACH), 0.0)
    edge_high, edge_low = two_parts(right + left)
    edge = np.concatenate([edge_high.astype(np.float32), edge_high.astype(np.float32)])
    edge[:LANES] += np.roll(edge_low.astype(np.float32), 32, axis=0)
    return high, low, edge.astype(BF16)


def split(value):
    high = value.astype(BF16)
    low = (value - high.astype(F32)).astype(BF16)
    return high, low


def mm(a, b):
    return jnp.dot(a, b, preferred_element_type=F32)


def edge_pair(high_left, high_right, low_left, low_right):
    lane = lax.broadcasted_iota(jnp.int32, high_left.shape, 1)
    eh = jnp.where(lane < LANES // 2, high_right, high_left)
    el = jnp.where(lane < LANES // 2, low_right, low_left)
    again = pltpu.roll(eh.astype(F32), 32, 1).astype(BF16)
    eh = jnp.where((lane >= 16) & (lane < 64), again, eh)
    return jnp.concatenate([eh, el], axis=1)


def edge_columns(high, low, at, width):
    left, right = slice(at - LANES, at), slice(at + width, at + width + LANES)
    return edge_pair(high[:, left], high[:, right], low[:, left], low[:, right])


def hess_tiles(d, top, rows, first_tile, count, gain, put):
    tall = rows + 2 * PAD
    lane = lax.broadcasted_iota(jnp.int32, (rows, LANES), 1)
    mid, slope, total = {}, {}, {}
    back, ahead = {}, {}

    def load(t):
        lanes = slice((first_tile + t + 1) * LANES, (first_tile + t + 2) * LANES)
        value = d[top : top + tall, lanes]
        up, down = pltpu.roll(value, 1, 0)[PAD : PAD + rows], pltpu.roll(value, tall - 1, 0)[PAD : PAD + rows]
        mid[t] = value[PAD : PAD + rows]
        slope[t], total[t] = down - up, up + down
        if t < count:
            back[t] = [pltpu.roll(v, 1, 1) for v in (mid[t], slope[t])]
        if t >= 0:
            ahead[t] = [pltpu.roll(v, LANES - 1, 1) for v in (mid[t], slope[t])]

    load(-1)
    load(0)
    for t in range(count):
        load(t + 1)
        before = [jnp.where(lane == 0, a, b) for a, b in zip(back[t - 1], back[t])]
        after = [jnp.where(lane == LANES - 1, a, b) for a, b in zip(ahead[t + 1], ahead[t])]
        twice = 2.0 * mid[t]
        dxx = after[0] + before[0] - twice
        dyy = total[t] - twice
        dxy = (after[1] - before[1]) * 0.25
        put(first_tile + t, (gain * (dxx * dyy - dxy * dxy)).astype(BF16))


def mesh_place():
    return lax.axis_index("row"), lax.axis_index("col")


def border_kernel(x_hbm, side_ref, sem):
    _, col = mesh_place()
    start = pl.multiple_of(jnp.where(col == 0, x_hbm.shape[1] - LANES, 0), LANES)
    copy = pltpu.make_async_copy(x_hbm.at[:, pl.ds(start, LANES)], side_ref, sem)
    copy.start()
    copy.wait()


def build_message(own_ref, part, rows, to):
    up_near = own_ref[:rows, to].astype(F32)[:NEAR]
    down_near = own_ref[:rows, to].astype(F32)[rows - NEAR :]
    up_low = own_ref[rows:, to].astype(F32)[:1]
    down_low = own_ref[rows:, to].astype(F32)[rows - 1 :]
    up = jnp.concatenate([up_near, up_low, part[0]], axis=0)
    down = jnp.concatenate([down_near, down_low, part[1]], axis=0)
    return up, down


def send_kernel(x_ref, early_ref, own_ref, even_ref, odd_ref, base_ref, bvh, bvl):
    row, col = mesh_place()
    rows, cols = x_ref.shape
    half = cols // 2
    base_rows = base_ref.shape[0]
    is_left = col == 0
    even = row % 2 == 0
    bm = early_ref[:base_rows, : 3 * rows]
    dc, dl, de = (early_ref[base_rows + i * BLOCK : base_rows + (i + 1) * BLOCK, : BLOCK // 2] for i in range(3))

    zero = jnp.zeros((base_rows, LANES), BF16)
    for ref in (bvh, bvl):
        ref[:, :LANES] = zero
        ref[:, LANES + cols :] = zero
    for at in range(0, cols, BLOCK):
        high, low = split(x_ref[:, at : at + BLOCK])
        own_ref[:rows, at : at + BLOCK] = high
        own_ref[rows:, at : at + BLOCK] = low
        value = mm(bm, jnp.concatenate([high, low, high], axis=0))
        to = slice(LANES + at, LANES + at + BLOCK)
        bvh[:, to], bvl[:, to] = split(value)
    first, last = slice(LANES, 2 * LANES), slice(cols, cols + LANES)
    pick = lambda ref: (
        jnp.where(is_left, ref[:, last].astype(F32), 0.0).astype(BF16),
        jnp.where(is_left, 0.0, ref[:, first].astype(F32)).astype(BF16),
    )
    beyond = edge_pair(*pick(bvh), *pick(bvl))
    group = 4
    for g in range(0, cols // BLOCK, group):
        ats = [LANES + BLOCK * (g + i) for i in range(group)]
        high = jnp.concatenate([bvh[:, at : at + BLOCK] for at in ats], axis=0)
        low = jnp.concatenate([bvl[:, at : at + BLOCK] for at in ats], axis=0)
        edge = jnp.concatenate([edge_columns(bvh, bvl, at, BLOCK) for at in ats], axis=0)
        value = mm(high, dc) + mm(low, dc) + mm(high, dl) + mm(edge, de)
        for i in range(group):
            base_ref[:, (g + i) * LANES : (g + i + 1) * LANES] = value[i * base_rows : (i + 1) * base_rows]
    base_ref[:, half:] = mm(beyond, de)

    first_up = REACH + 1 - 6
    first_down = REACH + 1 + SPAN
    for at in range(0, cols + LANES, LANES):
        to = slice(at, at + LANES)
        if at < cols:
            lanes = slice(at % half, at % half + LANES)
            skip = PART * (at // half)
            part = [base_ref[f + skip : f + skip + PART, lanes] for f in (first_up, first_down)]
        else:
            part = [
                base_ref[f : f + PART, half:] + pltpu.roll(base_ref[f + PART : f + 2 * PART, half:], LANES // 2, 1)
                for f in (first_up, first_down)
            ]
        up, down = build_message(own_ref, part, rows, to)
        if at == cols:
            index = lax.broadcasted_iota(jnp.int32, up.shape, 0)
            up = jnp.where(index > NEAR, up, 0.0)
            down = jnp.where(index > NEAR, down, 0.0)
        even_ref[:, to] = jnp.where(even, down, up).astype(BF16)
        odd_ref[:, to] = jnp.where(even, up, down).astype(BF16)


def side_kernel(side_ref, own_in, even_in, odd_in, own_ref, even_ref, odd_ref):
    row, _ = mesh_place()
    rows = own_ref.shape[0] // 2
    cols = own_ref.shape[1] - LANES
    even = row % 2 == 0
    high, low = split(side_ref[...])
    own_ref[:rows, cols:] = high
    own_ref[rows:, cols:] = low
    high, low = high.astype(F32), low.astype(F32)
    none = jnp.zeros((PART, LANES), F32)
    up = jnp.concatenate([high[:NEAR], low[:1], none], axis=0)
    down = jnp.concatenate([high[rows - NEAR :], low[rows - 1 :], none], axis=0)
    index = lax.broadcasted_iota(jnp.int32, up.shape, 0)
    for old, ref, a, b in ((even_in, even_ref, down, up), (odd_in, odd_ref, up, down)):
        kept = old[:, cols:].astype(F32)
        ref[:, cols:] = jnp.where(index > NEAR, kept, jnp.where(even, a, b)).astype(BF16)


def base_kernel(row_count, tile_base, base_ref, even_ref, _, keep_ref, send_ref, sum_ref):
    row, col = mesh_place()
    base_rows, wide = base_ref.shape
    half = wide - LANES
    count = keep_ref.shape[0]
    shift = tile_base // 2
    even = row % 2 == 0
    is_left = col == 0
    index = lax.broadcasted_iota(jnp.int32, (base_rows, LANES), 0)
    place = row * tile_base - REACH - 1 + index
    inside = (place >= 0) & (place < row_count * tile_base)
    first_bot = tile_base + REACH + 1 - 6
    for at in range(0, wide, LANES):
        to = slice(at, at + LANES)
        if at < half:
            both = [even_ref[:, lanes].astype(F32) for lanes in (to, slice(half + at, half + at + LANES))]
        else:
            both = unpack_extra(even_ref[:, 2 * half :].astype(F32))
        part = jnp.concatenate([both[0][NEAR + 1 :], both[1][NEAR + 1 : NEAR + 1 + SPAN - PART]], axis=0)
        sum_ref[...] = base_ref[:, to]
        sum_ref[:SPAN, :] += jnp.where(even, 0.0, part)
        sum_ref[first_bot : first_bot + SPAN, :] += jnp.where(even, part, 0.0)
        total = jnp.where(inside, sum_ref[...], 0.0)
        keep_ref[:, to] = jnp.where(is_left, total[:count], total[shift : shift + count])
        send_ref[:, to] = jnp.where(is_left, total[shift : shift + count], total[:count])


def unpack_extra(value):
    lane = lax.broadcasted_iota(jnp.int32, value.shape, 1)
    outside = (lane >= LANES // 4) & (lane < 3 * LANES // 4)
    return [jnp.where(outside, 0.0, v) for v in (value, pltpu.roll(value, LANES // 2, 1))]


def filter_columns(vh, vl, w_refs, group, cols, lev, emit, after_group, after_level):
    wc_ref, wl_ref, we_ref = w_refs
    tall = vh.shape[1]
    for s in ORDER:
        band = slice(s * BLOCK, (s + 1) * BLOCK)
        for g in range(0, cols // BLOCK, group):
            ats = [LANES + BLOCK * (g + i) for i in range(group)]
            high = jnp.concatenate([vh[s, :, at : at + BLOCK] for at in ats], axis=0)
            low = jnp.concatenate([vl[s, :, at : at + BLOCK] for at in ats], axis=0)
            edge = jnp.concatenate([edge_columns(vh.at[s], vl.at[s], at, BLOCK) for at in ats], axis=0)
            value = (
                mm(high, wc_ref[band]) + mm(low, wc_ref[band]) + mm(high, wl_ref[band]) + mm(edge, we_ref[band])
            )
            for i, at in enumerate(ats):
                new = value[i * tall : (i + 1) * tall]
                to = slice(at, at + BLOCK)
                if s == 0:
                    emit(0, at, lev[0, :, to] - new)
                elif s > 1:
                    emit(s - 1, at, new - lev[0 if s == 2 else 1, :, to])
                if s in (1, 2, 3):
                    lev[0 if s == 1 else 1, :, to] = new
            if s in (0, 3):
                after_group(0 if s == 3 else 1, g * BLOCK // LANES, group * BLOCK // LANES)
        after_level(s)


def place_rows(vh, vl, rows_of, cols, is_left):
    tall = vh.shape[1]
    for at in range(0, cols, BLOCK):
        value = rows_of(slice(at, at + BLOCK))
        to = slice(LANES + at, LANES + at + BLOCK)
        for s in range(LEVELS):
            vh[s, :, to], vl[s, :, to] = split(value[s * tall : (s + 1) * tall])
    value = rows_of(slice(cols, cols + LANES))
    left, right = slice(0, LANES), slice(LANES + cols, 2 * LANES + cols)
    for s in range(LEVELS):
        part = value[s * tall : (s + 1) * tall]
        vh[s, :, left], vl[s, :, left] = split(jnp.where(is_left, 0.0, part))
        vh[s, :, right], vl[s, :, right] = split(jnp.where(is_left, part, 0.0))


def seam_filter(vh, vl, w_refs, cols, lev, is_left, emit):
    wc_ref, wl_ref, _ = w_refs
    start = pl.multiple_of(jnp.where(is_left, cols, 0), LANES)

    def seam(s):
        if s not in (1, 2, 3):
            return
        high = vh[s, :, pl.ds(start, BLOCK)]
        low = vl[s, :, pl.ds(start, BLOCK)]
        band = slice(s * BLOCK, (s + 1) * BLOCK)
        new = mm(high, wc_ref[band]) + mm(low, wc_ref[band]) + mm(high, wl_ref[band])
        if s > 1:
            d = new - lev[0, :, cols + 2 * LANES :]
            emit(s - 1, 0, jnp.where(is_left, 0.0, d[:, :LANES]))
            emit(s - 1, cols + LANES, jnp.where(is_left, d[:, LANES:], 0.0))
        if s < 3:
            lev[0, :, cols + 2 * LANES :] = new

    return seam


def band_refs(late_ref):
    size = LEVELS * BLOCK
    return [late_ref.at[i * size : (i + 1) * size] for i in range(3)]


def inner_kernel(own_ref, late_ref, dog_ref, hess_ref, rim_ref, vh, vl, lev, d1, d2):
    _, rows, cols = dog_ref.shape
    _, col = mesh_place()
    is_left = col == 0
    diffs = {1: d1, 2: d2}
    mid_rows = rows - 2 * RIM
    rim_tall = RIM + PAD

    def rows_of(part):
        own = own_ref[:, part]
        return mm(lh, jnp.concatenate([own, own[:rows]], axis=0))

    def emit(k, at, d):
        to = slice(at, at + d.shape[1])
        rim_ref[k, :rim_tall, to] = d[:rim_tall]
        rim_ref[k, rim_tall:, to] = d[rows - rim_tall :]
        if 0 < at <= cols:
            mid = d[RIM : RIM + mid_rows]
            dog_ref[k, RIM : RIM + mid_rows, at - LANES : at - LANES + BLOCK] = (20.0 * mid).astype(BF16)
        if k in diffs:
            diffs[k][:, to] = d

    def after_group(m, first, count):
        def put(t, value):
            hess_ref[m, RIM : RIM + mid_rows, t * LANES : (t + 1) * LANES] = value

        hess_tiles(diffs[m + 1], RIM - PAD, mid_rows, first, count, 5000.0, put)

    first = 3 * LEVELS * BLOCK
    lh = late_ref[first : first + LEVELS * rows, : 3 * rows]
    place_rows(vh, vl, rows_of, cols, is_left)
    w_refs = band_refs(late_ref)
    seam = seam_filter(vh, vl, w_refs, cols, lev, is_left, emit)
    filter_columns(vh, vl, w_refs, 4, cols, lev, emit, after_group, seam)


def outer_kernel(last_row, one_hop, message_ref, own_ref, late_ref, rim_ref, dog_in, hess_in, dog_ref, hess_ref, *scratch):
    row, _ = mesh_place()
    from_above = (row % 2 == 1) if one_hop else (row % 2 == 0)
    for above in (True, False):

        @pl.when(from_above if above else jnp.logical_not(from_above))
        def _():
            outer_side(last_row, above, message_ref, own_ref, late_ref, rim_ref, dog_ref, hess_ref, *scratch)


def outer_side(last_row, above, message_ref, own_ref, late_ref, rim_ref, dog_ref, hess_ref, vh, vl, lev, d1, d2):
    _, rows, cols = dog_ref.shape
    row, col = mesh_place()
    is_left = col == 0
    diffs = {1: d1, 2: d2}
    rim_tall = RIM + 2 * PAD
    skip = PAD - 1 if above else PAD + 1
    outs = slice(0, RIM) if above else slice(rows - RIM, rows)
    height = LEVELS * RIM
    start = 3 * LEVELS * BLOCK + LEVELS * rows + (0 if above else 2 * height)
    lt_high = late_ref[start : start + height, : 3 * RIM + MESSAGE]
    lt_low = late_ref[start + height : start + 2 * height, :MESSAGE]
    own_first = 0 if above else rows - RIM

    def rows_of(part):
        message = message_ref[:, part]
        high = own_ref[own_first : own_first + RIM, part]
        low = own_ref[rows + own_first : rows + own_first + RIM, part]
        return mm(lt_high, jnp.concatenate([high, low, high, message], axis=0)) + mm(lt_low, message)

    def emit(k, at, d):
        to = slice(at, at + d.shape[1])
        zero = lambda count: jnp.zeros((count, d.shape[1]), F32)
        total = jnp.concatenate([zero(skip), d, zero(rim_tall - RIM - skip)], axis=0)
        if above:
            total = jnp.concatenate([total[:PAD], total[PAD:] + rim_ref[k, : rim_tall - PAD, to]], axis=0)
        else:
            own = total[: rim_tall - PAD] + rim_ref[k, rim_tall - PAD :, to]
            total = jnp.concatenate([own, total[rim_tall - PAD :]], axis=0)
        if 0 < at <= cols:
            dog_ref[k, outs, at - LANES : at - LANES + BLOCK] = (20.0 * total[PAD : PAD + RIM]).astype(BF16)
        if k in diffs:
            d = diffs[k]
            if above:
                d[:PAD, to] = jnp.where(row == 0, 0.0, total[:PAD])
                d[PAD:, to] = total[PAD:]
            else:
                d[: rim_tall - PAD, to] = total[: rim_tall - PAD]
                d[rim_tall - PAD :, to] = jnp.where(row == last_row, 0.0, total[rim_tall - PAD :])

    def after_group(m, tile, count):
        def put(t, value):
            hess_ref[m, outs, t * LANES : (t + 1) * LANES] = value

        hess_tiles(diffs[m + 1], 0, RIM, tile, count, 5000.0, put)

    place_rows(vh, vl, rows_of, cols, is_left)
    w_refs = band_refs(late_ref)
    seam = seam_filter(vh, vl, w_refs, cols, lev, is_left, emit)
    filter_columns(vh, vl, w_refs, 8, cols, lev, emit, after_group, seam)


def coarse_kernel(last_row, keep_ref, other_ref, odd_ref, odd_other_ref, fine_dog_ref, fine_hess_ref, late_ref,
                  fine_dog_hbm, fine_hess_hbm, dog_hbm, hess_hbm,
                  dog_ref, hess_ref, vh, vl, lev, d1, d2, sems):
    fine_copies = [
        pltpu.make_async_copy(fine_dog_ref, fine_dog_hbm, sems.at[0]),
        pltpu.make_async_copy(fine_hess_ref, fine_hess_hbm, sems.at[1]),
    ]
    for copy in fine_copies:
        copy.start()
    _, rows, cols = dog_ref.shape
    row, col = mesh_place()
    tall = rows + 2 * PAD
    diffs = {1: d1, 2: d2}
    is_left = col == 0
    half = cols // 2
    zero = jnp.zeros((tall, LANES), BF16)
    for s in range(LEVELS):
        for ref in (vh, vl):
            ref[s, :, :LANES] = zero
            ref[s, :, LANES + cols :] = zero
    zero = jnp.zeros((tall, LANES), F32)
    for d in (d1, d2):
        d[:, :LANES] = zero
        d[:, LANES + cols :] = zero

    strip_rows = keep_ref.shape[0]
    height = LEVELS * tall
    variant = 2 * (row % 2) + col
    start = pl.multiple_of(late_ref.shape[0] - 4 * height + variant * height, 16)
    lh = late_ref[pl.ds(start, height), : 3 * strip_rows + 4 * MESSAGE]
    lp = lh[:, 3 * strip_rows :]
    for at in range(0, cols, BLOCK):
        source = slice(at % half, at % half + BLOCK)
        second = slice(half + at % half, half + at % half + BLOCK)
        first = is_left if at < half else jnp.logical_not(is_left)
        value = jnp.where(first, keep_ref[:, source], other_ref[:, source])
        message = [jnp.where(first, odd_ref[:, lanes], odd_other_ref[:, lanes]) for lanes in (source, second)]
        at_seam = at in (half - BLOCK, half)
        if at_seam:
            join = lambda v: jnp.concatenate(
                [jnp.zeros(v.shape, v.dtype), v] if at < half else [v, jnp.zeros(v.shape, v.dtype)], axis=1
            )
            value = value + join(jnp.where(first, other_ref[:, half:], keep_ref[:, half:]))
            extra = jnp.where(first, odd_other_ref[:, cols:], odd_ref[:, cols:]).astype(F32)
            extra = [v.astype(BF16) for v in unpack_extra(extra)]
        high, low = split(value)
        stack = jnp.concatenate([high, low, high, *message, *message], axis=0)
        value = mm(lh, stack)
        if at_seam:
            value = value + join(mm(lp, jnp.concatenate([*extra, *extra], axis=0)))
        to = slice(LANES + at, LANES + at + BLOCK)
        for s in range(LEVELS):
            vh[s, :, to], vl[s, :, to] = split(value[s * tall : (s + 1) * tall])

    def emit(k, at, d):
        dog_ref[k, :, at - LANES : at - LANES + BLOCK] = (80.0 * d[PAD : PAD + rows]).astype(BF16)
        if k in diffs:
            to = slice(at, at + BLOCK)
            diffs[k][:PAD, to] = jnp.where((row == 0) & (col == 0), 0.0, d[:PAD])
            diffs[k][PAD : PAD + rows, to] = d[PAD : PAD + rows]
            diffs[k][PAD + rows :, to] = jnp.where((row == last_row) & (col == 1), 0.0, d[PAD + rows :])

    dog_copies = [pltpu.make_async_copy(dog_ref.at[k], dog_hbm.at[k], sems.at[4 + k]) for k in range(4)]
    hess_copies = [pltpu.make_async_copy(hess_ref.at[m], hess_hbm.at[m], sems.at[2 + m]) for m in range(2)]

    def after_group(m, first, count):
        def put(t, value):
            hess_ref[m, :, t * LANES : (t + 1) * LANES] = value

        hess_tiles(diffs[m + 1], 0, rows, first, count, 200000.0, put)

    def after_level(s):
        if s == 0:
            for copy in (dog_copies[1], dog_copies[2], hess_copies[0]):
                copy.start()
        if s == 4:
            for copy in (hess_copies[1], dog_copies[0], dog_copies[3]):
                copy.start()

    filter_columns(vh, vl, band_refs(late_ref), 8, cols, lev, emit, after_group, after_level)
    for copy in fine_copies + dog_copies + hess_copies:
        copy.wait()


def fine_constants(rows):
    own = np.arange(rows)
    own_inputs = np.concatenate([own, own, own])
    own_low = np.arange(3 * rows) >= 2 * rows
    nowhere = -1000
    top = np.full(MESSAGE, nowhere)
    top[: NEAR + 1] = np.append(np.arange(-NEAR, 0), -1)
    bot = np.full(MESSAGE, nowhere)
    bot[: NEAR + 1] = rows + np.append(np.arange(NEAR), 0)

    def matrix(sigma, centres, valid, inputs, use_low):
        high, low = two_parts(row_matrix(sigma, centres, inputs) * valid[:, None])
        return np.where(use_low[None, :], low.astype(np.float32), high.astype(np.float32)).astype(BF16)

    level = [matrix(s, own, np.ones(rows, np.float32), own_inputs, own_low) for s in SIGMAS]
    halo = []
    for inputs, rim, near_own, outer in (
        (top, np.arange(-1, RIM - 1), own[:RIM], 0),
        (bot, np.arange(rows + 1 - RIM, rows + 1), own[rows - RIM :], RIM - 1),
    ):
        ones = np.ones(RIM, np.float32)
        alone = (np.arange(RIM) == outer).astype(np.float32)
        triple = np.concatenate([near_own, near_own, near_own])
        triple_low = np.arange(3 * RIM) >= 2 * RIM
        again = inputs.copy()
        again[NEAR] = nowhere
        for s in SIGMAS:
            beside = matrix(s, rim, alone, triple, triple_low).astype(np.float32)
            beyond = matrix(s, rim, ones, inputs, np.zeros(MESSAGE, bool)).astype(np.float32)
            halo.append(np.concatenate([beside, beyond], axis=1))
        for s in SIGMAS:
            low = matrix(s, rim, ones, again, np.ones(MESSAGE, bool)).astype(np.float32)
            halo.append(np.pad(low, ((0, 0), (0, 3 * RIM))))
    count = rows // 2 + 2 * (REACH + 1)
    index = np.arange(-(-count // 8) * 8)
    base = matrix(SIGMAS[-1], 2 * (index - REACH - 1), (index < count).astype(np.float32), own_inputs, own_low)
    strip_rows = -(-(rows // 4 + 2 * (REACH + 1)) // 16) * 16
    return np.concatenate(level), np.concatenate(halo), base, strip_rows


def coarse_constants(strip, padded):
    inputs = np.arange(padded) - REACH - 1
    centres = np.arange(-PAD, strip + PAD)
    valid = ((centres >= -1) & (centres <= strip)).astype(np.float32)
    variants = []
    for parity in range(2):
        for core in range(2):
            first = (2 * strip + REACH + 1 - 6) * parity - strip * core - REACH - 1
            message = np.full(2 * MESSAGE, -1000)
            message[NEAR + 1 : MESSAGE] = first + np.arange(PART)
            message[MESSAGE + NEAR + 1 : 2 * MESSAGE - 1] = first + np.arange(PART, SPAN)
            for s in SIGMAS:
                high, low = two_parts(row_matrix(s, centres, inputs) * valid[:, None])
                more_high, more_low = two_parts(row_matrix(s, centres, message) * valid[:, None])
                variants.append(np.concatenate([high, high, low, more_high, more_low], axis=1))
    return np.concatenate(variants)


def joined(matrices, columns=BLOCK):
    return np.concatenate(
        [np.pad(m.reshape(-1, m.shape[-1]).astype(np.float32), ((0, 0), (0, columns - m.shape[-1]))) for m in matrices]
    ).astype(BF16)


def vmem_specs(count):
    return [pl.BlockSpec(memory_space=pltpu.VMEM) for _ in range(count)]


def far_specs(count):
    return [pl.BlockSpec(memory_space=pltpu.HBM) for _ in range(count)]


def limit(mib):
    return pltpu.CompilerParams(vmem_limit_bytes=mib * 2**20)


def far(value):
    return pltpu.with_memory_space_constraint(jnp.asarray(value), pltpu.HBM)


def local(image):
    rows, cols = image.shape
    row_count = lax.axis_size("row")
    strip = rows // 4
    wide = cols + LANES
    small = strip + 2 * PAD
    lh, lt, bm, strip_rows = fine_constants(rows)
    cw = coarse_constants(strip, strip_rows)
    bands = [column_weights(s, 1) for s in SIGMAS]
    wc, wl, we = (np.stack([b[i] for b in bands]) for i in range(3))
    early = jnp.asarray(joined([bm, *column_weights(SIGMAS[-1], 2)]))
    late = jnp.asarray(joined([wc, wl, we, lh, lt, cw]))
    base_rows = bm.shape[0]
    own_shape = jax.ShapeDtypeStruct((2 * rows, wide), BF16)
    message = jax.ShapeDtypeStruct((MESSAGE, wide), BF16)

    side = pl.pallas_call(
        border_kernel,
        out_shape=jax.ShapeDtypeStruct((rows, LANES), F32),
        in_specs=far_specs(1),
        out_specs=vmem_specs(1)[0],
        scratch_shapes=[pltpu.SemaphoreType.DMA],
        compiler_params=limit(1),
        cost_estimate=pl.CostEstimate(flops=2 * 10**9, bytes_accessed=10**7, transcendentals=0),
        name="border",
    )(far(image))
    side = lax.ppermute(side, "col", [(0, 1), (1, 0)])
    own, to_even, to_odd, base = pl.pallas_call(
        send_kernel,
        out_shape=(own_shape, message, message, jax.ShapeDtypeStruct((base_rows, cols // 2 + LANES), F32)),
        in_specs=vmem_specs(2),
        out_specs=tuple(vmem_specs(4)),
        scratch_shapes=[
            pltpu.VMEM((base_rows, cols + 2 * LANES), BF16),
            pltpu.VMEM((base_rows, cols + 2 * LANES), BF16),
        ],
        compiler_params=limit(6),
        cost_estimate=pl.CostEstimate(flops=10**9, bytes_accessed=10**6, transcendentals=0),
        name="send",
    )(image, early)
    own, to_even, to_odd = pl.pallas_call(
        side_kernel,
        out_shape=(own_shape, message, message),
        in_specs=vmem_specs(4),
        out_specs=tuple(vmem_specs(3)),
        input_output_aliases={1: 0, 2: 1, 3: 2},
        compiler_params=limit(4),
        name="side",
    )(side, own, to_even, to_odd)

    def swap(value, first):
        pairs = [(i, i + 1) for i in range(first, row_count - 1, 2)]
        return lax.ppermute(value, "row", pairs + [(j, i) for i, j in pairs])

    even = swap(to_even, 0)
    odd = swap(to_odd, 1)

    fine_shapes = (
        jax.ShapeDtypeStruct((4, rows, cols), BF16),
        jax.ShapeDtypeStruct((2, rows, cols), BF16),
    )
    coarse_shapes = (
        jax.ShapeDtypeStruct((4, strip, cols), BF16),
        jax.ShapeDtypeStruct((2, strip, cols), BF16),
    )

    def scratch(count, height, seam):
        padded_cols = cols + 2 * LANES
        return [
            pltpu.VMEM((LEVELS, height, padded_cols), BF16),
            pltpu.VMEM((LEVELS, height, padded_cols), BF16),
            pltpu.VMEM((2, height, padded_cols + seam), F32),
            pltpu.VMEM((count, padded_cols), F32),
            pltpu.VMEM((count, padded_cols), F32),
        ]

    rim_tall = RIM + 2 * PAD
    dog_fine, hess_fine, rim = pl.pallas_call(
        inner_kernel,
        out_shape=(*fine_shapes, jax.ShapeDtypeStruct((4, 2 * (RIM + PAD), cols + 2 * LANES), F32)),
        in_specs=vmem_specs(2),
        out_specs=tuple(vmem_specs(3)),
        scratch_shapes=scratch(rows, rows, BLOCK),
        compiler_params=limit(18),
        cost_estimate=pl.CostEstimate(flops=2 * 10**9, bytes_accessed=10**7, transcendentals=0),
        name="inner",
    )(own, late)

    def finish(one_hop, message, dog, hess):
        return pl.pallas_call(
            functools.partial(outer_kernel, row_count - 1, one_hop),
            out_shape=fine_shapes,
            in_specs=vmem_specs(6),
            out_specs=tuple(vmem_specs(2)),
            scratch_shapes=scratch(rim_tall, RIM, BLOCK),
            input_output_aliases={4: 0, 5: 1},
            compiler_params=limit(12),
            cost_estimate=pl.CostEstimate(flops=10**9, bytes_accessed=10**6, transcendentals=0),
            name="outer",
        )(message, own, late, rim, dog, hess)

    dog_fine, hess_fine = finish(True, even, dog_fine, hess_fine)

    keep, send = pl.pallas_call(
        functools.partial(base_kernel, row_count, rows // 2),
        out_shape=(
            jax.ShapeDtypeStruct((strip_rows, cols // 2 + LANES), F32),
            jax.ShapeDtypeStruct((strip_rows, cols // 2 + LANES), F32),
        ),
        in_specs=vmem_specs(2) + [pl.BlockSpec(memory_space=pl.ANY)],
        out_specs=tuple(vmem_specs(2)),
        scratch_shapes=[pltpu.VMEM((base_rows, LANES), F32)],
        compiler_params=limit(4),
        name="base",
    )(base, even, rim)
    other = lax.ppermute(send, "col", [(0, 1), (1, 0)])
    odd_other = lax.ppermute(odd, "col", [(0, 1), (1, 0)])
    dog_fine, hess_fine = finish(False, odd, dog_fine, hess_fine)

    return pl.pallas_call(
        functools.partial(coarse_kernel, row_count - 1),
        out_shape=fine_shapes + coarse_shapes,
        in_specs=vmem_specs(7),
        out_specs=tuple(far_specs(4)),
        scratch_shapes=[
            pltpu.VMEM((4, strip, cols), BF16),
            pltpu.VMEM((2, strip, cols), BF16),
            *scratch(small, small, 0),
            pltpu.SemaphoreType.DMA((8,)),
        ],
        compiler_params=limit(12),
        name="coarse",
    )(keep, other, odd, odd_other, dog_fine, hess_fine, late)


def solution(mesh):
    return jax.shard_map(
        local,
        mesh=mesh,
        in_specs=(P(("slab", "row"), "col"),),
        out_specs=(
            P(None, ("slab", "row"), "col"),
            P(None, ("slab", "row"), "col"),
            P(None, ("slab", "row", "col"), None),
            P(None, ("slab", "row", "col"), None),
        ),
        check_vma=False,
    )
```

```python
import functools

import jax
import jax.numpy as jnp
import numpy as np
from jax import lax
from jax.experimental import pallas as pl
from jax.experimental.pallas import tpu as pltpu
from jax.sharding import PartitionSpec as P


SIGMAS = [1.6 * 2.0 ** (k / 4.0) for k in range(5)]
LEVELS = len(SIGMAS)
ORDER = (1, 2, 3, 0, 4)
REACH = 12
LANES = 128
BLOCK = 256
PAD = 8
RIM = 16
NEAR = REACH + 1
SPAN = 19
PART = 10
MESSAGE = NEAR + 1 + PART
BF16 = jnp.bfloat16
F32 = jnp.float32


def taps(sigma):
    offset = np.arange(2 * REACH + 1, dtype=np.float64) - REACH
    weights = np.exp(-offset * offset / (2.0 * sigma * sigma))
    return (weights / weights.sum()).astype(np.float32)


def two_parts(matrix):
    high = np.asarray(matrix, np.float32).astype(BF16)
    low = (np.asarray(matrix, np.float32) - high.astype(np.float32)).astype(BF16)
    return high, low


def tap_at(sigma, index):
    weights = taps(sigma)
    inside = (index >= 0) & (index <= 2 * REACH)
    return np.where(inside, weights[np.clip(index, 0, 2 * REACH)], np.float32(0.0))


def row_matrix(sigma, centres, inputs):
    return tap_at(sigma, inputs[None, :] - centres[:, None] + REACH)


def column_weights(sigma, step):
    width = BLOCK
    out = np.arange(BLOCK // step)[None, :] * step
    high, low = two_parts(tap_at(sigma, np.arange(width)[:, None] - out + REACH))
    lane = np.arange(LANES)[:, None]
    right = np.where(lane < REACH, tap_at(sigma, width + lane - out + REACH), 0.0)
    left = np.where(lane >= LANES - REACH, tap_at(sigma, lane - LANES - out + REACH), 0.0)
    edge_high, edge_low = two_parts(right + left)
    edge = np.concatenate([edge_high.astype(np.float32), edge_high.astype(np.float32)])
    edge[:LANES] += np.roll(edge_low.astype(np.float32), 32, axis=0)
    return high, low, edge.astype(BF16)


def split(value):
    high = value.astype(BF16)
    low = (value - high.astype(F32)).astype(BF16)
    return high, low


def mm(a, b):
    return jnp.dot(a, b, preferred_element_type=F32)


def edge_pair(high_left, high_right, low_left, low_right):
    lane = lax.broadcasted_iota(jnp.int32, high_left.shape, 1)
    eh = jnp.where(lane < LANES // 2, high_right, high_left)
    el = jnp.where(lane < LANES // 2, low_right, low_left)
    again = pltpu.roll(eh.astype(F32), 32, 1).astype(BF16)
    eh = jnp.where((lane >= 16) & (lane < 64), again, eh)
    return jnp.concatenate([eh, el], axis=1)


def edge_columns(high, low, at, width):
    left, right = slice(at - LANES, at), slice(at + width, at + width + LANES)
    return edge_pair(high[:, left], high[:, right], low[:, left], low[:, right])


def hess_tiles(d, top, rows, first_tile, count, gain, put, pad=PAD, tall=None):
    tall = tall or rows + 2 * pad
    lane = lax.broadcasted_iota(jnp.int32, (rows, LANES), 1)
    mid, slope, total = {}, {}, {}
    back, ahead = {}, {}

    def load(t):
        lanes = slice((first_tile + t + 1) * LANES, (first_tile + t + 2) * LANES)
        value = d[top : top + tall, lanes]
        up, down = pltpu.roll(value, 1, 0)[pad : pad + rows], pltpu.roll(value, tall - 1, 0)[pad : pad + rows]
        mid[t] = value[pad : pad + rows]
        slope[t], total[t] = down - up, up + down
        if t < count:
            back[t] = [pltpu.roll(v, 1, 1) for v in (mid[t], slope[t])]
        if t >= 0:
            ahead[t] = [pltpu.roll(v, LANES - 1, 1) for v in (mid[t], slope[t])]

    load(-1)
    load(0)
    for t in range(count):
        load(t + 1)
        before = [jnp.where(lane == 0, a, b) for a, b in zip(back[t - 1], back[t])]
        after = [jnp.where(lane == LANES - 1, a, b) for a, b in zip(ahead[t + 1], ahead[t])]
        twice = 2.0 * mid[t]
        dxx = after[0] + before[0] - twice
        dyy = total[t] - twice
        dxy = (after[1] - before[1]) * 0.25
        put(first_tile + t, (gain * (dxx * dyy - dxy * dxy)).astype(BF16))


def mesh_place():
    return lax.axis_index("row"), lax.axis_index("col")


def border_kernel(x_hbm, side_ref, sem):
    _, col = mesh_place()
    start = pl.multiple_of(jnp.where(col == 0, x_hbm.shape[1] - LANES, 0), LANES)
    copy = pltpu.make_async_copy(x_hbm.at[:, pl.ds(start, LANES)], side_ref, sem)
    copy.start()
    copy.wait()


def build_message(own_ref, part, rows, to):
    up_near = own_ref[:rows, to].astype(F32)[:NEAR]
    down_near = own_ref[:rows, to].astype(F32)[rows - NEAR :]
    up_low = own_ref[rows:, to].astype(F32)[:1]
    down_low = own_ref[rows:, to].astype(F32)[rows - 1 :]
    up = jnp.concatenate([up_near, up_low, part[0]], axis=0)
    down = jnp.concatenate([down_near, down_low, part[1]], axis=0)
    return up, down


def send_kernel(x_ref, early_ref, own_ref, even_ref, odd_ref, base_ref, bvh, bvl):
    row, col = mesh_place()
    rows, cols = x_ref.shape
    half = cols // 2
    base_rows = base_ref.shape[0]
    is_left = col == 0
    even = row % 2 == 0
    bm = early_ref[:base_rows, : 3 * rows]
    dc, dl, de = (early_ref[base_rows + i * BLOCK : base_rows + (i + 1) * BLOCK, : BLOCK // 2] for i in range(3))

    zero = jnp.zeros((base_rows, LANES), BF16)
    for ref in (bvh, bvl):
        ref[:, :LANES] = zero
        ref[:, LANES + cols :] = zero
    for at in range(0, cols, BLOCK):
        high, low = split(x_ref[:, at : at + BLOCK])
        own_ref[:rows, at : at + BLOCK] = high
        own_ref[rows:, at : at + BLOCK] = low
        value = mm(bm, jnp.concatenate([high, low, high], axis=0))
        to = slice(LANES + at, LANES + at + BLOCK)
        bvh[:, to], bvl[:, to] = split(value)
    first, last = slice(LANES, 2 * LANES), slice(cols, cols + LANES)
    pick = lambda ref: (
        jnp.where(is_left, ref[:, last].astype(F32), 0.0).astype(BF16),
        jnp.where(is_left, 0.0, ref[:, first].astype(F32)).astype(BF16),
    )
    beyond = edge_pair(*pick(bvh), *pick(bvl))
    group = 4
    for g in range(0, cols // BLOCK, group):
        ats = [LANES + BLOCK * (g + i) for i in range(group)]
        high = jnp.concatenate([bvh[:, at : at + BLOCK] for at in ats], axis=0)
        low = jnp.concatenate([bvl[:, at : at + BLOCK] for at in ats], axis=0)
        edge = jnp.concatenate([edge_columns(bvh, bvl, at, BLOCK) for at in ats], axis=0)
        value = mm(high, dc) + mm(low, dc) + mm(high, dl) + mm(edge, de)
        for i in range(group):
            base_ref[:, (g + i) * LANES : (g + i + 1) * LANES] = value[i * base_rows : (i + 1) * base_rows]
    base_ref[:, half:] = mm(beyond, de)

    first_up = REACH + 1 - 6
    first_down = REACH + 1 + SPAN
    for at in range(0, cols + LANES, LANES):
        to = slice(at, at + LANES)
        if at < cols:
            lanes = slice(at % half, at % half + LANES)
            skip = PART * (at // half)
            part = [base_ref[f + skip : f + skip + PART, lanes] for f in (first_up, first_down)]
        else:
            part = [
                base_ref[f : f + PART, half:] + pltpu.roll(base_ref[f + PART : f + 2 * PART, half:], LANES // 2, 1)
                for f in (first_up, first_down)
            ]
        up, down = build_message(own_ref, part, rows, to)
        if at == cols:
            index = lax.broadcasted_iota(jnp.int32, up.shape, 0)
            up = jnp.where(index > NEAR, up, 0.0)
            down = jnp.where(index > NEAR, down, 0.0)
        even_ref[:, to] = jnp.where(even, down, up).astype(BF16)
        odd_ref[:, to] = jnp.where(even, up, down).astype(BF16)


def side_kernel(side_ref, own_in, even_in, odd_in, own_ref, even_ref, odd_ref):
    row, _ = mesh_place()
    rows = own_ref.shape[0] // 2
    cols = own_ref.shape[1] - LANES
    even = row % 2 == 0
    high, low = split(side_ref[...])
    own_ref[:rows, cols:] = high
    own_ref[rows:, cols:] = low
    high, low = high.astype(F32), low.astype(F32)
    none = jnp.zeros((PART, LANES), F32)
    up = jnp.concatenate([high[:NEAR], low[:1], none], axis=0)
    down = jnp.concatenate([high[rows - NEAR :], low[rows - 1 :], none], axis=0)
    index = lax.broadcasted_iota(jnp.int32, up.shape, 0)
    for old, ref, a, b in ((even_in, even_ref, down, up), (odd_in, odd_ref, up, down)):
        kept = old[:, cols:].astype(F32)
        ref[:, cols:] = jnp.where(index > NEAR, kept, jnp.where(even, a, b)).astype(BF16)


def base_kernel(row_count, tile_base, base_ref, even_ref, _, keep_ref, send_ref, sum_ref):
    row, col = mesh_place()
    base_rows, wide = base_ref.shape
    half = wide - LANES
    count = keep_ref.shape[0]
    shift = tile_base // 2
    even = row % 2 == 0
    is_left = col == 0
    index = lax.broadcasted_iota(jnp.int32, (base_rows, LANES), 0)
    place = row * tile_base - REACH - 1 + index
    inside = (place >= 0) & (place < row_count * tile_base)
    first_bot = tile_base + REACH + 1 - 6
    for at in range(0, wide, LANES):
        to = slice(at, at + LANES)
        if at < half:
            both = [even_ref[:, lanes].astype(F32) for lanes in (to, slice(half + at, half + at + LANES))]
        else:
            both = unpack_extra(even_ref[:, 2 * half :].astype(F32))
        part = jnp.concatenate([both[0][NEAR + 1 :], both[1][NEAR + 1 : NEAR + 1 + SPAN - PART]], axis=0)
        sum_ref[...] = base_ref[:, to]
        sum_ref[:SPAN, :] += jnp.where(even, 0.0, part)
        sum_ref[first_bot : first_bot + SPAN, :] += jnp.where(even, part, 0.0)
        total = jnp.where(inside, sum_ref[...], 0.0)
        keep_ref[:, to] = jnp.where(is_left, total[:count], total[shift : shift + count])
        send_ref[:, to] = jnp.where(is_left, total[shift : shift + count], total[:count])


def unpack_extra(value):
    lane = lax.broadcasted_iota(jnp.int32, value.shape, 1)
    outside = (lane >= LANES // 4) & (lane < 3 * LANES // 4)
    return [jnp.where(outside, 0.0, v) for v in (value, pltpu.roll(value, LANES // 2, 1))]


def plain_lhs(vh, vl):
    def lhs(s, ats):
        high = jnp.concatenate([vh[s, :, at : at + BLOCK] for at in ats], axis=0)
        low = jnp.concatenate([vl[s, :, at : at + BLOCK] for at in ats], axis=0)
        edge = jnp.concatenate([edge_columns(vh.at[s], vl.at[s], at, BLOCK) for at in ats], axis=0)
        return high, low, edge

    return lhs


def filter_columns(lhs, w_refs, group, cols, lev, emit, after_group, after_level):
    wc_ref, wl_ref, we_ref = w_refs
    tall = lev.shape[1]
    for s in ORDER:
        band = slice(s * BLOCK, (s + 1) * BLOCK)
        for g in range(0, cols // BLOCK, group):
            ats = [LANES + BLOCK * (g + i) for i in range(group)]
            high, low, edge = lhs(s, ats)
            value = (
                mm(high, wc_ref[band]) + mm(low, wc_ref[band]) + mm(high, wl_ref[band]) + mm(edge, we_ref[band])
            )
            for i, at in enumerate(ats):
                new = value[i * tall : (i + 1) * tall]
                to = slice(at, at + BLOCK)
                if s == 0:
                    emit(0, at, lev[0, :, to] - new)
                elif s > 1:
                    emit(s - 1, at, new - lev[0 if s == 2 else 1, :, to])
                if s in (1, 2, 3):
                    lev[0 if s == 1 else 1, :, to] = new
            if s in (0, 3):
                after_group(0 if s == 3 else 1, g * BLOCK // LANES, group * BLOCK // LANES)
        after_level(s)


def place_rows(vh, vl, rows_of, cols, is_left):
    tall = vh.shape[1]
    for at in range(0, cols, BLOCK):
        value = rows_of(slice(at, at + BLOCK))
        to = slice(LANES + at, LANES + at + BLOCK)
        for s in range(LEVELS):
            vh[s, :, to], vl[s, :, to] = split(value[s * tall : (s + 1) * tall])
    value = rows_of(slice(cols, cols + LANES))
    left, right = slice(0, LANES), slice(LANES + cols, 2 * LANES + cols)
    for s in range(LEVELS):
        part = value[s * tall : (s + 1) * tall]
        vh[s, :, left], vl[s, :, left] = split(jnp.where(is_left, 0.0, part))
        vh[s, :, right], vl[s, :, right] = split(jnp.where(is_left, part, 0.0))


def seam_filter(vh, vl, w_refs, cols, lev, is_left, emit):
    wc_ref, wl_ref, _ = w_refs
    start = pl.multiple_of(jnp.where(is_left, cols, 0), LANES)

    def seam(s):
        if s not in (1, 2, 3):
            return
        high = vh[s, :, pl.ds(start, BLOCK)]
        low = vl[s, :, pl.ds(start, BLOCK)]
        band = slice(s * BLOCK, (s + 1) * BLOCK)
        new = mm(high, wc_ref[band]) + mm(low, wc_ref[band]) + mm(high, wl_ref[band])
        if s > 1:
            d = new - lev[0, :, cols + 2 * LANES :]
            emit(s - 1, 0, jnp.where(is_left, 0.0, d[:, :LANES]))
            emit(s - 1, cols + LANES, jnp.where(is_left, d[:, LANES:], 0.0))
        if s < 3:
            lev[0, :, cols + 2 * LANES :] = new

    return seam


def band_refs(late_ref):
    size = LEVELS * BLOCK
    return [late_ref.at[i * size : (i + 1) * size] for i in range(3)]


def inner_kernel(own_ref, late_ref, dog_ref, hess_ref, rim_ref, vh, vl, lev, d1, d2):
    _, rows, cols = dog_ref.shape
    _, col = mesh_place()
    is_left = col == 0
    diffs = {1: d1, 2: d2}
    mid_rows = rows - 2 * RIM
    rim_tall = RIM + PAD

    def rows_of(part):
        own = own_ref[:, part]
        return mm(lh, jnp.concatenate([own, own[:rows]], axis=0))

    def emit(k, at, d):
        to = slice(at, at + d.shape[1])
        rim_ref[k, :rim_tall, to] = d[:rim_tall]
        rim_ref[k, rim_tall:, to] = d[rows - rim_tall :]
        if 0 < at <= cols:
            mid = d[RIM : RIM + mid_rows]
            dog_ref[k, RIM : RIM + mid_rows, at - LANES : at - LANES + BLOCK] = (20.0 * mid).astype(BF16)
        if k in diffs:
            diffs[k][:, to] = d

    def after_group(m, first, count):
        def put(t, value):
            hess_ref[m, RIM : RIM + mid_rows, t * LANES : (t + 1) * LANES] = value

        hess_tiles(diffs[m + 1], RIM - PAD, mid_rows, first, count, 5000.0, put)

    first = 3 * LEVELS * BLOCK
    lh = late_ref[first : first + LEVELS * rows, : 3 * rows]
    place_rows(vh, vl, rows_of, cols, is_left)
    w_refs = band_refs(late_ref)
    seam = seam_filter(vh, vl, w_refs, cols, lev, is_left, emit)
    filter_columns(plain_lhs(vh, vl), w_refs, 4, cols, lev, emit, after_group, seam)


def outer_kernel(last_row, one_hop, message_ref, own_ref, late_ref, rim_ref, dog_in, hess_in, dog_ref, hess_ref, *scratch):
    row, _ = mesh_place()
    from_above = (row % 2 == 1) if one_hop else (row % 2 == 0)
    for above in (True, False):

        @pl.when(from_above if above else jnp.logical_not(from_above))
        def _():
            outer_side(last_row, above, message_ref, own_ref, late_ref, rim_ref, dog_ref, hess_ref, *scratch)


def outer_side(last_row, above, message_ref, own_ref, late_ref, rim_ref, dog_ref, hess_ref, vh, vl, lev, d1, d2):
    _, rows, cols = dog_ref.shape
    row, col = mesh_place()
    is_left = col == 0
    diffs = {1: d1, 2: d2}
    rim_tall = RIM + 2 * PAD
    skip = PAD - 1 if above else PAD + 1
    outs = slice(0, RIM) if above else slice(rows - RIM, rows)
    height = LEVELS * RIM
    start = 3 * LEVELS * BLOCK + LEVELS * rows + (0 if above else 2 * height)
    lt_high = late_ref[start : start + height, : 3 * RIM + MESSAGE]
    lt_low = late_ref[start + height : start + 2 * height, :MESSAGE]
    own_first = 0 if above else rows - RIM

    def rows_of(part):
        message = message_ref[:, part]
        high = own_ref[own_first : own_first + RIM, part]
        low = own_ref[rows + own_first : rows + own_first + RIM, part]
        return mm(lt_high, jnp.concatenate([high, low, high, message], axis=0)) + mm(lt_low, message)

    def emit(k, at, d):
        to = slice(at, at + d.shape[1])
        zero = lambda count: jnp.zeros((count, d.shape[1]), F32)
        total = jnp.concatenate([zero(skip), d, zero(rim_tall - RIM - skip)], axis=0)
        if above:
            total = jnp.concatenate([total[:PAD], total[PAD:] + rim_ref[k, : rim_tall - PAD, to]], axis=0)
        else:
            own = total[: rim_tall - PAD] + rim_ref[k, rim_tall - PAD :, to]
            total = jnp.concatenate([own, total[rim_tall - PAD :]], axis=0)
        if 0 < at <= cols:
            dog_ref[k, outs, at - LANES : at - LANES + BLOCK] = (20.0 * total[PAD : PAD + RIM]).astype(BF16)
        if k in diffs:
            d = diffs[k]
            if above:
                d[:PAD, to] = jnp.where(row == 0, 0.0, total[:PAD])
                d[PAD:, to] = total[PAD:]
            else:
                d[: rim_tall - PAD, to] = total[: rim_tall - PAD]
                d[rim_tall - PAD :, to] = jnp.where(row == last_row, 0.0, total[rim_tall - PAD :])

    def after_group(m, tile, count):
        def put(t, value):
            hess_ref[m, outs, t * LANES : (t + 1) * LANES] = value

        hess_tiles(diffs[m + 1], 0, RIM, tile, count, 5000.0, put)

    place_rows(vh, vl, rows_of, cols, is_left)
    w_refs = band_refs(late_ref)
    seam = seam_filter(vh, vl, w_refs, cols, lev, is_left, emit)
    filter_columns(plain_lhs(vh, vl), w_refs, 8, cols, lev, emit, after_group, seam)


def coarse_kernel(last_row, keep_ref, other_ref, odd_ref, odd_other_ref, fine_dog_ref, fine_hess_ref, late_ref,
                  fine_dog_hbm, fine_hess_hbm, dog_hbm, hess_hbm,
                  dog_ref, hess_ref, ch, cl, ce, lev, d1, d2, sems):
    fine_copies = [
        pltpu.make_async_copy(fine_dog_ref, fine_dog_hbm, sems.at[0]),
        pltpu.make_async_copy(fine_hess_ref, fine_hess_hbm, sems.at[1]),
    ]
    for copy in fine_copies:
        copy.start()
    _, rows, cols = dog_ref.shape
    row, col = mesh_place()
    tall = lev.shape[1]
    diffs = {1: d1, 2: d2}
    is_left = col == 0
    half = cols // 2
    zero = jnp.zeros((tall, LANES), F32)
    for d in (d1, d2):
        d[:, :LANES] = zero
        d[:, LANES + cols :] = zero

    strip_rows = keep_ref.shape[0]
    height = -(-LEVELS * tall // 16) * 16
    variant = 2 * (row % 2) + col
    start = pl.multiple_of(late_ref.shape[0] - 4 * height + variant * height, 16)
    lh = late_ref[pl.ds(start, height), : 3 * strip_rows + 4 * MESSAGE]
    lp = lh[:, 3 * strip_rows :]
    values = []
    for at in range(0, cols, BLOCK):
        source = slice(at % half, at % half + BLOCK)
        second = slice(half + at % half, half + at % half + BLOCK)
        first = is_left if at < half else jnp.logical_not(is_left)
        value = jnp.where(first, keep_ref[:, source], other_ref[:, source])
        message = [jnp.where(first, odd_ref[:, lanes], odd_other_ref[:, lanes]) for lanes in (source, second)]
        at_seam = at in (half - BLOCK, half)
        if at_seam:
            join = lambda v: jnp.concatenate(
                [jnp.zeros(v.shape, v.dtype), v] if at < half else [v, jnp.zeros(v.shape, v.dtype)], axis=1
            )
            value = value + join(jnp.where(first, other_ref[:, half:], keep_ref[:, half:]))
            extra = jnp.where(first, odd_other_ref[:, cols:], odd_ref[:, cols:]).astype(F32)
            extra = [v.astype(BF16) for v in unpack_extra(extra)]
        high, low = split(value)
        stack = jnp.concatenate([high, low, high, *message, *message], axis=0)
        value = mm(lh, stack)
        if at_seam:
            value = value + join(mm(lp, jnp.concatenate([*extra, *extra], axis=0)))
        values.append(value[: LEVELS * tall])

    none = jnp.zeros((LEVELS * tall, LANES), F32)
    lane = lax.broadcasted_iota(jnp.int32, none.shape, 1)
    edges = []
    for j in range(len(values)):
        left = values[j - 1][:, BLOCK - LANES :] if j else none
        right = values[j + 1][:, :LANES] if j + 1 < len(values) else none
        value = jnp.where(lane < LANES // 2, right, left)
        eh = value.astype(BF16).astype(F32)
        el = value - eh
        eh = jnp.where((lane >= 16) & (lane < 64), pltpu.roll(eh, 32, 1), eh)
        edges.append(jnp.concatenate([eh, el], axis=1))
    for p in range(len(values) // 2):
        for s in range(LEVELS):
            part = slice(s * tall, (s + 1) * tall)
            ch[s, p], cl[s, p] = split(jnp.concatenate([values[2 * p][part], values[2 * p + 1][part]], axis=0))
            ce[s, p] = jnp.concatenate([edges[2 * p][part], edges[2 * p + 1][part]], axis=0).astype(BF16)

    def lhs(s, ats):
        pairs = range((ats[0] - LANES) // (2 * BLOCK), (ats[-1] - LANES) // (2 * BLOCK) + 1)
        return [jnp.concatenate([ref[s, p] for p in pairs], axis=0) for ref in (ch, cl, ce)]

    def emit(k, at, d):
        dog_ref[k, :, at - LANES : at - LANES + BLOCK] = (80.0 * d[:rows]).astype(BF16)
        if k in diffs:
            to = slice(at, at + BLOCK)
            diffs[k][:rows, to] = d[:rows]
            index = lax.broadcasted_iota(jnp.int32, (tall - rows, BLOCK), 0)
            below = index < (tall - rows) // 2
            out = (below & (row == last_row) & (col == 1)) | (jnp.logical_not(below) & (row == 0) & (col == 0))
            diffs[k][rows:, to] = jnp.where(out, 0.0, d[rows:])

    dog_copies = [pltpu.make_async_copy(dog_ref.at[k], dog_hbm.at[k], sems.at[4 + k]) for k in range(4)]
    hess_copies = [pltpu.make_async_copy(hess_ref.at[m], hess_hbm.at[m], sems.at[2 + m]) for m in range(2)]

    def after_group(m, first, count):
        def put(t, value):
            hess_ref[m, :, t * LANES : (t + 1) * LANES] = value

        hess_tiles(diffs[m + 1], 0, rows, first, count, 200000.0, put, 0, tall)

    def after_level(s):
        if s in (2, 3):
            dog_copies[s - 1].start()
        if s == 0:
            dog_copies[0].start()
            hess_copies[0].start()
            hess_copies[1].start()
        if s == 4:
            dog_copies[3].start()

    filter_columns(lhs, band_refs(late_ref), 8, cols, lev, emit, after_group, after_level)
    for copy in fine_copies + dog_copies + hess_copies:
        copy.wait()


def fine_constants(rows):
    own = np.arange(rows)
    own_inputs = np.concatenate([own, own, own])
    own_low = np.arange(3 * rows) >= 2 * rows
    nowhere = -1000
    top = np.full(MESSAGE, nowhere)
    top[: NEAR + 1] = np.append(np.arange(-NEAR, 0), -1)
    bot = np.full(MESSAGE, nowhere)
    bot[: NEAR + 1] = rows + np.append(np.arange(NEAR), 0)

    def matrix(sigma, centres, valid, inputs, use_low):
        high, low = two_parts(row_matrix(sigma, centres, inputs) * valid[:, None])
        return np.where(use_low[None, :], low.astype(np.float32), high.astype(np.float32)).astype(BF16)

    level = [matrix(s, own, np.ones(rows, np.float32), own_inputs, own_low) for s in SIGMAS]
    halo = []
    for inputs, rim, near_own, outer in (
        (top, np.arange(-1, RIM - 1), own[:RIM], 0),
        (bot, np.arange(rows + 1 - RIM, rows + 1), own[rows - RIM :], RIM - 1),
    ):
        ones = np.ones(RIM, np.float32)
        alone = (np.arange(RIM) == outer).astype(np.float32)
        triple = np.concatenate([near_own, near_own, near_own])
        triple_low = np.arange(3 * RIM) >= 2 * RIM
        again = inputs.copy()
        again[NEAR] = nowhere
        for s in SIGMAS:
            beside = matrix(s, rim, alone, triple, triple_low).astype(np.float32)
            beyond = matrix(s, rim, ones, inputs, np.zeros(MESSAGE, bool)).astype(np.float32)
            halo.append(np.concatenate([beside, beyond], axis=1))
        for s in SIGMAS:
            low = matrix(s, rim, ones, again, np.ones(MESSAGE, bool)).astype(np.float32)
            halo.append(np.pad(low, ((0, 0), (0, 3 * RIM))))
    count = rows // 2 + 2 * (REACH + 1)
    index = np.arange(-(-count // 8) * 8)
    base = matrix(SIGMAS[-1], 2 * (index - REACH - 1), (index < count).astype(np.float32), own_inputs, own_low)
    strip_rows = -(-(rows // 4 + 2 * (REACH + 1)) // 16) * 16
    return np.concatenate(level), np.concatenate(halo), base, strip_rows


def coarse_constants(strip, padded):
    inputs = np.arange(padded) - REACH - 1
    centres = np.concatenate([np.arange(strip + PAD // 2), np.arange(-PAD // 2, 0)])
    valid = ((centres >= -1) & (centres <= strip)).astype(np.float32)
    variants = []
    for parity in range(2):
        for core in range(2):
            first = (2 * strip + REACH + 1 - 6) * parity - strip * core - REACH - 1
            message = np.full(2 * MESSAGE, -1000)
            message[NEAR + 1 : MESSAGE] = first + np.arange(PART)
            message[MESSAGE + NEAR + 1 : 2 * MESSAGE - 1] = first + np.arange(PART, SPAN)
            for s in SIGMAS:
                high, low = two_parts(row_matrix(s, centres, inputs) * valid[:, None])
                more_high, more_low = two_parts(row_matrix(s, centres, message) * valid[:, None])
                variants.append(np.concatenate([high, high, low, more_high, more_low], axis=1))
            rest = -LEVELS * len(centres) % 16
            variants.append(np.zeros((rest, variants[-1].shape[1]), BF16))
    return np.concatenate(variants)


def joined(matrices, columns=BLOCK):
    return np.concatenate(
        [np.pad(m.reshape(-1, m.shape[-1]).astype(np.float32), ((0, 0), (0, columns - m.shape[-1]))) for m in matrices]
    ).astype(BF16)


def vmem_specs(count):
    return [pl.BlockSpec(memory_space=pltpu.VMEM) for _ in range(count)]


def far_specs(count):
    return [pl.BlockSpec(memory_space=pltpu.HBM) for _ in range(count)]


def limit(mib):
    return pltpu.CompilerParams(vmem_limit_bytes=mib * 2**20)


def far(value):
    return pltpu.with_memory_space_constraint(jnp.asarray(value), pltpu.HBM)


def local(image):
    rows, cols = image.shape
    row_count = lax.axis_size("row")
    strip = rows // 4
    wide = cols + LANES
    small = strip + PAD
    lh, lt, bm, strip_rows = fine_constants(rows)
    cw = coarse_constants(strip, strip_rows)
    bands = [column_weights(s, 1) for s in SIGMAS]
    wc, wl, we = (np.stack([b[i] for b in bands]) for i in range(3))
    early = jnp.asarray(joined([bm, *column_weights(SIGMAS[-1], 2)]))
    late = jnp.asarray(joined([wc, wl, we, lh, lt, cw]))
    base_rows = bm.shape[0]
    own_shape = jax.ShapeDtypeStruct((2 * rows, wide), BF16)
    message = jax.ShapeDtypeStruct((MESSAGE, wide), BF16)

    side = pl.pallas_call(
        border_kernel,
        out_shape=jax.ShapeDtypeStruct((rows, LANES), F32),
        in_specs=far_specs(1),
        out_specs=vmem_specs(1)[0],
        scratch_shapes=[pltpu.SemaphoreType.DMA],
        compiler_params=limit(1),
        cost_estimate=pl.CostEstimate(flops=2 * 10**9, bytes_accessed=10**7, transcendentals=0),
        name="border",
    )(far(image))
    side = lax.ppermute(side, "col", [(0, 1), (1, 0)])
    own, to_even, to_odd, base = pl.pallas_call(
        send_kernel,
        out_shape=(own_shape, message, message, jax.ShapeDtypeStruct((base_rows, cols // 2 + LANES), F32)),
        in_specs=vmem_specs(2),
        out_specs=tuple(vmem_specs(4)),
        scratch_shapes=[
            pltpu.VMEM((base_rows, cols + 2 * LANES), BF16),
            pltpu.VMEM((base_rows, cols + 2 * LANES), BF16),
        ],
        compiler_params=limit(6),
        cost_estimate=pl.CostEstimate(flops=10**9, bytes_accessed=10**6, transcendentals=0),
        name="send",
    )(image, early)
    own, to_even, to_odd = pl.pallas_call(
        side_kernel,
        out_shape=(own_shape, message, message),
        in_specs=vmem_specs(4),
        out_specs=tuple(vmem_specs(3)),
        input_output_aliases={1: 0, 2: 1, 3: 2},
        compiler_params=limit(4),
        name="side",
    )(side, own, to_even, to_odd)

    def swap(value, first):
        pairs = [(i, i + 1) for i in range(first, row_count - 1, 2)]
        return lax.ppermute(value, "row", pairs + [(j, i) for i, j in pairs])

    even = swap(to_even, 0)
    odd = swap(to_odd, 1)

    fine_shapes = (
        jax.ShapeDtypeStruct((4, rows, cols), BF16),
        jax.ShapeDtypeStruct((2, rows, cols), BF16),
    )
    coarse_shapes = (
        jax.ShapeDtypeStruct((4, strip, cols), BF16),
        jax.ShapeDtypeStruct((2, strip, cols), BF16),
    )

    def scratch(count, height, seam):
        padded_cols = cols + 2 * LANES
        return [
            pltpu.VMEM((LEVELS, height, padded_cols), BF16),
            pltpu.VMEM((LEVELS, height, padded_cols), BF16),
            pltpu.VMEM((2, height, padded_cols + seam), F32),
            pltpu.VMEM((count, padded_cols), F32),
            pltpu.VMEM((count, padded_cols), F32),
        ]

    rim_tall = RIM + 2 * PAD
    dog_fine, hess_fine, rim = pl.pallas_call(
        inner_kernel,
        out_shape=(*fine_shapes, jax.ShapeDtypeStruct((4, 2 * (RIM + PAD), cols + 2 * LANES), F32)),
        in_specs=vmem_specs(2),
        out_specs=tuple(vmem_specs(3)),
        scratch_shapes=scratch(rows, rows, BLOCK),
        compiler_params=limit(18),
        cost_estimate=pl.CostEstimate(flops=2 * 10**9, bytes_accessed=10**7, transcendentals=0),
        name="inner",
    )(own, late)

    def finish(one_hop, message, dog, hess):
        return pl.pallas_call(
            functools.partial(outer_kernel, row_count - 1, one_hop),
            out_shape=fine_shapes,
            in_specs=vmem_specs(6),
            out_specs=tuple(vmem_specs(2)),
            scratch_shapes=scratch(rim_tall, RIM, BLOCK),
            input_output_aliases={4: 0, 5: 1},
            compiler_params=limit(12),
            cost_estimate=pl.CostEstimate(flops=10**9, bytes_accessed=10**6, transcendentals=0),
            name="outer",
        )(message, own, late, rim, dog, hess)

    dog_fine, hess_fine = finish(True, even, dog_fine, hess_fine)

    keep, send = pl.pallas_call(
        functools.partial(base_kernel, row_count, rows // 2),
        out_shape=(
            jax.ShapeDtypeStruct((strip_rows, cols // 2 + LANES), F32),
            jax.ShapeDtypeStruct((strip_rows, cols // 2 + LANES), F32),
        ),
        in_specs=vmem_specs(2) + [pl.BlockSpec(memory_space=pl.ANY)],
        out_specs=tuple(vmem_specs(2)),
        scratch_shapes=[pltpu.VMEM((base_rows, LANES), F32)],
        compiler_params=limit(4),
        name="base",
    )(base, even, rim)
    other = lax.ppermute(send, "col", [(0, 1), (1, 0)])
    odd_other = lax.ppermute(odd, "col", [(0, 1), (1, 0)])
    dog_fine, hess_fine = finish(False, odd, dog_fine, hess_fine)

    return pl.pallas_call(
        functools.partial(coarse_kernel, row_count - 1),
        out_shape=fine_shapes + coarse_shapes,
        in_specs=vmem_specs(7),
        out_specs=tuple(far_specs(4)),
        scratch_shapes=[
            pltpu.VMEM((4, strip, cols), BF16),
            pltpu.VMEM((2, strip, cols), BF16),
            *[pltpu.VMEM((LEVELS, cols // (2 * BLOCK), 2 * small, BLOCK), BF16) for _ in range(3)],
            *scratch(small, small, 0)[2:],
            pltpu.SemaphoreType.DMA((8,)),
        ],
        compiler_params=limit(12),
        name="coarse",
    )(keep, other, odd, odd_other, dog_fine, hess_fine, late)


def solution(mesh):
    return jax.shard_map(
        local,
        mesh=mesh,
        in_specs=(P(("slab", "row"), "col"),),
        out_specs=(
            P(None, ("slab", "row"), "col"),
            P(None, ("slab", "row"), "col"),
            P(None, ("slab", "row", "col"), None),
            P(None, ("slab", "row", "col"), None),
        ),
        check_vma=False,
    )
```
